32 devices in a mesh: dp: 8 (over z, core), tensor: 4 (over y, x).
Axes of the slice: x: 2, y: 2, z: 4, core: 2. Of those that a mesh axis runs over, the one named last changes fastest.
Arguments:
- image_in: bfloat16 [8, 896, 1536], P('dp', None, 'tensor'), may hold values from -6 to 6
- text_in: bfloat16 [8, 154, 1536], P('dp', None, 'tensor'), may hold values from -6 to 6
- cond_in: bfloat16 [8, 1536], P(None, 'dp'), may hold values from -6 to 6
- mod_weight: bfloat16 [1, 2, 1536, 6, 1536], P(None, None, 'dp', None, 'tensor'), may hold values from -0.21875 to 0.21875
- mod_bias: bfloat16 [1, 2, 6, 1536], P(None, None, None, 'tensor'), may hold values from -3 to 3
- qkv_weight: bfloat16 [1, 2, 1536, 3, 1536], P(None, None, None, None, 'tensor'), may hold values from -0.15625 to 0.15625
- qkv_bias: bfloat16 [1, 2, 3, 1536], P(None, None, None, 'tensor'), may hold values from -2 to 2
- out_weight: bfloat16 [1, 2, 1536, 1536], P(None, None, None, 'tensor'), may hold values from -0.875 to 0.875
- out_bias: bfloat16 [1, 2, 1536], P(None, None, 'tensor'), may hold values from -2 to 2
- up_weight: bfloat16 [1, 2, 1536, 6144], P(None, None, None, 'tensor'), may hold values from -0.15625 to 0.15625
- up_bias: bfloat16 [1, 2, 6144], P(None, None, 'tensor'), may hold values from -3 to 3
- down_weight: bfloat16 [1, 2, 1536, 6144], P(None, None, None, 'tensor'), may hold values from -0.078125 to 0.078125
- down_bias: bfloat16 [1, 2, 1536], P(None, None, 'tensor'), may hold values from -2 to 2
- image_cot: bfloat16 [8, 896, 1536], P('dp', None, 'tensor'), may hold values from -6 to 6
- text_cot: bfloat16 [8, 154, 1536], P('dp', None, 'tensor'), may hold values from -6 to 6
Outputs:
- image_out: float32 [8, 896, 1536], P('dp', None, 'tensor')
- text_out: float32 [8, 154, 1536], P('dp', None, 'tensor')
- image_grad: float32 [8, 896, 1536], P('dp', None, 'tensor')
- text_grad: float32 [8, 154, 1536], P('dp', None, 'tensor')
- cond_grad: float32 [8, 1536], P(None, 'dp')
- mod_wgrad: float32 [1, 2, 1536, 6, 1536], P(None, None, 'dp', None, 'tensor')
- mod_bgrad: float32 [1, 2, 6, 1536], P(None, None, None, 'tensor')
- qkv_wgrad: float32 [1, 2, 1536, 3, 1536], P(None, None, 'dp', None, 'tensor')
- qkv_bgrad: float32 [1, 2, 3, 1536], P(None, None, None, 'tensor')
- out_wgrad: float32 [1, 2, 1536, 1536], P(None, None, 'dp', 'tensor')
- out_bgrad: float32 [1, 2, 1536], P(None, None, 'tensor')
- up_wgrad: float32 [1, 2, 1536, 6144], P(None, None, 'dp', 'tensor')
- up_bgrad: float32 [1, 2, 6144], P(None, None, 'tensor')
- down_wgrad: float32 [1, 2, 1536, 6144], P(None, None, 'dp', 'tensor')
- down_bgrad: float32 [1, 2, 1536], P(None, None, 'tensor')
The draws below stay inside these ranges and needn't reach their ends.
All inputs are finite; a program needn't handle non-finite values.
Results may differ from the reference program's by a relative error of at most 0.023.
The reference program's roundings to bfloat16 on the way count: a program that leaves them out, or rounds other values in their place, can miss the bound.
Values may be sent and summed in bfloat16 or wider, within the bound.
A program may use at most 320 MiB of HBM per device.

```python
import jax
import jax.numpy as jnp
from jax import lax

D = 1536
HEADS = 24
HEAD_DIM = 64
FF = 6144
NI = 896
NT = 154
LAYERS = 1
SEQS = 8


def spiked(result, rng, source, target, parts, factor):
    owner, partner = [(jnp.arange(result.shape[position]) // (result.shape[position] // parts)).reshape([-1 if axis == position else 1 for axis in range(result.ndim)]) for position in (source, target)]
    chosen = jax.random.permutation(rng, parts)[partner]
    strong = (owner == chosen) | (owner == (partner + parts // 2) % parts)
    return jnp.where(strong, factor * result, result)


def shard_levels(rng, extent, split, smallest, top_value):
    factor_of = 1.0
    for position, parts in split:
        steps = jax.random.uniform(jax.random.fold_in(jax.random.fold_in(rng, 6), position), (parts,), jnp.float32, smallest / len(split), top_value / len(split))
        factor_of = factor_of * jnp.repeat(jnp.exp(steps), extent[position] // parts).reshape((-1,) + (1,) * (len(extent) - 1 - position))
    return factor_of


def bell_draw(key, shape, deviation, reach, split=(), kind=jnp.bfloat16):
    factor_of = shard_levels(key, shape, split, -0.22, 0.18) if split else 1.0
    array = jax.random.normal(key, shape, jnp.float32) * deviation * factor_of
    return jnp.minimum(jnp.maximum(array, -reach), reach).astype(kind)


def heavy_noise(own_key, extent, spread, limit, cuts, heavy, kind=jnp.bfloat16):
    array = spread * jax.random.normal(own_key, extent, jnp.float32)
    if cuts:
        array = array * shard_levels(own_key, extent, cuts, -0.22, 0.18)
    return jnp.clip(spiked(array, jax.random.fold_in(own_key, 3), *heavy), -limit, limit).astype(kind)


def setup_inputs(seed: int = 0) -> dict:
    seeds = jax.random.split(jax.random.key(seed), 16)
    return {
        "image_in": bell_draw(seeds[0], (SEQS, NI, D), 1.0, 6.0, ((0, 8), (2, 4))),
        "text_in": bell_draw(seeds[1], (SEQS, NT, D), 1.0, 6.0, ((0, 8), (2, 4))),
        "cond_in": bell_draw(seeds[2], (SEQS, D), 1.0, 6.0, ((1, 8),)),
        "mod_weight": bell_draw(seeds[3], (LAYERS, 2, D, 6, D), (D // 2) ** -0.5, 0.21875, ((2, 8), (4, 4))),
        "mod_bias": bell_draw(seeds[4], (LAYERS, 2, 6, D), 0.5, 3.0, ((3, 4),)),
        "qkv_weight": bell_draw(seeds[5], (LAYERS, 2, D, 3, HEADS * HEAD_DIM), D ** -0.5, 0.15625, ((4, 4),)),
        "qkv_bias": bell_draw(seeds[6], (LAYERS, 2, 3, HEADS * HEAD_DIM), 0.3, 2.0, ((3, 4),)),
        "out_weight": bell_draw(seeds[7], (LAYERS, 2, D, HEADS * HEAD_DIM), (HEADS * HEAD_DIM // 32) ** -0.5, 0.875, ((3, 4),)),
        "out_bias": bell_draw(seeds[8], (LAYERS, 2, D), 0.3, 2.0, ((2, 4),)),
        "up_weight": bell_draw(seeds[9], (LAYERS, 2, D, FF), D ** -0.5, 0.15625, ((3, 4),)),
        "up_bias": bell_draw(seeds[10], (LAYERS, 2, FF), 0.5, 3.0, ((2, 4),)),
        "down_weight": bell_draw(seeds[11], (LAYERS, 2, D, FF), FF ** -0.5, 0.078125, ((3, 4),)),
        "down_bias": bell_draw(seeds[12], (LAYERS, 2, D), 0.3, 2.0, ((2, 4),)),
        "image_cot": heavy_noise(seeds[13], (SEQS, NI, D), 1.0, 6.0, ((0, 8), (2, 4)), (0, 2, 8, 2.0)),
        "text_cot": heavy_noise(seeds[14], (SEQS, NT, D), 1.0, 6.0, ((0, 8), (2, 4)), (0, 2, 8, 2.0)),
    }


@jax.custom_vjp
def low(v):
    return lax.optimization_barrier(v.astype(jnp.bfloat16)).astype(jnp.float32)

@jax.custom_vjp
def low_back(v):
    return v

def low_keep(v):
    return (low(v), None)

def low_pass(kept, grad):
    return (grad,)

def back_keep(v):
    return (v, None)

def back_low(kept, grad):
    return (low(grad),)
low.defvjp(low_keep, low_pass)
low_back.defvjp(back_keep, back_low)
highest = lax.Precision.HIGHEST
eps_norm = 1e-06

def layer_norm(values):
    row_mean = lax.optimization_barrier(jnp.mean(values, axis=-1, keepdims=True))
    centred = values - row_mean
    variance = lax.optimization_barrier(jnp.mean(centred * centred, axis=-1, keepdims=True))
    return centred * lax.rsqrt(variance + eps_norm)

def modulated(values, shift_row, scale_row):
    return low(layer_norm(values) * (1.0 + scale_row) + shift_row)

def joint_attention(joint_qkv):
    tokens = joint_qkv.shape[0]
    separated = joint_qkv.reshape(tokens, 3, HEADS, HEAD_DIM)
    scores = low_back(jnp.einsum('qhd,khd->hqk', separated[:, 0], separated[:, 1], precision=highest) * HEAD_DIM ** (-0.5))
    highest_score = lax.optimization_barrier(jnp.max(scores, axis=-1, keepdims=True))
    raised = jnp.exp(scores - highest_score)
    weights = raised / lax.optimization_barrier(jnp.sum(raised, axis=-1, keepdims=True))
    mixed_heads = jnp.einsum('hqk,khd->qhd', low(weights), separated[:, 2], precision=highest)
    return low_back(low(mixed_heads.reshape(tokens, HEADS * HEAD_DIM)))

def one_sequence(image_seq, text_seq, mod_seq, params):
    qkv_weight, qkv_bias, out_weight, out_bias, up_weight, up_bias, down_weight, down_bias = params
    streams = [image_seq, text_seq]
    for layer_at in range(LAYERS):
        projected = []
        for stream in range(2):
            normed = modulated(streams[stream], mod_seq[layer_at, stream, 0], mod_seq[layer_at, stream, 1])
            linear = jnp.einsum('nd,dje->nje', normed, qkv_weight[layer_at, stream], precision=highest) + qkv_bias[layer_at, stream]
            projected.append(low_back(low(linear)))
        mixed_heads = joint_attention(jnp.concatenate(projected, axis=0))
        pieces = [mixed_heads[:NI], mixed_heads[NI:]]
        for stream in range(2):
            branch = low_back(jnp.einsum('ne,de->nd', pieces[stream], out_weight[layer_at, stream], precision=highest) + out_bias[layer_at, stream])
            streams[stream] = streams[stream] + mod_seq[layer_at, stream, 2] * branch
            normed = modulated(streams[stream], mod_seq[layer_at, stream, 3], mod_seq[layer_at, stream, 4])
            hidden = low_back(jnp.einsum('nd,df->nf', normed, up_weight[layer_at, stream], precision=highest) + up_bias[layer_at, stream])
            activated = low(jax.nn.gelu(hidden, approximate=True))
            branch = low_back(jnp.einsum('nf,df->nd', activated, down_weight[layer_at, stream], precision=highest) + down_bias[layer_at, stream])
            streams[stream] = streams[stream] + mod_seq[layer_at, stream, 5] * branch
    return (streams[0], streams[1])

def forward(image_in, text_in, cond_in, mod_weight, mod_bias, qkv_weight, qkv_bias, out_weight, out_bias, up_weight, up_bias, down_weight, down_bias):
    cond_act = low(jax.nn.silu(cond_in))
    modulation = low_back(jnp.einsum('sc,lxcjd->slxjd', cond_act, mod_weight, precision=highest) + mod_bias)
    params = (qkv_weight, qkv_bias, out_weight, out_bias, up_weight, up_bias, down_weight, down_bias)

    def per_sequence(carried):
        return one_sequence(carried[0], carried[1], carried[2], params)
    return lax.map(jax.checkpoint(per_sequence), (image_in, text_in, modulation))

def reference(image_in, text_in, cond_in, mod_weight, mod_bias, qkv_weight, qkv_bias, out_weight, out_bias, up_weight, up_bias, down_weight, down_bias, image_cot, text_cot):
    inputs = tuple((array_in.astype(jnp.float32) for array_in in (image_in, text_in, cond_in, mod_weight, mod_bias, qkv_weight, qkv_bias, out_weight, out_bias, up_weight, up_bias, down_weight, down_bias)))
    outputs, pullback = jax.vjp(forward, *inputs)
    gradients = pullback((image_cot.astype(jnp.float32), text_cot.astype(jnp.float32)))
    return (outputs[0], outputs[1], gradients[0], gradients[1], gradients[2], gradients[3], gradients[4], gradients[5], gradients[6], gradients[7], gradients[8], gradients[9], gradients[10], gradients[11], gradients[12])
```

```python
import functools

import jax
import jax.numpy as jnp
from jax import lax
from jax.experimental import pallas as pl
from jax.experimental.pallas import tpu as pltpu
from jax.sharding import PartitionSpec as P

HEAD_DIM = 64
EPS = 1e-06
F32 = jnp.float32
BF16 = jnp.bfloat16
GELU_C = 0.7978845608028654
GELU_K = 0.044715
MIB = 1 << 20


def nt_dot(a, b):
    return lax.dot_general(a, b, (((1,), (1,)), ((), ())), preferred_element_type=F32)


def nn_dot(a, b):
    return lax.dot_general(a, b, (((1,), (0,)), ((), ())), preferred_element_type=F32)


def tn_dot(a, b):
    return lax.dot_general(a, b, (((0,), (0,)), ((), ())), preferred_element_type=F32)


def exact_nt(a, b):
    return lax.dot_general(
        a, b, (((1,), (1,)), ((), ())), preferred_element_type=F32, precision=lax.Precision.HIGHEST
    )


def exact_tn(a, b):
    return lax.dot_general(
        a, b, (((0,), (0,)), ((), ())), preferred_element_type=F32, precision=lax.Precision.HIGHEST
    )


def call(kernel, name, base, arrays, in_specs, outs, out_specs, grid, scratch=(), flops=0, vmem=48):
    moved = sum(a.size * a.dtype.itemsize for a in arrays)
    moved += sum(o.size * o.dtype.itemsize for o in outs)
    return pl.pallas_call(
        kernel,
        out_shape=outs,
        grid_spec=pltpu.PrefetchScalarGridSpec(
            num_scalar_prefetch=1,
            grid=grid,
            in_specs=in_specs,
            out_specs=out_specs,
            scratch_shapes=list(scratch),
        ),
        compiler_params=pltpu.CompilerParams(
            dimension_semantics=("arbitrary",) * len(grid), vmem_limit_bytes=vmem * MIB
        ),
        cost_estimate=pl.CostEstimate(flops=flops, bytes_accessed=moved, transcendentals=0),
        name=name,
    )(base, *arrays)


def sds(shape, dtype):
    return jax.ShapeDtypeStruct(shape, dtype)


def rows_spec(block, width):
    return pl.BlockSpec((block, width), lambda i, t: (i, 0))


def whole_spec(shape):
    zeros = (0,) * len(shape)
    return pl.BlockSpec(shape, lambda *_: zeros)


def stream_spec(shape, stream):
    tail = (0,) * (len(shape) - 1)
    return pl.BlockSpec((1,) + shape[1:], lambda *_: (stream,) + tail)


def row_block(rows):
    return rows // 2 if rows % 32 == 0 and rows >= 256 else rows


def norm_stats(pieces, width):
    total = sum(jnp.sum(p, axis=-1, keepdims=True) for p in pieces)
    mean = total / width
    centred = [p - mean for p in pieces]
    var = sum(jnp.sum(c * c, axis=-1, keepdims=True) for c in centred) / width
    return mean, lax.rsqrt(var + EPS), centred


def qkv_kernel(n, width, row, t_ref, *refs):
    x_refs, (mod_ref, w_ref, b_ref, m_ref, out_ref) = refs[:n], refs[n:]
    base = t_ref[0]
    _, inv, centred = norm_stats([x[...].astype(F32) for x in x_refs], width)
    acc = [None] * 3
    for k in range(n):
        shift, scale = mod_ref[k, row : row + 1, :], mod_ref[k, row + 1 : row + 2, :]
        m = (centred[k] * inv * (1.0 + scale) + shift).astype(BF16)
        m_ref[k] = m
        for j in range(3):
            part = nn_dot(m, w_ref[0, j, base ^ k])
            acc[j] = part if k == 0 else acc[j] + part
    for j in range(3):
        out_ref[j] = (acc[j] + b_ref[j : j + 1, :]).astype(BF16)


def qkv_call(base, pieces, mods, weight, bias, stream):
    n = len(pieces)
    rows, feats = pieces[0].shape
    cols = weight.shape[-1]
    rb = row_block(rows)
    return call(
        functools.partial(qkv_kernel, n, n * feats, stream * 6),
        f"qkv{stream}",
        base,
        [*pieces, mods, weight, bias],
        [rows_spec(rb, feats)] * n
        + [whole_spec(mods.shape), stream_spec(weight.shape, stream), whole_spec(bias.shape)],
        [sds((n, rows, feats), BF16), sds((3, rows, cols), BF16)],
        [
            pl.BlockSpec((n, rb, feats), lambda i, t: (0, i, 0)),
            pl.BlockSpec((3, rb, cols), lambda i, t: (0, i, 0)),
        ],
        (rows // rb,),
        flops=2 * rows * n * feats * 3 * cols,
    )


def lane_block(cols):
    return 128 if cols % 128 == 0 else cols


def attn_fwd_kernel(counts, t_ref, *refs):
    s = len(counts)
    q_ref, k_refs, v_refs = refs[0], refs[1 : 1 + s], refs[1 + s : 1 + 2 * s]
    o_ref, lse_ref, k_all, v_all = refs[1 + 2 * s :]
    at = 0
    for i, c in enumerate(counts):
        k_all[at : at + c, :] = k_refs[i][0]
        v_all[at : at + c, :] = v_refs[i][0]
        at += c
    rows, lanes = o_ref.shape
    heads = lanes // HEAD_DIM
    rb = row_block(rows)
    owner = lax.broadcasted_iota(jnp.int32, (1, lanes), 1) // HEAD_DIM
    keys = k_all[...]
    values = v_all[...]
    aug = [jnp.where(owner == h, values, jnp.ones_like(values)) for h in range(heads)]
    for r in range(rows // rb):
        at = r * rb
        q = q_ref[0, at : at + rb, :] * jnp.asarray(HEAD_DIM**-0.5, BF16)
        out = jnp.zeros((rb, lanes), F32)
        lse = jnp.zeros((rb, lanes), F32)
        for h in range(heads):
            mine = owner == h
            scores = nt_dot(jnp.where(mine, q, jnp.zeros_like(q)), keys)
            top = jnp.max(scores, axis=-1, keepdims=True)
            raised = jnp.exp(scores - top).astype(BF16)
            acc = nn_dot(raised, aug[h])
            other = ((h + 1) % heads) * HEAD_DIM
            denom = acc[:, other : other + 1]
            out = jnp.where(mine, acc / denom, out)
            lse = jnp.where(mine, top + jnp.log(denom), lse)
        o_ref[at : at + rb, :] = out.astype(BF16)
        lse_ref[at : at + rb, :] = lse


def attn_fwd_call(base, qkvs, seg):
    counts = [a.shape[1] for a in qkvs]
    total = sum(counts)
    cols = qkvs[0].shape[2]
    lanes = lane_block(cols)
    rows = counts[seg]

    def spec(j, c):
        return pl.BlockSpec((1, c, lanes), lambda g, t: (j, 0, g))

    out_spec = pl.BlockSpec((rows, lanes), lambda g, t: (0, g))
    return call(
        functools.partial(attn_fwd_kernel, counts),
        f"attn_fwd{seg}",
        base,
        [qkvs[seg], *qkvs, *qkvs],
        [spec(0, rows)] + [spec(1, c) for c in counts] + [spec(2, c) for c in counts],
        [sds((rows, cols), BF16), sds((rows, cols), F32)],
        [out_spec, out_spec],
        (cols // lanes,),
        scratch=[pltpu.VMEM((total, lanes), BF16), pltpu.VMEM((total, lanes), BF16)],
        flops=4 * rows * total * cols * 4,
    )


def attn_bwd_kernel(counts, blocks, t_ref, *refs):
    s = len(counts)
    groups = [refs[i * s : (i + 1) * s] for i in range(6)]
    q_refs, k_refs, v_refs, o_refs, do_refs, lse_refs = groups
    outs = refs[6 * s : 7 * s]
    q_all, k_all, v_all, do_all, lse_all, od_all, dk_all, dv_all, dqt_all, dq_all = refs[7 * s :]
    total, lanes = q_all.shape
    heads = lanes // HEAD_DIM
    at = 0
    for i, c in enumerate(counts):
        sl = slice(at, at + c)
        q_all[sl, :] = q_refs[i][0] * jnp.asarray(HEAD_DIM**-0.5, BF16)
        k_all[sl, :] = k_refs[i][0]
        v_all[sl, :] = v_refs[i][0]
        do_all[sl, :] = do_refs[i][...]
        lse_all[sl, :] = lse_refs[i][...]
        od_all[sl, :] = o_refs[i][...].astype(F32) * do_refs[i][...].astype(F32)
        at += c
    head_row = lax.broadcasted_iota(jnp.int32, (8, lanes), 0)
    lane = lax.broadcasted_iota(jnp.int32, (8, lanes), 1)
    first = (lane == head_row * HEAD_DIM).astype(F32)
    within = (lane // HEAD_DIM == head_row).astype(F32)
    lse_rows = exact_nt(first, lse_all[...])
    dot_rows = exact_nt(within, od_all[...])
    owner = lax.broadcasted_iota(jnp.int32, (1, lanes), 1) // HEAD_DIM
    dqt = jnp.zeros((lanes, total), F32)
    for h in range(heads):
        mine = owner == h
        q = jnp.where(mine, q_all[...], jnp.zeros((), BF16))
        do = jnp.where(mine, do_all[...], jnp.zeros((), BF16))
        lse_row, dot_row = lse_rows[h : h + 1, :], dot_rows[h : h + 1, :]
        for start, size in blocks:
            sl = slice(start, start + size)
            keys, values = k_all[sl, :], v_all[sl, :]
            weights = jnp.exp(nt_dot(keys, q) - lse_row)
            grads = (weights * (nt_dot(values, do) - dot_row)).astype(BF16)
            dv = nn_dot(weights.astype(BF16), do)
            dk = nn_dot(grads, q)
            if h == 0:
                dv_all[sl, :] = dv
                dk_all[sl, :] = dk
            else:
                dv_all[sl, :] += dv
                dk_all[sl, :] += dk
            scaled = jnp.where(mine, keys, jnp.zeros((), BF16)) * jnp.asarray(HEAD_DIM**-0.5, BF16)
            dqt = dqt + tn_dot(scaled, grads)
    dqt_all[:, :total] = dqt
    dq_all[...] = dqt_all[...].T
    at = 0
    for i, c in enumerate(counts):
        sl = slice(at, at + c)
        outs[i][0] = dq_all[sl, :].astype(BF16)
        outs[i][1] = dk_all[sl, :].astype(BF16)
        outs[i][2] = dv_all[sl, :].astype(BF16)
        at += c


def attn_bwd_call(base, qkvs, os, dos, lses):
    counts = [a.shape[1] for a in qkvs]
    total = sum(counts)
    cols = qkvs[0].shape[2]
    lanes = lane_block(cols)
    padded = -(-total // 128) * 128
    step = -(-total // 3 // 16) * 16
    step += 16 * (step * 3 < total)
    blocks = [(b, min(step, total - b)) for b in range(0, total, step)]

    def spec3(j, c):
        return pl.BlockSpec((1, c, lanes), lambda g, t: (j, 0, g))

    def spec2(c):
        return pl.BlockSpec((c, lanes), lambda g, t: (0, g))

    in_specs = [spec3(j, c) for j in range(3) for c in counts] + [spec2(c) for c in counts] * 3
    return call(
        functools.partial(attn_bwd_kernel, counts, blocks),
        "attn_bwd",
        base,
        [*qkvs, *qkvs, *qkvs, *os, *dos, *lses],
        in_specs,
        [sds((3, c, cols), BF16) for c in counts],
        [pl.BlockSpec((3, c, lanes), lambda g, t: (0, 0, g)) for c in counts],
        (cols // lanes,),
        scratch=[pltpu.VMEM((total, lanes), BF16)] * 4
        + [pltpu.VMEM((total, lanes), F32)] * 4
        + [pltpu.VMEM((lanes, padded), F32), pltpu.VMEM((padded, lanes), F32)],
        flops=10 * total * total * cols * 4,
        vmem=56,
    )


def out_kernel(n, t_ref, o_ref, w_ref, *outs):
    base = t_ref[0]
    o = o_ref[...]
    for k in range(n):
        outs[k][...] = nt_dot(o, w_ref[0, base ^ k]).astype(BF16)


def out_call(base, o, weight, stream):
    rows, cols = o.shape
    n, feats = weight.shape[1], weight.shape[2]
    return call(
        functools.partial(out_kernel, n),
        f"out{stream}",
        base,
        [o, weight],
        [whole_spec(o.shape), stream_spec(weight.shape, stream)],
        [sds((rows, feats), BF16)] * n,
        [whole_spec((rows, feats))] * n,
        (1,),
        flops=2 * rows * cols * n * feats,
    )


def do_kernel(n, t_ref, *refs):
    base = t_ref[0]
    w_ref, out_ref = refs[n:]
    acc = nn_dot(refs[0][...], w_ref[0, base])
    for k in range(1, n):
        acc = acc + nn_dot(refs[k][...], w_ref[0, base ^ k])
    out_ref[...] = acc.astype(BF16)


def do_call(base, pieces, weight, stream):
    n = len(pieces)
    rows, feats = pieces[0].shape
    cols = weight.shape[-1]
    return call(
        functools.partial(do_kernel, n),
        f"do{stream}",
        base,
        [*pieces, weight],
        [whole_spec((rows, feats))] * n + [stream_spec(weight.shape, stream)],
        [sds((rows, cols), BF16)],
        [whole_spec((rows, cols))],
        (1,),
        flops=2 * rows * cols * n * feats,
    )[0]


def pack_stats(mean, inv, first, second):
    lane = lax.broadcasted_iota(jnp.int32, (mean.shape[0], 128), 1)
    cols = jnp.where(lane == 0, mean, jnp.where(lane == 1, inv, 0.0))
    sums = jnp.where(lane == 0, first, jnp.where(lane == 1, second, 0.0))
    pick = (
        lax.broadcasted_iota(jnp.int32, (8, 128), 0) == lax.broadcasted_iota(jnp.int32, (8, 128), 1)
    ).astype(F32)
    return cols, exact_nt(pick, sums)


def mlp_kernel(n, width, row, t_ref, *refs):
    x_refs, g_refs = refs[:n], refs[n : 2 * n]
    mod_ref, up_ref, bias_ref, down_ref = refs[2 * n : 2 * n + 4]
    m_ref, a_ref, du_ref, cols_ref, sums_ref, dub_ref = refs[2 * n + 4 : 2 * n + 10]
    b_refs, dm_refs = refs[2 * n + 10 : 3 * n + 10], refs[3 * n + 10 :]
    base = t_ref[0]
    mean, inv, centred = norm_stats([x[...].astype(F32) for x in x_refs], width)
    u = None
    for k in range(n):
        shift, scale = mod_ref[k, row : row + 1, :], mod_ref[k, row + 1 : row + 2, :]
        m = (centred[k] * inv * (1.0 + scale) + shift).astype(BF16)
        m_ref[k] = m
        part = nn_dot(m, up_ref[0, base ^ k])
        u = part if u is None else u + part
    u = u + bias_ref[...]
    square = u * u
    th = jnp.tanh(GELU_C * (u + GELU_K * square * u))
    a = (0.5 * u * (1.0 + th)).astype(BF16)
    slope = 0.5 * (1.0 + th) + 0.5 * u * (1.0 - th * th) * (
        GELU_C * (1.0 + 3.0 * GELU_K * square)
    )
    a_ref[...] = a
    da = None
    for k in range(n):
        part = nn_dot(g_refs[k][...], down_ref[0, base ^ k])
        da = part if da is None else da + part
    du = (da * slope).astype(BF16)
    du_ref[...] = du
    du_sum = jnp.sum(du.astype(F32), axis=0, keepdims=True)

    @pl.when(pl.program_id(0) == 0)
    def _():
        dub_ref[...] = du_sum

    @pl.when(pl.program_id(0) != 0)
    def _():
        dub_ref[...] += du_sum

    first = second = None
    for k in range(n):
        dm = nt_dot(du, up_ref[0, base ^ k])
        dm_refs[k][...] = dm.astype(BF16)
        dh = dm * (1.0 + mod_ref[k, row + 1 : row + 2, :])
        one = jnp.sum(dh, axis=-1, keepdims=True)
        two = jnp.sum(dh * centred[k], axis=-1, keepdims=True)
        first = one if first is None else first + one
        second = two if second is None else second + two
    for k in range(n):
        b_refs[k][...] = nt_dot(a, down_ref[0, base ^ k]).astype(BF16)
    cols, sums = pack_stats(mean, inv, first, second * inv)
    cols_ref[...] = cols
    sums_ref[0] = sums


def mlp_call(base, pieces, grads, mods, up, up_bias, down, stream):
    n = len(pieces)
    rows, feats = pieces[0].shape
    hidden = up.shape[-1]
    rb = row_block(rows)
    steps = rows // rb
    outs = call(
        functools.partial(mlp_kernel, n, n * feats, stream * 6 + 3),
        f"mlp{stream}",
        base,
        [*pieces, *grads, mods, up, up_bias, down],
        [rows_spec(rb, feats)] * (2 * n)
        + [
            whole_spec(mods.shape),
            stream_spec(up.shape, stream),
            whole_spec(up_bias.shape),
            stream_spec(down.shape, stream),
        ],
        [
            sds((n, rows, feats), BF16),
            sds((rows, hidden), BF16),
            sds((rows, hidden), BF16),
            sds((rows, 128), F32),
            sds((steps, 8, rb), F32),
            sds((1, hidden), F32),
        ]
        + [sds((rows, feats), BF16)] * (2 * n),
        [
            pl.BlockSpec((n, rb, feats), lambda i, t: (0, i, 0)),
            rows_spec(rb, hidden),
            rows_spec(rb, hidden),
            rows_spec(rb, 128),
            pl.BlockSpec((1, 8, rb), lambda i, t: (i, 0, 0)),
            whole_spec((1, hidden)),
        ]
        + [rows_spec(rb, feats)] * (2 * n),
        (steps,),
        flops=8 * rows * n * feats * hidden,
        vmem=56,
    )
    m, a, du, cols, sums, dub = outs[:6]
    return m, a, du, cols, sums, dub, outs[6 : 6 + n], outs[6 + n :]


def dm_kernel(n, width, row, t_ref, *refs):
    x_refs = refs[:n]
    mod_ref, dq_ref, w_ref, cols_ref, sums_ref, bias_ref = refs[n : n + 6]
    dm_refs = refs[n + 6 :]
    base = t_ref[0]
    mean, inv, centred = norm_stats([x[...].astype(F32) for x in x_refs], width)
    first = second = None
    parts = [dq_ref[j] for j in range(3)]
    for k in range(n):
        dm = nt_dot(parts[0], w_ref[0, 0, base ^ k])
        for j in range(1, 3):
            dm = dm + nt_dot(parts[j], w_ref[0, j, base ^ k])
        dm_refs[k][...] = dm.astype(BF16)
        dh = dm * (1.0 + mod_ref[k, row + 1 : row + 2, :])
        one = jnp.sum(dh, axis=-1, keepdims=True)
        two = jnp.sum(dh * centred[k], axis=-1, keepdims=True)
        first = one if first is None else first + one
        second = two if second is None else second + two
    for j in range(3):
        total = jnp.sum(parts[j].astype(F32), axis=0, keepdims=True)

        @pl.when(pl.program_id(0) == 0)
        def _():
            bias_ref[j : j + 1, :] = total

        @pl.when(pl.program_id(0) != 0)
        def _():
            bias_ref[j : j + 1, :] += total

    cols, sums = pack_stats(mean, inv, first, second * inv)
    cols_ref[...] = cols
    sums_ref[0] = sums


def dm_call(base, pieces, mods, dqkv, weight, stream):
    n = len(pieces)
    rows, feats = pieces[0].shape
    cols = dqkv.shape[-1]
    rb = row_block(rows)
    steps = rows // rb
    outs = call(
        functools.partial(dm_kernel, n, n * feats, stream * 6),
        f"dm{stream}",
        base,
        [*pieces, mods, dqkv, weight],
        [rows_spec(rb, feats)] * n
        + [
            whole_spec(mods.shape),
            pl.BlockSpec((3, rb, cols), lambda i, t: (0, i, 0)),
            stream_spec(weight.shape, stream),
        ],
        [sds((rows, 128), F32), sds((steps, 8, rb), F32), sds((3, cols), F32)]
        + [sds((rows, feats), BF16)] * n,
        [
            rows_spec(rb, 128),
            pl.BlockSpec((1, 8, rb), lambda i, t: (i, 0, 0)),
            whole_spec((3, cols)),
        ]
        + [rows_spec(rb, feats)] * n,
        (steps,),
        flops=2 * rows * n * feats * 3 * cols,
    )
    return outs[0], outs[1], outs[2], outs[3:]


def norm_back_kernel(width, row, gate_row, has_gate, t_ref, *refs):
    p_refs = refs[:3]
    x_ref, cols_ref, sums_ref, g_ref, mod_ref = refs[3:8]
    rest = refs[8:]
    total = sum(p[...].astype(F32) for p in p_refs)
    mean, inv = cols_ref[:, 0:1], cols_ref[:, 1:2]
    pick = (
        lax.broadcasted_iota(jnp.int32, (8, 128), 0) == lax.broadcasted_iota(jnp.int32, (8, 128), 1)
    ).astype(F32)
    sums = exact_tn(sums_ref[0], pick)
    mean_grad, mean_cross = sums[:, 0:1] / width, sums[:, 1:2] / width
    normed = (x_ref[...].astype(F32) - mean) * inv
    grad = total * (1.0 + mod_ref[0, row + 1 : row + 2, :])
    g = g_ref[...].astype(F32) + inv * (grad - mean_grad - normed * mean_cross)
    lines = [
        jnp.sum(total, axis=0, keepdims=True),
        jnp.sum(total * normed, axis=0, keepdims=True),
    ]
    if has_gate:
        branch_ref, g_out, db_ref, line_ref = rest
        db = (mod_ref[0, gate_row : gate_row + 1, :] * g).astype(BF16)
        db_ref[...] = db
        lines.append(jnp.sum(branch_ref[...] * g, axis=0, keepdims=True))
        lines.append(jnp.sum(db.astype(F32), axis=0, keepdims=True))
    else:
        g_out, line_ref = rest
    g_out[...] = g

    @pl.when(pl.program_id(0) == 0)
    def _():
        for i, line in enumerate(lines):
            line_ref[i : i + 1, :] = line

    @pl.when(pl.program_id(0) != 0)
    def _():
        for i, line in enumerate(lines):
            line_ref[i : i + 1, :] += line


def norm_back_call(base, parts, x_own, cols, sums, g, mods, stream, width, which, branch=None):
    rows, feats = x_own.shape
    rb = sums.shape[2]
    row = stream * 6 + (3 if which == 2 else 0)
    gated = branch is not None
    arrays = [*parts, x_own, cols, sums, g, mods]
    specs = [rows_spec(rb, feats)] * 4 + [
        rows_spec(rb, 128),
        pl.BlockSpec((1, 8, rb), lambda i, t: (i, 0, 0)),
        rows_spec(rb, feats),
        pl.BlockSpec((1,) + mods.shape[1:], lambda i, t: (0, 0, 0)),
    ]
    outs = [sds((rows, feats), F32)]
    out_specs = [rows_spec(rb, feats)]
    if gated:
        arrays.append(branch)
        specs.append(rows_spec(rb, feats))
        outs.append(sds((rows, feats), BF16))
        out_specs.append(rows_spec(rb, feats))
    outs.append(sds((4 if gated else 2, feats), F32))
    out_specs.append(whole_spec((4 if gated else 2, feats)))
    return call(
        functools.partial(norm_back_kernel, width, row, stream * 6 + 2, gated),
        f"norm_back{which}_{stream}",
        base,
        arrays,
        specs,
        outs,
        out_specs,
        (rows // rb,),
        flops=rows * feats * 20,
    )


def wgrad_kernel(segs, groups, split, t_ref, *refs):
    lhs, rhs, out_ref = refs[:segs], refs[segs : 2 * segs], refs[2 * segs]
    for j in range(groups):
        acc = None
        for i in range(segs):
            right = rhs[i][j] if groups > 1 else rhs[i][...]
            part = tn_dot(lhs[i][0], right)
            acc = part if acc is None else acc + part
        rows = acc.shape[0] // split
        for p in range(split):
            piece = acc[p * rows : (p + 1) * rows].astype(out_ref.dtype)
            if groups > 1:
                out_ref[p, j] = piece
            else:
                out_ref[p] = piece


def wgrad_call(base, lefts, rights, dp, name, dtype=BF16):
    segs = len(lefts)
    n, _, feats = lefts[0].shape
    groups = rights[0].shape[0] if rights[0].ndim == 3 else 1
    cols = rights[0].shape[-1]
    split = dp // n
    rows = feats // split
    mid = (groups,) if groups > 1 else ()
    zeros = (0,) * len(mid)
    return call(
        functools.partial(wgrad_kernel, segs, groups, split),
        name,
        base,
        [*lefts, *rights],
        [pl.BlockSpec((1, a.shape[1], feats), lambda k, t: (k, 0, 0)) for a in lefts]
        + [whole_spec(a.shape) for a in rights],
        [sds((dp, *mid, rows, cols), dtype)],
        [pl.BlockSpec((split, *mid, rows, cols), lambda k, t: (t[0] ^ k, *zeros, 0, 0))],
        (n,),
        flops=2 * n * feats * groups * cols * sum(a.shape[1] for a in lefts),
    )[0]


class Square:
    X = [(0, 1), (1, 0), (2, 3), (3, 2)]
    Y = [(0, 2), (2, 0), (1, 3), (3, 1)]
    DIAG = [(0, 3), (3, 0), (1, 2), (2, 1)]

    def __init__(self):
        self.count = 4
        self.base = lax.axis_index("tensor").astype(jnp.int32).reshape(1)

    def send(self, value, pairs):
        return lax.ppermute(value, "tensor", pairs)

    def gather(self, value, route):
        along_x, along_y = self.send(value, self.X), self.send(value, self.Y)
        corner = self.send(along_x, self.Y) if route == 0 else self.send(along_y, self.X)
        return [value, along_x, along_y, corner]

    def scatter(self, parts, route):
        own, by_x, by_y, corner = parts
        if route == 0:
            relayed = self.send(corner, self.X) + by_y
            return [own, self.send(by_x, self.X), self.send(relayed, self.Y)]
        relayed = self.send(corner, self.Y) + by_x
        return [own, self.send(by_y, self.Y), self.send(relayed, self.X)]

    def gather_small(self, value):
        return [value] + [self.send(value, p) for p in (self.X, self.Y, self.DIAG)]

    def total(self, value):
        return sum(self.gather_small(value))


class Line:
    def __init__(self, count):
        self.count = count
        self.base = jnp.zeros((1,), jnp.int32)

    def gather(self, value, route):
        whole = lax.all_gather(value, "tensor", axis=0)
        return [whole[k] for k in range(self.count)]

    gather_small = functools.partialmethod(gather, route=0)

    def scatter(self, parts, route):
        got = lax.psum_scatter(jnp.stack(parts), "tensor", scatter_dimension=0)
        return [got, jnp.zeros_like(got), jnp.zeros_like(got)]

    def total(self, value):
        return lax.psum(value, "tensor")


def own_of(mods, ring):
    if isinstance(ring, Square):
        return mods
    return lax.dynamic_index_in_dim(mods, lax.axis_index("tensor"), 0)


def body(
    dp,
    tensor,
    image_in,
    text_in,
    cond_in,
    mod_weight,
    mod_bias,
    qkv_weight,
    qkv_bias,
    out_weight,
    out_bias,
    up_weight,
    up_bias,
    down_weight,
    down_bias,
    image_cot,
    text_cot,
):
    ring = Square() if tensor == 4 else Line(tensor)
    base, n = ring.base, ring.count
    feats = image_in.shape[2]
    width = feats * n
    half = image_in.shape[1] // 2
    segs = [(0, 0, half), (0, half, half), (1, 0, text_in.shape[1])]
    routes = [0, 1, 0]
    inputs, cots = (image_in[0], text_in[0]), (image_cot[0], text_cot[0])

    def cut(pair, seg):
        stream, start, rows = seg
        value = pair[stream]
        return value if value.shape[0] == rows else value[start : start + rows]

    xs = [cut(inputs, seg) for seg in segs]
    gs = [cut(cots, seg) for seg in segs]
    count = len(segs)
    every = range(count)
    x_pieces = [ring.gather(xs[i], routes[i]) for i in every]

    cond_float = cond_in.astype(F32)
    cond_act = jax.nn.silu(cond_float).astype(BF16)
    mod_w = jnp.transpose(mod_weight[0], (0, 2, 1, 3)).reshape(12, -1, feats)
    terms = jnp.einsum("sc,gcd->sgd", cond_act, mod_w, preferred_element_type=F32)
    mine = jnp.sum(lax.all_to_all(terms, "dp", split_axis=0, concat_axis=0, tiled=True), axis=0)
    mine = mine + mod_bias[0].reshape(12, feats).astype(F32)
    mods = jnp.stack(ring.gather_small(mine))
    own = own_of(mods, ring)

    def line(stream, group):
        return mine[stream * 6 + group][None, :]

    qkv_w = jnp.transpose(qkv_weight[0], (0, 2, 1, 3))
    qkv_w = qkv_w.reshape(2, 3, n, feats, qkv_w.shape[-1])
    out_w = out_weight[0].reshape(2, n, feats, -1)
    up_w = up_weight[0].reshape(2, n, feats, -1)
    down_w = down_weight[0].reshape(2, n, feats, -1)
    qkv_b = qkv_bias[0].astype(F32)
    up_b = up_bias[0].astype(F32)
    out_b = out_bias[0].astype(F32)
    down_b = down_bias[0].astype(F32)

    db2 = [(line(segs[i][0], 5) * gs[i].astype(F32)).astype(BF16) for i in every]
    db2_sum = [jnp.sum(d.astype(F32), axis=0) for d in db2]
    db2_pieces = [ring.gather(db2[i], routes[i]) for i in every]

    ms, qkvs = [], []
    for i in every:
        stream = segs[i][0]
        m, q = qkv_call(base, x_pieces[i], mods, qkv_w, qkv_b[stream], stream)
        ms.append(m)
        qkvs.append(q)
    os, lses, x1, x1b, branch1, x1_pieces = [], [], [], [], [], []
    for i in every:
        stream = segs[i][0]
        o, lse = attn_fwd_call(base, qkvs, i)
        os.append(o)
        lses.append(lse)
        parts = ring.scatter(out_call(base, o, out_w, stream), routes[i])
        branch = sum(p.astype(F32) for p in parts) + out_b[stream]
        moved = xs[i].astype(F32) + line(stream, 2) * branch
        branch1.append(branch)
        x1.append(moved)
        x1b.append(moved.astype(BF16))
        x1_pieces.append(ring.gather(x1b[i], routes[i]))

    m2, act, du, du_sum, b2_parts, g1, do, lines2, db1_pieces = [], [], [], [], [], [], [], [], []
    for i in every:
        stream = segs[i][0]
        m, a, d, cols, sums, dub, b_part, dm_part = mlp_call(
            base, x1_pieces[i], db2_pieces[i], mods, up_w, up_b[stream][None], down_w, stream
        )
        m2.append(m)
        act.append(a)
        du.append(d)
        du_sum.append(dub[0])
        b2_parts.append(b_part)
        parts = ring.scatter(dm_part, routes[i])
        sums = ring.total(sums)
        g, db1, lines = norm_back_call(
            base, parts, x1b[i], cols, sums, gs[i], own, stream, width, 2, branch1[i]
        )
        g1.append(g)
        lines2.append(lines)
        pieces = ring.gather(db1, routes[i])
        db1_pieces.append(jnp.stack(pieces))
        do.append(do_call(base, pieces, out_w, stream))

    def stack_cot(i):
        return jnp.stack(db2_pieces[i])

    def reduce_weight(lefts, rights, name):
        part = wgrad_call(base, lefts, rights, dp, name)
        return lax.psum_scatter(part, "dp", scatter_dimension=0, tiled=True)[0].astype(F32)

    def of_stream(values, stream):
        return [values[i] for i in every if segs[i][0] == stream]

    cot_stack = [stack_cot(i) for i in every]
    up_grad = [reduce_weight(of_stream(m2, s), of_stream(du, s), f"dw_up{s}") for s in (0, 1)]
    down_grad = [
        reduce_weight(of_stream(cot_stack, s), of_stream(act, s), f"dw_down{s}") for s in (0, 1)
    ]
    out_grad = [
        reduce_weight(of_stream(db1_pieces, s), of_stream(os, s), f"dw_out{s}") for s in (0, 1)
    ]

    dqkv = attn_bwd_call(base, qkvs, os, do, lses)

    outs, gate2 = [], []
    for i in every:
        stream = segs[i][0]
        parts = ring.scatter(b2_parts[i], routes[i])
        branch = sum(p.astype(F32) for p in parts) + down_b[stream]
        outs.append(x1[i] + line(stream, 5) * branch)
        gate2.append(jnp.sum(branch * gs[i].astype(F32), axis=0))

    grads, lines1, qkv_sum = [], [], []
    for i in every:
        stream = segs[i][0]
        cols, sums, bias_sum, dm_part = dm_call(base, x_pieces[i], mods, dqkv[i], qkv_w, stream)
        qkv_sum.append(bias_sum)
        parts = ring.scatter(dm_part, routes[i])
        sums = ring.total(sums)
        g, lines = norm_back_call(base, parts, xs[i], cols, sums, g1[i], own, stream, width, 1)
        grads.append(g)
        lines1.append(lines)
    qkv_grad = [reduce_weight(of_stream(ms, s), of_stream(dqkv, s), f"dw_qkv{s}") for s in (0, 1)]

    def joined(values, stream):
        mine_ = of_stream(values, stream)
        return (mine_[0] if len(mine_) == 1 else jnp.concatenate(mine_, axis=0))[None]

    def summed(values, stream):
        return sum(of_stream(values, stream))

    rows = []
    for s in (0, 1):
        late, early = summed(lines1, s), summed(lines2, s)
        rows += [late[0], late[1], early[2], early[0], early[1], summed(gate2, s)]
    mod_grad = jnp.stack(rows).astype(BF16)
    all_mod = lax.all_gather(mod_grad, "dp", axis=0)
    mod_wgrad = jnp.einsum("sc,sgd->gcd", cond_act, all_mod, preferred_element_type=F32)
    mod_wgrad = jnp.transpose(mod_wgrad.reshape(1, 2, 6, -1, feats), (0, 1, 3, 2, 4))
    mod_bgrad = jnp.sum(all_mod.astype(F32), axis=0).reshape(1, 2, 6, feats)
    act_part = jnp.einsum("sgd,gcd->sc", all_mod, mod_w, preferred_element_type=F32)
    cond_grad = jax.vjp(jax.nn.silu, cond_float)[1](ring.total(act_part))[0]

    biases = lax.psum(
        (
            jnp.stack([summed(qkv_sum, s) for s in (0, 1)])[None],
            jnp.stack([summed(lines2, s)[3] for s in (0, 1)])[None],
            jnp.stack([summed(du_sum, s) for s in (0, 1)])[None],
            jnp.stack([summed(db2_sum, s) for s in (0, 1)])[None],
        ),
        "dp",
    )
    qkv_wgrad = jnp.transpose(jnp.stack(qkv_grad)[None], (0, 1, 3, 2, 4))
    return (
        joined(outs, 0),
        joined(outs, 1),
        joined(grads, 0),
        joined(grads, 1),
        cond_grad,
        mod_wgrad,
        mod_bgrad,
        qkv_wgrad,
        biases[0],
        jnp.stack(out_grad)[None],
        biases[1],
        jnp.stack(up_grad)[None],
        biases[2],
        jnp.stack(down_grad)[None],
        biases[3],
    )


def solution(mesh):
    dp, tensor = mesh.shape["dp"], mesh.shape["tensor"]
    return jax.shard_map(
        functools.partial(body, dp, tensor),
        mesh=mesh,
        in_specs=(
            P("dp", None, "tensor"),
            P("dp", None, "tensor"),
            P(None, "dp"),
            P(None, None, "dp", None, "tensor"),
            P(None, None, None, "tensor"),
            P(None, None, None, None, "tensor"),
            P(None, None, None, "tensor"),
            P(None, None, None, "tensor"),
            P(None, None, "tensor"),
            P(None, None, None, "tensor"),
            P(None, None, "tensor"),
            P(None, None, None, "tensor"),
            P(None, None, "tensor"),
            P("dp", None, "tensor"),
            P("dp", None, "tensor"),
        ),
        out_specs=(
            P("dp", None, "tensor"),
            P("dp", None, "tensor"),
            P("dp", None, "tensor"),
            P("dp", None, "tensor"),
            P(None, "dp"),
            P(None, None, "dp", None, "tensor"),
            P(None, None, None, "tensor"),
            P(None, None, "dp", None, "tensor"),
            P(None, None, None, "tensor"),
            P(None, None, "dp", "tensor"),
            P(None, None, "tensor"),
            P(None, None, "dp", "tensor"),
            P(None, None, "tensor"),
            P(None, None, "dp", "tensor"),
            P(None, None, "tensor"),
        ),
        check_vma=False,
    )
```

```python
import functools

import jax
import jax.numpy as jnp
from jax import lax
from jax.experimental import pallas as pl
from jax.experimental.pallas import tpu as pltpu
from jax.sharding import PartitionSpec as P

HEAD_DIM = 64
EPS = 1e-06
F32 = jnp.float32
BF16 = jnp.bfloat16
GELU_C = 0.7978845608028654
GELU_K = 0.044715
MIB = 1 << 20
MESH = pl.DeviceIdType.MESH
VMEM = pl.BlockSpec(memory_space=pltpu.VMEM)
ANY = pl.BlockSpec(memory_space=pl.ANY)


eps_norm = 1e-06


def gelu_tanh(values):
    return jax.nn.gelu(values, approximate=True)


def share_of(whole_row, offset, share_width):
    return lax.dynamic_slice_in_dim(whole_row, offset, share_width, whole_row.ndim - 1)


def norm_forward(shards, shifts, scales):
    saved_norm = []
    gathered = (
        lax.all_gather(shards[0].astype(jnp.bfloat16), "tensor", axis=2, tiled=True).astype(
            jnp.float32
        ),
        lax.all_gather(shards[1].astype(jnp.bfloat16), "tensor", axis=2, tiled=True).astype(
            jnp.float32
        ),
    )
    moddeds = []
    for stream in range(2):
        row_mean = jnp.mean(gathered[stream], axis=-1, keepdims=True)
        centred = gathered[stream] - row_mean
        inv_std = lax.rsqrt(jnp.mean(centred * centred, axis=-1, keepdims=True) + eps_norm)
        normed = centred * inv_std
        moddeds.append(
            (normed * (1.0 + scales[stream][:, None, :]) + shifts[stream][:, None, :]).astype(
                jnp.bfloat16
            )
        )
        saved_norm.append((normed, inv_std))
    return (moddeds, saved_norm)


def norm_backward(partials, saved_norm, scales, offset, share_width):
    results = []
    totals = (
        lax.psum(partials[0].astype(jnp.bfloat16), "tensor").astype(jnp.float32),
        lax.psum(partials[1].astype(jnp.bfloat16), "tensor").astype(jnp.float32),
    )
    for stream in range(2):
        normed, inv_std = saved_norm[stream]
        grad_normed = totals[stream] * (1.0 + scales[stream][:, None, :])
        mean_grad = jnp.mean(grad_normed, axis=-1, keepdims=True)
        mean_cross = jnp.mean(grad_normed * normed, axis=-1, keepdims=True)
        local_total = share_of(totals[stream], offset, share_width)
        local_normed = share_of(normed, offset, share_width)
        local_grad = share_of(grad_normed, offset, share_width)
        results.append(
            (
                inv_std * (local_grad - mean_grad - local_normed * mean_cross),
                jnp.sum(local_total, axis=1),
                jnp.sum(local_total * local_normed, axis=1),
            )
        )
    return results


def reduce_branches(partials):
    return (
        lax.psum_scatter(
            partials[0].astype(jnp.bfloat16), "tensor", scatter_dimension=2, tiled=True
        ).astype(jnp.float32),
        lax.psum_scatter(
            partials[1].astype(jnp.bfloat16), "tensor", scatter_dimension=2, tiled=True
        ).astype(jnp.float32),
    )


def gather_grads(branch_grads):
    return (
        lax.all_gather(branch_grads[0], "tensor", axis=2, tiled=True),
        lax.all_gather(branch_grads[1], "tensor", axis=2, tiled=True),
    )


def attend(joint_qkv, heads_here, score_scale):
    seq_count, tokens = (joint_qkv.shape[0], joint_qkv.shape[1])
    separated = joint_qkv.reshape(seq_count, tokens, 3, heads_here, HEAD_DIM)
    scores = (
        jnp.einsum(
            "sqhd,skhd->shqk",
            separated[:, :, 0],
            separated[:, :, 1],
            preferred_element_type=jnp.float32,
        )
        * score_scale
    )
    highest_score = jnp.max(scores, axis=-1, keepdims=True)
    raised = jnp.exp(scores - highest_score)
    denominator = jnp.sum(raised, axis=-1, keepdims=True)
    weights = (raised / denominator).astype(jnp.bfloat16)
    mixed_heads = jnp.einsum(
        "shqk,skhd->sqhd", weights, separated[:, :, 2], preferred_element_type=jnp.float32
    )
    return (
        mixed_heads.astype(jnp.bfloat16).reshape(seq_count, tokens, heads_here * HEAD_DIM),
        highest_score + jnp.log(denominator),
    )


def attend_back(joint_qkv, log_total, head_grads, heads_here, score_scale):
    seq_count, tokens = (joint_qkv.shape[0], joint_qkv.shape[1])
    separated = joint_qkv.reshape(seq_count, tokens, 3, heads_here, HEAD_DIM)
    queries, keys_all, values = (separated[:, :, 0], separated[:, :, 1], separated[:, :, 2])
    outgrad = head_grads.reshape(seq_count, tokens, heads_here, HEAD_DIM)
    scores = (
        jnp.einsum("sqhd,skhd->shqk", queries, keys_all, preferred_element_type=jnp.float32)
        * score_scale
    )
    weights = jnp.exp(scores - log_total)
    weight_grad = jnp.einsum("sqhd,skhd->shqk", outgrad, values, preferred_element_type=jnp.float32)
    row_dot = jnp.sum(weights * weight_grad, axis=-1, keepdims=True)
    score_grad = (weights * (weight_grad - row_dot)).astype(jnp.bfloat16)
    query_grad = (
        jnp.einsum("shqk,skhd->sqhd", score_grad, keys_all, preferred_element_type=jnp.float32)
        * score_scale
    )
    key_grad = (
        jnp.einsum("shqk,sqhd->skhd", score_grad, queries, preferred_element_type=jnp.float32)
        * score_scale
    )
    value_grad = jnp.einsum(
        "shqk,sqhd->skhd", weights.astype(jnp.bfloat16), outgrad, preferred_element_type=jnp.float32
    )
    stacked = jnp.stack([query_grad, key_grad, value_grad], axis=2)
    return stacked.reshape(seq_count, tokens, 3, heads_here * HEAD_DIM).astype(jnp.bfloat16)


def plain_body(
    image_in,
    text_in,
    cond_in,
    mod_weight,
    mod_bias,
    qkv_weight,
    qkv_bias,
    out_weight,
    out_bias,
    up_weight,
    up_bias,
    down_weight,
    down_bias,
    image_cot,
    text_cot,
):
    share_width = image_in.shape[2]
    offset = lax.axis_index("tensor") * share_width
    heads_here = qkv_weight.shape[4] // HEAD_DIM
    score_scale = HEAD_DIM ** (-0.5)
    image_rows = image_in.shape[1]
    layer_count = qkv_weight.shape[0]
    cond_float = cond_in.astype(jnp.float32)
    cond_act = jax.nn.silu(cond_float).astype(jnp.bfloat16)
    mod_terms = jnp.einsum(
        "sc,lxcjd->slxjd", cond_act, mod_weight, preferred_element_type=jnp.float32
    )
    modulation = lax.psum_scatter(
        mod_terms, "dp", scatter_dimension=0, tiled=True
    ) + mod_bias.astype(jnp.float32)
    mod_view = lax.all_gather(modulation, "tensor", axis=4, tiled=True)
    residual = [image_in.astype(jnp.float32), text_in.astype(jnp.float32)]
    layer_at = 0
    moddeds, first_norm = norm_forward(
        residual,
        [mod_view[:, layer_at, stream, 0] for stream in range(2)],
        [mod_view[:, layer_at, stream, 1] for stream in range(2)],
    )
    projected = [
        (
            jnp.einsum(
                "snd,dje->snje",
                moddeds[stream],
                qkv_weight[layer_at, stream],
                preferred_element_type=jnp.float32,
            )
            + qkv_bias[layer_at, stream]
        ).astype(jnp.bfloat16)
        for stream in range(2)
    ]
    joint_qkv = jnp.concatenate(projected, axis=1)
    attended, log_total = attend(joint_qkv, heads_here, score_scale)
    pieces = [attended[:, :image_rows], attended[:, image_rows:]]
    summed = reduce_branches(
        [
            jnp.einsum(
                "puj,oj->puo",
                pieces[stream],
                out_weight[layer_at, stream],
                preferred_element_type=jnp.float32,
            )
            for stream in range(2)
        ]
    )
    first_branch = [summed[stream] + out_bias[layer_at, stream] for stream in range(2)]
    residual = [
        residual[stream] + modulation[:, layer_at, stream, 2][:, None, :] * first_branch[stream]
        for stream in range(2)
    ]
    second_mod, second_norm = norm_forward(
        residual,
        [mod_view[:, layer_at, stream, 3] for stream in range(2)],
        [mod_view[:, layer_at, stream, 4] for stream in range(2)],
    )
    hidden = [
        jnp.einsum(
            "snd,df->snf",
            second_mod[stream],
            up_weight[layer_at, stream],
            preferred_element_type=jnp.float32,
        )
        + up_bias[layer_at, stream]
        for stream in range(2)
    ]
    activated = [gelu_tanh(hidden[stream]).astype(jnp.bfloat16) for stream in range(2)]
    summed = reduce_branches(
        [
            jnp.einsum(
                "snf,df->snd",
                activated[stream],
                down_weight[layer_at, stream],
                preferred_element_type=jnp.float32,
            )
            for stream in range(2)
        ]
    )
    second_branch = [summed[stream] + down_bias[layer_at, stream] for stream in range(2)]
    residual = [
        residual[stream] + modulation[:, layer_at, stream, 5][:, None, :] * second_branch[stream]
        for stream in range(2)
    ]
    forward_saved = [
        (
            moddeds,
            first_norm,
            joint_qkv,
            attended,
            log_total,
            first_branch,
            second_mod,
            second_norm,
            hidden,
            activated,
            second_branch,
        )
    ]
    gradients = [image_cot.astype(jnp.float32), text_cot.astype(jnp.float32)]
    mod_parts = [None] * layer_count
    weight_parts = [None] * layer_count
    bias_parts = [None] * layer_count
    for layer_at in reversed(range(layer_count)):
        (
            moddeds,
            first_norm,
            joint_qkv,
            attended,
            log_total,
            first_branch,
            second_mod,
            second_norm,
            hidden,
            activated,
            second_branch,
        ) = forward_saved[layer_at]
        second_gate = [
            jnp.sum(second_branch[stream] * gradients[stream], axis=1) for stream in range(2)
        ]
        branch_grads = [
            (modulation[:, layer_at, stream, 5][:, None, :] * gradients[stream]).astype(
                jnp.bfloat16
            )
            for stream in range(2)
        ]
        down_bias_grad = [
            jnp.sum(branch_grads[stream].astype(jnp.float32), axis=(0, 1)) for stream in range(2)
        ]
        whole_grads = gather_grads(branch_grads)
        down_grad = [
            jnp.einsum(
                "snd,snf->df",
                whole_grads[stream],
                activated[stream],
                preferred_element_type=jnp.float32,
            )
            for stream in range(2)
        ]
        act_grad = [
            jnp.einsum(
                "snd,df->snf",
                whole_grads[stream],
                down_weight[layer_at, stream],
                preferred_element_type=jnp.float32,
            )
            for stream in range(2)
        ]
        hidden_grad = [
            jax.vjp(gelu_tanh, hidden[stream])[1](act_grad[stream])[0].astype(jnp.bfloat16)
            for stream in range(2)
        ]
        up_bias_grad = [
            jnp.sum(hidden_grad[stream].astype(jnp.float32), axis=(0, 1)) for stream in range(2)
        ]
        up_grad = [
            jnp.einsum(
                "snd,snf->df",
                second_mod[stream],
                hidden_grad[stream],
                preferred_element_type=jnp.float32,
            )
            for stream in range(2)
        ]
        norm_partials = [
            jnp.einsum(
                "snf,df->snd",
                hidden_grad[stream],
                up_weight[layer_at, stream],
                preferred_element_type=jnp.float32,
            )
            for stream in range(2)
        ]
        second_back = norm_backward(
            norm_partials,
            second_norm,
            [mod_view[:, layer_at, stream, 4] for stream in range(2)],
            offset,
            share_width,
        )
        gradients = [gradients[stream] + second_back[stream][0] for stream in range(2)]
        first_gate = [
            jnp.sum(first_branch[stream] * gradients[stream], axis=1) for stream in range(2)
        ]
        branch_grads = [
            (modulation[:, layer_at, stream, 2][:, None, :] * gradients[stream]).astype(
                jnp.bfloat16
            )
            for stream in range(2)
        ]
        out_bias_grad = [
            jnp.sum(branch_grads[stream].astype(jnp.float32), axis=(0, 1)) for stream in range(2)
        ]
        whole_grads = gather_grads(branch_grads)
        pieces = [attended[:, :image_rows], attended[:, image_rows:]]
        out_grad = [
            jnp.einsum(
                "kux,kut->xt",
                whole_grads[stream],
                pieces[stream],
                preferred_element_type=jnp.float32,
            )
            for stream in range(2)
        ]
        head_grads = jnp.concatenate(
            [
                jnp.einsum(
                    "hom,mr->hor",
                    whole_grads[stream],
                    out_weight[layer_at, stream],
                    preferred_element_type=jnp.float32,
                )
                for stream in range(2)
            ],
            axis=1,
        ).astype(jnp.bfloat16)
        joint_grad = attend_back(joint_qkv, log_total, head_grads, heads_here, score_scale)
        stream_grads = [joint_grad[:, :image_rows], joint_grad[:, image_rows:]]
        qkv_bias_grad = [
            jnp.sum(stream_grads[stream].astype(jnp.float32), axis=(0, 1)) for stream in range(2)
        ]
        qkv_grad = [
            jnp.einsum(
                "snd,snje->dje",
                moddeds[stream],
                stream_grads[stream],
                preferred_element_type=jnp.float32,
            )
            for stream in range(2)
        ]
        norm_partials = [
            jnp.einsum(
                "snje,dje->snd",
                stream_grads[stream],
                qkv_weight[layer_at, stream],
                preferred_element_type=jnp.float32,
            )
            for stream in range(2)
        ]
        first_back = norm_backward(
            norm_partials,
            first_norm,
            [mod_view[:, layer_at, stream, 1] for stream in range(2)],
            offset,
            share_width,
        )
        gradients = [gradients[stream] + first_back[stream][0] for stream in range(2)]
        mod_parts[layer_at] = jnp.stack(
            [
                jnp.stack(
                    [
                        first_back[stream][1],
                        first_back[stream][2],
                        first_gate[stream],
                        second_back[stream][1],
                        second_back[stream][2],
                        second_gate[stream],
                    ],
                    axis=1,
                )
                for stream in range(2)
            ],
            axis=1,
        )
        bias_parts[layer_at] = (
            jnp.stack(qkv_bias_grad, axis=0),
            jnp.stack(out_bias_grad, axis=0),
            jnp.stack(up_bias_grad, axis=0),
            jnp.stack(down_bias_grad, axis=0),
        )
        weight_parts[layer_at] = (
            jnp.stack(qkv_grad, axis=0),
            jnp.stack(out_grad, axis=0),
            jnp.stack(up_grad, axis=0),
            jnp.stack(down_grad, axis=0),
        )
    reduced = (
        lax.psum_scatter(
            jnp.stack([weight_parts[0][0]], axis=0).astype(jnp.bfloat16),
            "dp",
            scatter_dimension=2,
            tiled=True,
        ).astype(jnp.float32),
        lax.psum_scatter(
            jnp.stack([weight_parts[0][1]], axis=0).astype(jnp.bfloat16),
            "dp",
            scatter_dimension=2,
            tiled=True,
        ).astype(jnp.float32),
        lax.psum_scatter(
            jnp.stack([weight_parts[0][2]], axis=0).astype(jnp.bfloat16),
            "dp",
            scatter_dimension=2,
            tiled=True,
        ).astype(jnp.float32),
        lax.psum_scatter(
            jnp.stack([weight_parts[0][3]], axis=0).astype(jnp.bfloat16),
            "dp",
            scatter_dimension=2,
            tiled=True,
        ).astype(jnp.float32),
    )
    bias_totals = lax.psum(
        (
            jnp.stack([bias_parts[0][0]], axis=0),
            jnp.stack([bias_parts[0][1]], axis=0),
            jnp.stack([bias_parts[0][2]], axis=0),
            jnp.stack([bias_parts[0][3]], axis=0),
        ),
        "dp",
    )
    mod_grad = jnp.stack(mod_parts, axis=1).astype(jnp.bfloat16)
    all_mod = lax.all_gather(mod_grad, "dp", axis=0, tiled=True)
    mod_wgrad = jnp.einsum("sc,slxjd->lxcjd", cond_act, all_mod, preferred_element_type=jnp.float32)
    mod_bgrad = jnp.sum(all_mod.astype(jnp.float32), axis=0)
    act_partial = jnp.einsum(
        "slxjd,lxcjd->sc", all_mod, mod_weight, preferred_element_type=jnp.float32
    )
    act_total = lax.psum(act_partial, "tensor")
    cond_grad = jax.vjp(jax.nn.silu, cond_float)[1](act_total)[0]
    return (
        residual[0],
        residual[1],
        gradients[0],
        gradients[1],
        cond_grad,
        mod_wgrad,
        mod_bgrad,
        reduced[0],
        bias_totals[0],
        reduced[1],
        bias_totals[1],
        reduced[2],
        bias_totals[2],
        reduced[3],
        bias_totals[3],
    )


def nt_dot(a, b):
    return lax.dot_general(a, b, (((1,), (1,)), ((), ())), preferred_element_type=F32)


def nn_dot(a, b):
    return lax.dot_general(a, b, (((1,), (0,)), ((), ())), preferred_element_type=F32)


def tn_dot(a, b):
    return lax.dot_general(a, b, (((0,), (0,)), ((), ())), preferred_element_type=F32)


def exact_nt(a, b):
    return lax.dot_general(
        a, b, (((1,), (1,)), ((), ())), preferred_element_type=F32, precision=lax.Precision.HIGHEST
    )


def exact_tn(a, b):
    return lax.dot_general(
        a, b, (((0,), (0,)), ((), ())), preferred_element_type=F32, precision=lax.Precision.HIGHEST
    )


def sds(shape, dtype):
    return jax.ShapeDtypeStruct(shape, dtype)


def cost(flops, arrays, outs):
    moved = sum(a.size * a.dtype.itemsize for a in arrays)
    moved += sum(o.size * o.dtype.itemsize for o in outs)
    return pl.CostEstimate(flops=flops, bytes_accessed=moved, transcendentals=0)


def eye_rows():
    return (
        lax.broadcasted_iota(jnp.int32, (8, 128), 0) == lax.broadcasted_iota(jnp.int32, (8, 128), 1)
    ).astype(F32)


def norm_stats(pieces, width):
    total = sum(jnp.sum(p, axis=-1, keepdims=True) for p in pieces)
    mean = total / width
    centred = [p - mean for p in pieces]
    var = sum(jnp.sum(c * c, axis=-1, keepdims=True) for c in centred) / width
    return mean, lax.rsqrt(var + EPS), centred


def stat_rows(first, second):
    lane = lax.broadcasted_iota(jnp.int32, (first.shape[0], 128), 1)
    both = jnp.where(lane == 0, first, jnp.where(lane == 1, second, 0.0))
    return exact_nt(eye_rows(), both)


def stat_cols(first, second):
    lane = lax.broadcasted_iota(jnp.int32, (first.shape[0], 128), 1)
    return jnp.where(lane == 0, first, jnp.where(lane == 1, second, 0.0))


class Links:
    def __init__(self, send, recv):
        self.send_sem, self.recv_sem = send, recv
        me = lax.axis_index("tensor")
        self.peers = [me, me + 1 - 2 * (me % 2), (me + 2) % 4, 3 - me]

    def enter(self, extra=()):
        barrier = pltpu.get_barrier_semaphore()
        for peer in self.peers[1:]:
            pl.semaphore_signal(barrier, inc=1, device_id={"tensor": peer}, device_id_type=MESH)
        for peer in extra:
            pl.semaphore_signal(barrier, inc=1, device_id={"dp": peer}, device_id_type=MESH)
        pl.semaphore_wait(barrier, 3 + len(extra))

    def copy(self, src, dst, kind, c, peer):
        return pltpu.make_async_remote_copy(
            src_ref=src,
            dst_ref=dst,
            send_sem=self.send_sem.at[kind, c],
            recv_sem=self.recv_sem.at[kind, c],
            device_id={"tensor": peer},
            device_id_type=MESH,
        )

    def route(self, c):
        odd = c % 2
        first = self.peers[1] * (1 - odd) + self.peers[2] * odd
        second = self.peers[2] * (1 - odd) + self.peers[1] * odd
        return 1 + odd, 2 - odd, first, second

    def gather_copy(self, i, src, buf, kind, c):
        near, far, first, second = self.route(c)
        if i == 0:
            return self.copy(src, buf.at[c, near], kind, c, first)
        if i == 1:
            return self.copy(src, buf.at[c, far], kind + 1, c, second)
        return self.copy(buf.at[c, near], buf.at[c, 3], kind + 2, c, second)

    def gather_start(self, *args):
        self.gather_copy(0, *args).start()
        self.gather_copy(1, *args).start()

    def gather_relay(self, *args):
        self.gather_copy(0, *args).wait_recv()
        self.gather_copy(2, *args).start()

    def gather_finish(self, *args):
        self.gather_copy(1, *args).wait_recv()
        self.gather_copy(2, *args).wait_recv()

    def gather_sent(self, *args):
        for i in range(3):
            self.gather_copy(i, *args).wait_send()

    def scatter_copy(self, i, part, relayed, got, kind, c):
        near, _, first, second = self.route(c)
        if i == 0:
            return self.copy(part.at[c, 3], got.at[c, 0], kind, c, first)
        if i == 1:
            return self.copy(part.at[c, near], got.at[c, 1], kind + 1, c, first)
        return self.copy(relayed.at[c], got.at[c, 2], kind + 2, c, second)

    def scatter_start(self, *args):
        self.scatter_copy(0, *args).start()
        self.scatter_copy(1, *args).start()

    def scatter_relay(self, part, relayed, got, kind, c):
        self.scatter_copy(0, part, relayed, got, kind, c).wait_recv()
        _, far, _, _ = self.route(c)
        relayed[c] = (part[c, far].astype(F32) + got[c, 0].astype(F32)).astype(BF16)
        self.scatter_copy(2, part, relayed, got, kind, c).start()

    def scatter_sent(self, *args):
        for i in range(3):
            self.scatter_copy(i, *args).wait_send()

    def scatter_finish(self, part, relayed, got, kind, c):
        self.scatter_copy(1, part, relayed, got, kind, c).wait_recv()
        self.scatter_copy(2, part, relayed, got, kind, c).wait_recv()
        return part[c, 0].astype(F32) + got[c, 1].astype(F32) + got[c, 2].astype(F32)

    def rows_copies(self, src, dst, kind, c):
        return [
            self.copy(src.at[c], dst.at[c, k - 1], kind + k - 1, c, self.peers[k]) for k in (1, 2, 3)
        ]

    def rows_start(self, src, dst, kind, c):
        for copy in self.rows_copies(src, dst, kind, c):
            copy.start()

    def rows_finish(self, src, dst, kind, c):
        for copy in self.rows_copies(src, dst, kind, c):
            copy.wait_recv()
        return src[c] + dst[c, 0] + dst[c, 1] + dst[c, 2]


def wait_sends(copies):
    for copy in copies:
        copy.wait_send()


def stages(count, steps):
    last = max(offset for offset, _ in steps)

    def tick(t, carry):
        for offset, step in steps:
            c = t - offset

            @pl.when((c >= 0) & (c < count))
            def _():
                step(c)

        return carry

    lax.fori_loop(0, count + last, tick, 0)


def front_kernel(dp, valid, refs_in, refs_out, scratch):
    x_ref, cot_ref, act_ref, modw_ref, modb_ref, wq_ref, bq_ref = refs_in
    m_ref, qkv_ref, o_ref, lse_ref, g_ref, xp_ref, mod_ref, gsum_ref = refs_out
    modw, wq, terms, got, k_all, aug, local, send, recv, msend, mrecv = scratch
    count, rows, feats = x_ref.shape
    cols = qkv_ref.shape[-1]
    width = 4 * feats
    links = Links(send, recv)
    mine = lax.axis_index("dp")
    others = [(mine + r) % dp for r in range(1, dp)]
    load_mod = pltpu.make_async_copy(modw_ref, modw, local.at[0])
    load_wq = pltpu.make_async_copy(wq_ref, wq, local.at[1])
    load_mod.start()
    load_wq.start()
    links.enter(others)
    for c in range(count):
        links.gather_start(x_ref.at[c], xp_ref, 0, c)
    load_mod.wait()
    act = act_ref[...]
    for j in range(12):
        terms[:, j, :] = nn_dot(act, modw[j])
    pushes = [
        pltpu.make_async_remote_copy(
            src_ref=terms.at[others[r]],
            dst_ref=got.at[r],
            send_sem=msend.at[r],
            recv_sem=mrecv.at[r],
            device_id={"dp": others[r]},
            device_id_type=MESH,
        )
        for r in range(dp - 1)
    ]
    for push in pushes:
        push.start()
    for c in range(count):
        xp_ref[c, 0] = x_ref[c]
    total = terms[mine] + modb_ref[...]
    for r, push in enumerate(pushes):
        push.wait_recv()
        total = total + got[r]
    mod_ref[0] = total
    mod_copies = [
        links.copy(mod_ref.at[0], mod_ref.at[k], 6, k, links.peers[k]) for k in (1, 2, 3)
    ]
    for copy in mod_copies:
        copy.start()
    for c in range(count):
        links.gather_relay(x_ref.at[c], xp_ref, 0, c)
    for c in range(count):
        stream = c // (count - 1)
        g = (total[stream * 6 + 5 : stream * 6 + 6, :] * cot_ref[c].astype(F32)).astype(BF16)
        g_ref[c, 0] = g
        gsum_ref[c : c + 1, :] = jnp.sum(g.astype(F32), axis=0, keepdims=True)
    for c in range(count):
        links.gather_start(g_ref.at[c, 0], g_ref, 3, c)
    for copy in mod_copies:
        copy.wait_recv()
    load_wq.wait()

    def project(c, carry):
        stream = c // (count - 1)
        links.gather_finish(x_ref.at[c], xp_ref, 0, c)
        _, inv, centred = norm_stats([xp_ref[c, k].astype(F32) for k in range(4)], width)
        acc = [None] * 3
        for k in range(4):
            shift = mod_ref[k, pl.ds(stream * 6, 1), :]
            scale = mod_ref[k, pl.ds(stream * 6 + 1, 1), :]
            m = (centred[k] * inv * (1.0 + scale) + shift).astype(BF16)
            m_ref[c, k] = m
            for j in range(3):
                part = nn_dot(m, wq[stream, j, links.peers[k]])
                acc[j] = part if k == 0 else acc[j] + part
        for j in range(3):
            qkv_ref[j, c] = (acc[j] + bq_ref[stream, j : j + 1, :]).astype(BF16)
        links.gather_relay(g_ref.at[c, 0], g_ref, 3, c)
        return carry

    lax.fori_loop(0, count, project, 0)

    owner = lax.broadcasted_iota(jnp.int32, (1, 128), 1) // HEAD_DIM

    def heads_pair(p, carry):
        lanes = pl.ds(pl.multiple_of(p * 128, 128), 128)
        for c in range(count):
            size = min(rows, valid - c * rows)
            sl = slice(c * rows, c * rows + size)
            k_all[sl, :] = qkv_ref[1, c, :size, lanes]
            values = qkv_ref[2, c, :size, lanes]
            for h in range(2):
                aug[h, sl, :] = jnp.where(owner == h, values, jnp.ones_like(values))

        def chunk(c, inner):
            q = qkv_ref[0, c, :, lanes] * jnp.asarray(HEAD_DIM**-0.5, BF16)
            out, lse = [], []
            for h in range(2):
                scores = nt_dot(jnp.where(owner == h, q, jnp.zeros_like(q)), k_all[...])
                top = jnp.max(scores, axis=-1, keepdims=True)
                acc = nn_dot(jnp.exp(scores - top).astype(BF16), aug[h])
                other = (1 - h) * HEAD_DIM
                denom = acc[:, other : other + 1]
                out.append(acc / denom)
                lse.append(top + jnp.log(denom))
            o_ref[c, :, lanes] = jnp.where(owner == 0, out[0], out[1]).astype(BF16)
            lse_ref[c, :, lanes] = jnp.where(owner == 0, lse[0], lse[1])
            return inner

        lax.fori_loop(0, count, chunk, 0)
        return carry

    lax.fori_loop(0, cols // 128, heads_pair, 0)
    for c in range(count):
        links.gather_finish(g_ref.at[c, 0], g_ref, 3, c)
        links.gather_sent(x_ref.at[c], xp_ref, 0, c)
        links.gather_sent(g_ref.at[c, 0], g_ref, 3, c)
    wait_sends(mod_copies)
    wait_sends(pushes)


def front_call(dp, valid, x, cot, act, mod_w, mod_b, wq, bq):
    count, rows, feats = x.shape
    cols = wq.shape[-1]
    arrays = [x, cot, act, mod_w, mod_b, wq, bq]
    outs = [
        sds((count, 4, rows, feats), BF16),
        sds((3, count, rows, cols), BF16),
        sds((count, rows, cols), BF16),
        sds((count, rows, cols), F32),
        sds((count, 4, rows, feats), BF16),
        sds((count, 4, rows, feats), BF16),
        sds((4, 12, feats), F32),
        sds((count, feats), F32),
    ]
    n_in, n_out = len(arrays), len(outs)

    def kernel(*refs):
        front_kernel(dp, valid, refs[:n_in], refs[n_in : n_in + n_out], refs[n_in + n_out :])

    return pl.pallas_call(
        kernel,
        out_shape=outs,
        in_specs=[VMEM, VMEM, VMEM, ANY, VMEM, ANY, VMEM],
        out_specs=[VMEM] * n_out,
        scratch_shapes=[
            pltpu.VMEM(mod_w.shape, BF16),
            pltpu.VMEM(wq.shape, BF16),
            pltpu.VMEM((dp, 12, feats), F32),
            pltpu.VMEM((dp - 1, 12, feats), F32),
            pltpu.VMEM((valid, 128), BF16),
            pltpu.VMEM((2, valid, 128), BF16),
            pltpu.SemaphoreType.DMA((2,)),
            pltpu.SemaphoreType.DMA((7, count)),
            pltpu.SemaphoreType.DMA((7, count)),
            pltpu.SemaphoreType.DMA((dp - 1,)),
            pltpu.SemaphoreType.DMA((dp - 1,)),
        ],
        compiler_params=pltpu.CompilerParams(
            collective_id=1, has_side_effects=True, vmem_limit_bytes=56 * MIB
        ),
        cost_estimate=cost(20 * 10**9, arrays, outs),
        name="front",
    )(*arrays)


HB = 512


def middle_kernel(refs_in, refs_out, scratch):
    o_ref, x_ref, cot_ref, db2_ref, mod_ref, wo_ref, up_ref, down_ref, ub_ref, ob_ref = refs_in
    x1_out, m2_out, a_out, du_out, b2_out, g1_out, g_ref, do_ref, line_ref, dub_ref = refs_out
    (wo, up, down, db2, part, relayed, got, xp, branch, acc_m, acc_b, cols_s) = scratch[:12]
    (x1_s, m2_s, a_s, du_s, b2_s, g1_s, srow, sgot, local, out_sem, send, recv) = scratch[12:]
    count, _, feats = x_ref.shape
    width = 4 * feats
    hidden = up.shape[-1]
    links = Links(send, recv)
    loads = [
        pltpu.make_async_copy(src, dst, local.at[i])
        for i, (src, dst) in enumerate(
            [(wo_ref, wo), (up_ref, up), (down_ref, down), (db2_ref, db2)]
        )
    ]
    for load in loads:
        load.start()
    links.enter()
    loads[0].wait()

    def flush(staged, out, kind, c):
        return pltpu.make_async_copy(staged.at[c % 2], out.at[c], out_sem.at[kind, c % 2])

    def project(c):
        stream = c // (count - 1)
        o = o_ref[c]
        for k in (3, 1, 2, 0):
            part[c, k] = nt_dot(o, wo[stream, links.peers[k]]).astype(BF16)
        links.scatter_start(part, relayed, got, 0, c)

    def first_relay(c):
        links.scatter_relay(part, relayed, got, 0, c)

    def residual(c):
        stream = c // (count - 1)
        total = links.scatter_finish(part, relayed, got, 0, c)
        add = total + ob_ref[pl.ds(stream, 1), :]
        branch[c] = add
        moved = x_ref[c].astype(F32) + mod_ref[0, pl.ds(stream * 6 + 2, 1), :] * add

        @pl.when(c >= 2)
        def _():
            flush(x1_s, x1_out, 0, c - 2).wait()

        x1_s[c % 2] = moved
        flush(x1_s, x1_out, 0, c).start()
        xp[c, 0] = moved.astype(BF16)
        links.gather_start(xp.at[c, 0], xp, 3, c)

    def second_relay(c):
        links.gather_relay(xp.at[c, 0], xp, 3, c)

    def feed_forward(c):
        stream = c // (count - 1)
        slot = c % 2

        @pl.when(c == 0)
        def _():
            for load in loads[1:]:
                load.wait()

        @pl.when(c >= 2)
        def _():
            for kind, (staged, out) in enumerate(
                [(m2_s, m2_out), (a_s, a_out), (du_s, du_out), (b2_s, b2_out)]
            ):
                flush(staged, out, kind + 1, c - 2).wait()

        links.gather_finish(xp.at[c, 0], xp, 3, c)
        links.scatter_sent(part, relayed, got, 0, c)
        mean, inv, centred = norm_stats([xp[c, k].astype(F32) for k in range(4)], width)
        for k in range(4):
            shift = mod_ref[k, pl.ds(stream * 6 + 3, 1), :]
            scale = mod_ref[k, pl.ds(stream * 6 + 4, 1), :]
            m2_s[slot, k] = (centred[k] * inv * (1.0 + scale) + shift).astype(BF16)

        def block(b, carry):
            cols = pl.ds(pl.multiple_of(b * HB, HB), HB)
            u = ub_ref[pl.ds(stream, 1), cols]
            for k in range(4):
                u = u + nn_dot(m2_s[slot, k], up[stream, links.peers[k], :, cols])
            da = None
            for k in range(4):
                piece = nn_dot(db2[c, k], down[stream, links.peers[k], :, cols])
                da = piece if da is None else da + piece
            square = u * u
            th = jnp.tanh(u * (GELU_C + (GELU_C * GELU_K) * square))
            up_half = 0.5 + 0.5 * th
            a = (u * up_half).astype(BF16)
            slope = up_half * (
                1.0 + u * (1.0 - th) * (GELU_C + (3.0 * GELU_C * GELU_K) * square)
            )
            du = (da * slope).astype(BF16)
            a_s[slot, :, cols] = a
            du_s[slot, :, cols] = du
            dub_ref[pl.ds(c, 1), cols] = jnp.sum(du.astype(F32), axis=0, keepdims=True)
            for k in range(4):
                dm = nt_dot(du, up[stream, links.peers[k], :, cols])
                bb = nt_dot(a, down[stream, links.peers[k], :, cols])

                @pl.when(b == 0)
                def _():
                    acc_m[k] = dm
                    acc_b[k] = bb

                @pl.when(b != 0)
                def _():
                    acc_m[k] += dm
                    acc_b[k] += bb

            return carry

        lax.fori_loop(0, hidden // HB, block, 0)
        first = second = None
        for k in range(4):
            dm = acc_m[k]
            part[c, k] = dm.astype(BF16)
            dh = dm * (1.0 + mod_ref[k, pl.ds(stream * 6 + 4, 1), :])
            one = jnp.sum(dh, axis=-1, keepdims=True)
            two = jnp.sum(dh * (xp[c, k].astype(F32) - mean), axis=-1, keepdims=True)
            first = one if first is None else first + one
            second = two if second is None else second + two
        srow[c] = stat_rows(first, second * inv)
        links.scatter_start(part, relayed, got, 6, c)
        links.rows_start(srow, sgot, 12, c)
        cols_s[c] = stat_cols(mean, inv)
        for k in range(4):
            b2_s[slot, k] = acc_b[k].astype(BF16)
        for kind, (staged, out) in enumerate(
            [(m2_s, m2_out), (a_s, a_out), (du_s, du_out), (b2_s, b2_out)]
        ):
            flush(staged, out, kind + 1, c).start()

    def third_relay(c):
        links.scatter_relay(part, relayed, got, 6, c)

    def norm_back(c):
        stream = c // (count - 1)
        total = links.scatter_finish(part, relayed, got, 6, c)
        sums = exact_tn(links.rows_finish(srow, sgot, 12, c), eye_rows())
        mean, inv = cols_s[c, :, 0:1], cols_s[c, :, 1:2]
        normed = (xp[c, 0].astype(F32) - mean) * inv
        grad = total * (1.0 + mod_ref[0, pl.ds(stream * 6 + 4, 1), :])
        g = cot_ref[c].astype(F32) + inv * (
            grad - sums[:, 0:1] / width - normed * (sums[:, 1:2] / width)
        )
        db = (mod_ref[0, pl.ds(stream * 6 + 2, 1), :] * g).astype(BF16)
        g_ref[c, 0] = db
        links.gather_start(g_ref.at[c, 0], g_ref, 9, c)

        @pl.when(c >= 2)
        def _():
            flush(g1_s, g1_out, 5, c - 2).wait()

        g1_s[c % 2] = g
        flush(g1_s, g1_out, 5, c).start()
        line_ref[c, 0:1, :] = jnp.sum(total, axis=0, keepdims=True)
        line_ref[c, 1:2, :] = jnp.sum(total * normed, axis=0, keepdims=True)
        line_ref[c, 2:3, :] = jnp.sum(branch[c] * g, axis=0, keepdims=True)
        line_ref[c, 3:4, :] = jnp.sum(db.astype(F32), axis=0, keepdims=True)

    def fourth_relay(c):
        links.gather_relay(g_ref.at[c, 0], g_ref, 9, c)

    def head_grads(c):
        stream = c // (count - 1)
        links.gather_finish(g_ref.at[c, 0], g_ref, 9, c)
        acc = None
        for k in range(4):
            piece = nn_dot(g_ref[c, k], wo[stream, links.peers[k]])
            acc = piece if acc is None else acc + piece
        do_ref[c] = acc.astype(BF16)

    stages(
        count,
        [
            (7, fourth_relay),
            (5, third_relay),
            (3, second_relay),
            (1, first_relay),
            (6, norm_back),
            (2, residual),
            (0, project),
            (8, head_grads),
            (4, feed_forward),
        ],
    )
    for c in range(count):
        links.gather_sent(xp.at[c, 0], xp, 3, c)
        links.scatter_sent(part, relayed, got, 6, c)
        links.gather_sent(g_ref.at[c, 0], g_ref, 9, c)
        wait_sends(links.rows_copies(srow, sgot, 12, c))
    for c in (count - 2, count - 1):
        for kind, (staged, out) in enumerate(
            [
                (x1_s, x1_out),
                (m2_s, m2_out),
                (a_s, a_out),
                (du_s, du_out),
                (b2_s, b2_out),
                (g1_s, g1_out),
            ]
        ):
            flush(staged, out, kind, c).wait()


def middle_call(o, x, cot, db2, mods, wo, up, down, ub, ob):
    count, rows, feats = x.shape
    cols, hidden = wo.shape[-1], up.shape[-1]
    arrays = [o, x, cot, db2, mods, wo, up, down, ub, ob]
    outs = [
        sds((count, rows, feats), F32),
        sds((count, 4, rows, feats), BF16),
        sds((count, rows, hidden), BF16),
        sds((count, rows, hidden), BF16),
        sds((count, 4, rows, feats), BF16),
        sds((count, rows, feats), F32),
        sds((count, 4, rows, feats), BF16),
        sds((count, rows, cols), BF16),
        sds((count, 4, feats), F32),
        sds((count, hidden), F32),
    ]
    n_in, n_out = len(arrays), len(outs)

    def kernel(*refs):
        middle_kernel(refs[:n_in], refs[n_in : n_in + n_out], refs[n_in + n_out :])

    return pl.pallas_call(
        kernel,
        out_shape=outs,
        in_specs=[VMEM, VMEM, VMEM, ANY, VMEM, ANY, ANY, ANY, VMEM, VMEM],
        out_specs=[ANY] * 6 + [VMEM] * 4,
        scratch_shapes=[
            pltpu.VMEM(wo.shape, BF16),
            pltpu.VMEM(up.shape, BF16),
            pltpu.VMEM(down.shape, BF16),
            pltpu.VMEM(db2.shape, BF16),
            pltpu.VMEM((count, 4, rows, feats), BF16),
            pltpu.VMEM((count, rows, feats), BF16),
            pltpu.VMEM((count, 3, rows, feats), BF16),
            pltpu.VMEM((count, 4, rows, feats), BF16),
            pltpu.VMEM((count, rows, feats), F32),
            pltpu.VMEM((4, rows, feats), F32),
            pltpu.VMEM((4, rows, feats), F32),
            pltpu.VMEM((count, rows, 128), F32),
            pltpu.VMEM((2, rows, feats), F32),
            pltpu.VMEM((2, 4, rows, feats), BF16),
            pltpu.VMEM((2, rows, hidden), BF16),
            pltpu.VMEM((2, rows, hidden), BF16),
            pltpu.VMEM((2, 4, rows, feats), BF16),
            pltpu.VMEM((2, rows, feats), F32),
            pltpu.VMEM((count, 8, rows), F32),
            pltpu.VMEM((count, 3, 8, rows), F32),
            pltpu.SemaphoreType.DMA((4,)),
            pltpu.SemaphoreType.DMA((6, 2)),
            pltpu.SemaphoreType.DMA((15, count)),
            pltpu.SemaphoreType.DMA((15, count)),
        ],
        compiler_params=pltpu.CompilerParams(
            collective_id=2, has_side_effects=True, vmem_limit_bytes=63 * MIB
        ),
        cost_estimate=cost(30 * 10**9, arrays, outs),
        name="middle",
    )(*arrays)


def back_kernel(valid, blocks, refs_in, refs_out, scratch):
    qkv_ref, o_ref, do_ref, lse_ref, b2_ref, x1_ref, cot_ref, g1_ref, xp_ref, mod_ref = refs_in[:10]
    wq_ref, db_ref = refs_in[10:]
    dqkv_ref, x2_ref, grad_ref, line_ref, bias_ref = refs_out
    wq, q_all, k_all, v_all, do_all, lse_all, od_all, dk_all, dv_all, dqt_all, dq_all = scratch[:11]
    part, relayed, got, relayed2, got2, cols_s, srow, sgot, local, send, recv = scratch[11:]
    count, rows, feats = cot_ref.shape
    cols = o_ref.shape[-1]
    width = 4 * feats
    links = Links(send, recv)
    load = pltpu.make_async_copy(wq_ref, wq, local.at[0])
    load.start()
    links.enter()
    for c in range(count):
        links.scatter_start(b2_ref, relayed2, got2, 0, c)
    scale = jnp.asarray(HEAD_DIM**-0.5, BF16)
    head_row = lax.broadcasted_iota(jnp.int32, (8, 128), 0)
    lane = lax.broadcasted_iota(jnp.int32, (8, 128), 1)
    first_lane = (lane == head_row * HEAD_DIM).astype(F32)
    within = (lane // HEAD_DIM == head_row).astype(F32)
    owner = lax.broadcasted_iota(jnp.int32, (1, 128), 1) // HEAD_DIM
    zero = jnp.zeros((), BF16)
    for c in range(count):
        size = min(rows, valid - c * rows)
        if size < rows:
            for j in range(3):
                dqkv_ref[j, c] = jnp.zeros((rows, cols), BF16)

    def heads_pair(p, carry):
        lanes = pl.ds(pl.multiple_of(p * 128, 128), 128)
        for c in range(count):
            size = min(rows, valid - c * rows)
            sl = slice(c * rows, c * rows + size)
            q_all[sl, :] = qkv_ref[0, c, :size, lanes] * scale
            k_all[sl, :] = qkv_ref[1, c, :size, lanes]
            v_all[sl, :] = qkv_ref[2, c, :size, lanes]
            do = do_ref[c, :size, lanes]
            do_all[sl, :] = do
            lse_all[sl, :] = lse_ref[c, :size, lanes]
            od_all[sl, :] = o_ref[c, :size, lanes].astype(F32) * do.astype(F32)
        lse_rows = exact_nt(first_lane, lse_all[...])
        dot_rows = exact_nt(within, od_all[...])
        dqt = None
        for h in range(2):
            mine = owner == h
            q = jnp.where(mine, q_all[...], zero)
            do = jnp.where(mine, do_all[...], zero)
            lse_row, dot_row = lse_rows[h : h + 1, :], dot_rows[h : h + 1, :]
            for start, size in blocks:
                sl = slice(start, start + size)
                keys, values = k_all[sl, :], v_all[sl, :]
                weights = jnp.exp(nt_dot(keys, q) - lse_row)
                grads = (weights * (nt_dot(values, do) - dot_row)).astype(BF16)
                dv = nn_dot(weights.astype(BF16), do)
                dk = nn_dot(grads, q)
                if h == 0:
                    dv_all[sl, :] = dv
                    dk_all[sl, :] = dk
                else:
                    dv_all[sl, :] += dv
                    dk_all[sl, :] += dk
                piece = tn_dot(jnp.where(mine, keys, zero) * scale, grads)
                dqt = piece if dqt is None else dqt + piece
        dqt_all[:, :valid] = dqt
        dq_all[...] = dqt_all[...].T
        for c in range(count):
            size = min(rows, valid - c * rows)
            sl = slice(c * rows, c * rows + size)
            dqkv_ref[0, c, :size, lanes] = dq_all[sl, :].astype(BF16)
            dqkv_ref[1, c, :size, lanes] = dk_all[sl, :].astype(BF16)
            dqkv_ref[2, c, :size, lanes] = dv_all[sl, :].astype(BF16)

        @pl.when(p == 0)
        def _():
            for c in range(count):
                links.scatter_relay(b2_ref, relayed2, got2, 0, c)

        return carry

    lax.fori_loop(0, cols // 128, heads_pair, 0)
    load.wait()

    def input_grads(c):
        stream = c // (count - 1)
        mean, inv, centred = norm_stats([xp_ref[c, k].astype(F32) for k in range(4)], width)
        first = second = None
        for k in (3, 1, 2, 0):
            dm = None
            for j in range(3):
                piece = nt_dot(dqkv_ref[j, c], wq[stream, j, links.peers[k]])
                dm = piece if dm is None else dm + piece
            part[c, k] = dm.astype(BF16)
            dh = dm * (1.0 + mod_ref[k, pl.ds(stream * 6 + 1, 1), :])
            one = jnp.sum(dh, axis=-1, keepdims=True)
            two = jnp.sum(dh * centred[k], axis=-1, keepdims=True)
            first = one if first is None else first + one
            second = two if second is None else second + two
        srow[c] = stat_rows(first, second * inv)
        links.scatter_start(part, relayed, got, 3, c)
        links.rows_start(srow, sgot, 6, c)
        cols_s[c] = stat_cols(mean, inv)
        for j in range(3):
            bias_ref[c, j : j + 1, :] = jnp.sum(
                dqkv_ref[j, c].astype(F32), axis=0, keepdims=True
            )

    def last_relay(c):
        links.scatter_relay(part, relayed, got, 3, c)

    def out_stream(c):
        stream = c // (count - 1)
        total = links.scatter_finish(b2_ref, relayed2, got2, 0, c)
        add = total + db_ref[pl.ds(stream, 1), :]
        x2_ref[c] = x1_ref[c] + mod_ref[0, pl.ds(stream * 6 + 5, 1), :] * add
        line_ref[c, 2:3, :] = jnp.sum(add * cot_ref[c].astype(F32), axis=0, keepdims=True)

    def norm_back(c):
        stream = c // (count - 1)
        total = links.scatter_finish(part, relayed, got, 3, c)
        sums = exact_tn(links.rows_finish(srow, sgot, 6, c), eye_rows())
        mean, inv = cols_s[c, :, 0:1], cols_s[c, :, 1:2]
        normed = (xp_ref[c, 0].astype(F32) - mean) * inv
        grad = total * (1.0 + mod_ref[0, pl.ds(stream * 6 + 1, 1), :])
        grad_ref[c] = g1_ref[c] + inv * (
            grad - sums[:, 0:1] / width - normed * (sums[:, 1:2] / width)
        )
        line_ref[c, 0:1, :] = jnp.sum(total, axis=0, keepdims=True)
        line_ref[c, 1:2, :] = jnp.sum(total * normed, axis=0, keepdims=True)

    stages(count, [(1, last_relay), (0, input_grads), (2, norm_back), (1, out_stream)])
    for c in range(count):
        links.scatter_sent(b2_ref, relayed2, got2, 0, c)
        links.scatter_sent(part, relayed, got, 3, c)
        wait_sends(links.rows_copies(srow, sgot, 6, c))


def back_call(valid, qkv, o, do, lse, b2, x1, cot, g1, xp, mods, wq, down_b):
    count, rows, feats = cot.shape
    cols = o.shape[-1]
    padded = -(-valid // 128) * 128
    step = -(-valid // 3 // 16) * 16
    blocks = [(b, min(step, valid - b)) for b in range(0, valid, step)]
    arrays = [qkv, o, do, lse, b2, x1, cot, g1, xp, mods, wq, down_b]
    outs = [
        sds(qkv.shape, BF16),
        sds((count, rows, feats), F32),
        sds((count, rows, feats), F32),
        sds((count, 3, feats), F32),
        sds((count, 3, cols), F32),
    ]
    n_in, n_out = len(arrays), len(outs)

    def kernel(*refs):
        back_kernel(valid, blocks, refs[:n_in], refs[n_in : n_in + n_out], refs[n_in + n_out :])

    return pl.pallas_call(
        kernel,
        out_shape=outs,
        in_specs=[VMEM] * 10 + [ANY, VMEM],
        out_specs=[VMEM] * n_out,
        scratch_shapes=[pltpu.VMEM(wq.shape, BF16)]
        + [pltpu.VMEM((valid, 128), BF16)] * 4
        + [pltpu.VMEM((valid, 128), F32)] * 4
        + [
            pltpu.VMEM((128, padded), F32),
            pltpu.VMEM((padded, 128), F32),
            pltpu.VMEM((count, 4, rows, feats), BF16),
            pltpu.VMEM((count, rows, feats), BF16),
            pltpu.VMEM((count, 3, rows, feats), BF16),
            pltpu.VMEM((count, rows, feats), BF16),
            pltpu.VMEM((count, 3, rows, feats), BF16),
            pltpu.VMEM((count, rows, 128), F32),
            pltpu.VMEM((count, 8, rows), F32),
            pltpu.VMEM((count, 3, 8, rows), F32),
            pltpu.SemaphoreType.DMA((1,)),
            pltpu.SemaphoreType.DMA((9, count)),
            pltpu.SemaphoreType.DMA((9, count)),
        ],
        compiler_params=pltpu.CompilerParams(
            collective_id=3, has_side_effects=True, vmem_limit_bytes=63 * MIB
        ),
        cost_estimate=cost(40 * 10**9, arrays, outs),
        name="back",
    )(*arrays)


def flat(value):
    return value.reshape((-1,) + value.shape[-1:])


def wgrad_kernel(pairs, split, t_ref, *refs):
    out_ref = refs[-1]
    slot = 0
    at = 0
    for groups in pairs:
        left, right = flat(refs[at][:, 0]), refs[at + 1]
        at += 2
        for j in range(groups):
            acc = tn_dot(left, flat(right[j] if groups > 1 else right[...]))
            size = acc.shape[0] // split
            for p in range(split):
                out_ref[p, slot] = acc[p * size : (p + 1) * size].astype(BF16)
            slot += 1


def wgrad_call(base, pairs, into, stream, dp):
    count, _, rows, feats = pairs[0][0].shape
    chunks = 1 if stream else count - 1
    first = (count - 1) if stream else 0
    cols = pairs[0][1].shape[-1]
    split = dp // 4
    groups = [right.shape[0] if right.ndim == 4 else 1 for _, right in pairs]
    slots = sum(groups)
    arrays, specs = [], []
    for (left, right), g in zip(pairs, groups):
        arrays += [left, right]
        specs.append(
            pl.BlockSpec((chunks, 1, rows, feats), lambda k, t: (first // chunks, k, 0, 0))
        )
        if g > 1:
            specs.append(
                pl.BlockSpec((g, chunks, rows, cols), lambda k, t: (0, first // chunks, 0, 0))
            )
        else:
            specs.append(pl.BlockSpec((chunks, rows, cols), lambda k, t: (first // chunks, 0, 0)))
    out = sds((dp, 2 * slots, feats // split, cols), BF16)
    aliases = {}
    if into is not None:
        aliases = {1 + len(arrays): 0}
        arrays.append(into)
        specs.append(ANY)

    def kernel(*refs):
        wgrad_kernel(groups, split, *refs)

    return pl.pallas_call(
        kernel,
        out_shape=[out],
        grid_spec=pltpu.PrefetchScalarGridSpec(
            num_scalar_prefetch=1,
            grid=(4,),
            in_specs=specs,
            out_specs=[
                pl.BlockSpec(
                    (split, slots, feats // split, cols), lambda k, t: (t[0] ^ k, stream, 0, 0)
                )
            ],
        ),
        input_output_aliases=aliases,
        compiler_params=pltpu.CompilerParams(
            dimension_semantics=("arbitrary",), vmem_limit_bytes=48 * MIB
        ),
        cost_estimate=cost(2 * 4 * feats * slots * cols * chunks * rows, arrays, [out]),
    )(base, *arrays)[0]


def fast_body(
    dp,
    image_in,
    text_in,
    cond_in,
    mod_weight,
    mod_bias,
    qkv_weight,
    qkv_bias,
    out_weight,
    out_bias,
    up_weight,
    up_bias,
    down_weight,
    down_bias,
    image_cot,
    text_cot,
):
    base = lax.axis_index("tensor").astype(jnp.int32).reshape(1)
    feats = image_in.shape[2]
    images, texts = image_in.shape[1], text_in.shape[1]
    rows = images // 4
    valid = images + texts

    def join(image, text):
        padded = jnp.pad(text[0], ((0, rows - texts), (0, 0)))
        return jnp.concatenate([image[0].reshape(4, rows, feats), padded[None]], axis=0)

    def parted(value):
        image = value[:4].reshape(1, images, feats)
        return image, value[4:, :texts]

    x, cot = join(image_in, text_in), join(image_cot, text_cot)
    cond_float = cond_in.astype(F32)
    cond_act = jax.nn.silu(cond_float).astype(BF16)
    mod_w = jnp.transpose(mod_weight[0], (0, 2, 1, 3)).reshape(12, -1, feats)
    mod_b = mod_bias[0].reshape(12, feats).astype(F32)
    qkv_w = jnp.transpose(qkv_weight[0], (0, 2, 1, 3))
    qkv_w = qkv_w.reshape(2, 3, 4, feats, qkv_w.shape[-1])
    out_w = out_weight[0].reshape(2, 4, feats, -1)
    up_w = up_weight[0].reshape(2, 4, feats, -1)
    down_w = down_weight[0].reshape(2, 4, feats, -1)

    m, qkv, o, lse, db2, xp, mods, db2_sum = front_call(
        dp, valid, x, cot, cond_act, mod_w, mod_b, qkv_w, qkv_bias[0].astype(F32)
    )
    x1, m2, act, du, b2, g1, db1, do, lines2, du_sum = middle_call(
        o, x, cot, db2, mods, out_w, up_w, down_w, up_bias[0].astype(F32), out_bias[0].astype(F32)
    )
    part = wgrad_call(base, [(m2, du), (db2, act)], None, 0, dp)
    part = wgrad_call(base, [(m2, du), (db2, act)], part, 1, dp)
    do, part = lax.optimization_barrier((do, part))
    ff_sum = lax.psum_scatter(part, "dp", scatter_dimension=0, tiled=True)
    ff_grad = ff_sum[0].astype(F32)
    dqkv, x2, grad, lines1, qkv_sum = back_call(
        valid, qkv, o, do, lse, b2, x1, cot, g1, xp, mods, qkv_w, down_bias[0].astype(F32)
    )
    part2 = wgrad_call(base, [(m, dqkv), (db1, o)], None, 0, dp)
    part2 = wgrad_call(base, [(m, dqkv), (db1, o)], part2, 1, dp)
    at_sum = lax.psum_scatter(part2, "dp", scatter_dimension=0, tiled=True)
    at_grad = at_sum[0].astype(F32)

    def by_stream(value):
        return jnp.stack([jnp.sum(value[:4], axis=0), value[4]])

    late, early = by_stream(lines1), by_stream(lines2)
    mod_rows = jnp.stack(
        [late[:, 0], late[:, 1], early[:, 2], early[:, 0], early[:, 1], late[:, 2]], axis=1
    )
    mod_grad = mod_rows.reshape(12, feats).astype(BF16)
    all_mod = lax.all_gather(mod_grad, "dp", axis=0)
    mod_wgrad = jnp.einsum("sc,sgd->gcd", cond_act, all_mod, preferred_element_type=F32)
    mod_wgrad = jnp.transpose(mod_wgrad.reshape(1, 2, 6, -1, feats), (0, 1, 3, 2, 4))
    mod_bgrad = jnp.sum(all_mod.astype(F32), axis=0).reshape(1, 2, 6, feats)
    act_part = jnp.einsum("sgd,gcd->sc", all_mod, mod_w, preferred_element_type=F32)
    act_total = act_part + sum(
        lax.ppermute(act_part, "tensor", [(i, i ^ k) for i in range(4)]) for k in (1, 2, 3)
    )
    cond_grad = jax.vjp(jax.nn.silu, cond_float)[1](act_total)[0]
    biases = lax.psum(
        (
            by_stream(qkv_sum)[None],
            early[None, :, 3],
            by_stream(du_sum)[None],
            by_stream(db2_sum)[None],
        ),
        "dp",
    )
    at_grad = at_grad.reshape((2, 4) + at_grad.shape[1:])
    ff_grad = ff_grad.reshape((2, 2) + ff_grad.shape[1:])
    qkv_wgrad = jnp.transpose(at_grad[None, :, :3], (0, 1, 3, 2, 4))
    image_out, text_out = parted(x2)
    image_grad, text_grad = parted(grad)
    return (
        image_out,
        text_out,
        image_grad,
        text_grad,
        cond_grad,
        mod_wgrad,
        mod_bgrad,
        qkv_wgrad,
        biases[0],
        at_grad[None, :, 3],
        biases[1],
        ff_grad[None, :, 0],
        biases[2],
        ff_grad[None, :, 1],
        biases[3],
    )


def solution(mesh):
    dp, tensor = mesh.shape["dp"], mesh.shape["tensor"]
    chosen = functools.partial(fast_body, dp) if tensor == 4 else plain_body
    return jax.shard_map(
        chosen,
        mesh=mesh,
        in_specs=(
            P("dp", None, "tensor"),
            P("dp", None, "tensor"),
            P(None, "dp"),
            P(None, None, "dp", None, "tensor"),
            P(None, None, None, "tensor"),
            P(None, None, None, None, "tensor"),
            P(None, None, None, "tensor"),
            P(None, None, None, "tensor"),
            P(None, None, "tensor"),
            P(None, None, None, "tensor"),
            P(None, None, "tensor"),
            P(None, None, None, "tensor"),
            P(None, None, "tensor"),
            P("dp", None, "tensor"),
            P("dp", None, "tensor"),
        ),
        out_specs=(
            P("dp", None, "tensor"),
            P("dp", None, "tensor"),
            P("dp", None, "tensor"),
            P("dp", None, "tensor"),
            P(None, "dp"),
            P(None, None, "dp", None, "tensor"),
            P(None, None, None, "tensor"),
            P(None, None, "dp", None, "tensor"),
            P(None, None, None, "tensor"),
            P(None, None, "dp", "tensor"),
            P(None, None, "tensor"),
            P(None, None, "dp", "tensor"),
            P(None, None, "tensor"),
            P(None, None, "dp", "tensor"),
            P(None, None, "tensor"),
        ),
        check_vma=False,
    )
```

```python
import functools

import jax
import jax.numpy as jnp
from jax import lax
from jax.experimental import pallas as pl
from jax.experimental.pallas import tpu as pltpu
from jax.sharding import PartitionSpec as P

HEAD_DIM = 64
EPS = 1e-06
F32 = jnp.float32
BF16 = jnp.bfloat16
GELU_C = 0.7978845608028654
GELU_K = 0.044715
MIB = 1 << 20
MESH = pl.DeviceIdType.MESH
VMEM = pl.BlockSpec(memory_space=pltpu.VMEM)
ANY = pl.BlockSpec(memory_space=pl.ANY)


eps_norm = 1e-06


def gelu_tanh(values):
    return jax.nn.gelu(values, approximate=True)


def share_of(whole_row, offset, share_width):
    return lax.dynamic_slice_in_dim(whole_row, offset, share_width, whole_row.ndim - 1)


def norm_forward(shards, shifts, scales):
    saved_norm = []
    gathered = (
        lax.all_gather(shards[0].astype(jnp.bfloat16), "tensor", axis=2, tiled=True).astype(
            jnp.float32
        ),
        lax.all_gather(shards[1].astype(jnp.bfloat16), "tensor", axis=2, tiled=True).astype(
            jnp.float32
        ),
    )
    moddeds = []
    for stream in range(2):
        row_mean = jnp.mean(gathered[stream], axis=-1, keepdims=True)
        centred = gathered[stream] - row_mean
        inv_std = lax.rsqrt(jnp.mean(centred * centred, axis=-1, keepdims=True) + eps_norm)
        normed = centred * inv_std
        moddeds.append(
            (normed * (1.0 + scales[stream][:, None, :]) + shifts[stream][:, None, :]).astype(
                jnp.bfloat16
            )
        )
        saved_norm.append((normed, inv_std))
    return (moddeds, saved_norm)


def norm_backward(partials, saved_norm, scales, offset, share_width):
    results = []
    totals = (
        lax.psum(partials[0].astype(jnp.bfloat16), "tensor").astype(jnp.float32),
        lax.psum(partials[1].astype(jnp.bfloat16), "tensor").astype(jnp.float32),
    )
    for stream in range(2):
        normed, inv_std = saved_norm[stream]
        grad_normed = totals[stream] * (1.0 + scales[stream][:, None, :])
        mean_grad = jnp.mean(grad_normed, axis=-1, keepdims=True)
        mean_cross = jnp.mean(grad_normed * normed, axis=-1, keepdims=True)
        local_total = share_of(totals[stream], offset, share_width)
        local_normed = share_of(normed, offset, share_width)
        local_grad = share_of(grad_normed, offset, share_width)
        results.append(
            (
                inv_std * (local_grad - mean_grad - local_normed * mean_cross),
                jnp.sum(local_total, axis=1),
                jnp.sum(local_total * local_normed, axis=1),
            )
        )
    return results


def reduce_branches(partials):
    return (
        lax.psum_scatter(
            partials[0].astype(jnp.bfloat16), "tensor", scatter_dimension=2, tiled=True
        ).astype(jnp.float32),
        lax.psum_scatter(
            partials[1].astype(jnp.bfloat16), "tensor", scatter_dimension=2, tiled=True
        ).astype(jnp.float32),
    )


def gather_grads(branch_grads):
    return (
        lax.all_gather(branch_grads[0], "tensor", axis=2, tiled=True),
        lax.all_gather(branch_grads[1], "tensor", axis=2, tiled=True),
    )


def attend(joint_qkv, heads_here, score_scale):
    seq_count, tokens = (joint_qkv.shape[0], joint_qkv.shape[1])
    separated = joint_qkv.reshape(seq_count, tokens, 3, heads_here, HEAD_DIM)
    scores = (
        jnp.einsum(
            "sqhd,skhd->shqk",
            separated[:, :, 0],
            separated[:, :, 1],
            preferred_element_type=jnp.float32,
        )
        * score_scale
    )
    highest_score = jnp.max(scores, axis=-1, keepdims=True)
    raised = jnp.exp(scores - highest_score)
    denominator = jnp.sum(raised, axis=-1, keepdims=True)
    weights = (raised / denominator).astype(jnp.bfloat16)
    mixed_heads = jnp.einsum(
        "shqk,skhd->sqhd", weights, separated[:, :, 2], preferred_element_type=jnp.float32
    )
    return (
        mixed_heads.astype(jnp.bfloat16).reshape(seq_count, tokens, heads_here * HEAD_DIM),
        highest_score + jnp.log(denominator),
    )


def attend_back(joint_qkv, log_total, head_grads, heads_here, score_scale):
    seq_count, tokens = (joint_qkv.shape[0], joint_qkv.shape[1])
    separated = joint_qkv.reshape(seq_count, tokens, 3, heads_here, HEAD_DIM)
    queries, keys_all, values = (separated[:, :, 0], separated[:, :, 1], separated[:, :, 2])
    outgrad = head_grads.reshape(seq_count, tokens, heads_here, HEAD_DIM)
    scores = (
        jnp.einsum("sqhd,skhd->shqk", queries, keys_all, preferred_element_type=jnp.float32)
        * score_scale
    )
    weights = jnp.exp(scores - log_total)
    weight_grad = jnp.einsum("sqhd,skhd->shqk", outgrad, values, preferred_element_type=jnp.float32)
    row_dot = jnp.sum(weights * weight_grad, axis=-1, keepdims=True)
    score_grad = (weights * (weight_grad - row_dot)).astype(jnp.bfloat16)
    query_grad = (
        jnp.einsum("shqk,skhd->sqhd", score_grad, keys_all, preferred_element_type=jnp.float32)
        * score_scale
    )
    key_grad = (
        jnp.einsum("shqk,sqhd->skhd", score_grad, queries, preferred_element_type=jnp.float32)
        * score_scale
    )
    value_grad = jnp.einsum(
        "shqk,sqhd->skhd", weights.astype(jnp.bfloat16), outgrad, preferred_element_type=jnp.float32
    )
    stacked = jnp.stack([query_grad, key_grad, value_grad], axis=2)
    return stacked.reshape(seq_count, tokens, 3, heads_here * HEAD_DIM).astype(jnp.bfloat16)


def plain_body(
    image_in,
    text_in,
    cond_in,
    mod_weight,
    mod_bias,
    qkv_weight,
    qkv_bias,
    out_weight,
    out_bias,
    up_weight,
    up_bias,
    down_weight,
    down_bias,
    image_cot,
    text_cot,
):
    share_width = image_in.shape[2]
    offset = lax.axis_index("tensor") * share_width
    heads_here = qkv_weight.shape[4] // HEAD_DIM
    score_scale = HEAD_DIM ** (-0.5)
    image_rows = image_in.shape[1]
    layer_count = qkv_weight.shape[0]
    cond_float = cond_in.astype(jnp.float32)
    cond_act = jax.nn.silu(cond_float).astype(jnp.bfloat16)
    mod_terms = jnp.einsum(
        "sc,lxcjd->slxjd", cond_act, mod_weight, preferred_element_type=jnp.float32
    )
    modulation = lax.psum_scatter(
        mod_terms, "dp", scatter_dimension=0, tiled=True
    ) + mod_bias.astype(jnp.float32)
    mod_view = lax.all_gather(modulation, "tensor", axis=4, tiled=True)
    residual = [image_in.astype(jnp.float32), text_in.astype(jnp.float32)]
    layer_at = 0
    moddeds, first_norm = norm_forward(
        residual,
        [mod_view[:, layer_at, stream, 0] for stream in range(2)],
        [mod_view[:, layer_at, stream, 1] for stream in range(2)],
    )
    projected = [
        (
            jnp.einsum(
                "snd,dje->snje",
                moddeds[stream],
                qkv_weight[layer_at, stream],
                preferred_element_type=jnp.float32,
            )
            + qkv_bias[layer_at, stream]
        ).astype(jnp.bfloat16)
        for stream in range(2)
    ]
    joint_qkv = jnp.concatenate(projected, axis=1)
    attended, log_total = attend(joint_qkv, heads_here, score_scale)
    pieces = [attended[:, :image_rows], attended[:, image_rows:]]
    summed = reduce_branches(
        [
            jnp.einsum(
                "puj,oj->puo",
                pieces[stream],
                out_weight[layer_at, stream],
                preferred_element_type=jnp.float32,
            )
            for stream in range(2)
        ]
    )
    first_branch = [summed[stream] + out_bias[layer_at, stream] for stream in range(2)]
    residual = [
        residual[stream] + modulation[:, layer_at, stream, 2][:, None, :] * first_branch[stream]
        for stream in range(2)
    ]
    second_mod, second_norm = norm_forward(
        residual,
        [mod_view[:, layer_at, stream, 3] for stream in range(2)],
        [mod_view[:, layer_at, stream, 4] for stream in range(2)],
    )
    hidden = [
        jnp.einsum(
            "snd,df->snf",
            second_mod[stream],
            up_weight[layer_at, stream],
            preferred_element_type=jnp.float32,
        )
        + up_bias[layer_at, stream]
        for stream in range(2)
    ]
    activated = [gelu_tanh(hidden[stream]).astype(jnp.bfloat16) for stream in range(2)]
    summed = reduce_branches(
        [
            jnp.einsum(
                "snf,df->snd",
                activated[stream],
                down_weight[layer_at, stream],
                preferred_element_type=jnp.float32,
            )
            for stream in range(2)
        ]
    )
    second_branch = [summed[stream] + down_bias[layer_at, stream] for stream in range(2)]
    residual = [
        residual[stream] + modulation[:, layer_at, stream, 5][:, None, :] * second_branch[stream]
        for stream in range(2)
    ]
    forward_saved = [
        (
            moddeds,
            first_norm,
            joint_qkv,
            attended,
            log_total,
            first_branch,
            second_mod,
            second_norm,
            hidden,
            activated,
            second_branch,
        )
    ]
    gradients = [image_cot.astype(jnp.float32), text_cot.astype(jnp.float32)]
    mod_parts = [None] * layer_count
    weight_parts = [None] * layer_count
    bias_parts = [None] * layer_count
    for layer_at in reversed(range(layer_count)):
        (
            moddeds,
            first_norm,
            joint_qkv,
            attended,
            log_total,
            first_branch,
            second_mod,
            second_norm,
            hidden,
            activated,
            second_branch,
        ) = forward_saved[layer_at]
        second_gate = [
            jnp.sum(second_branch[stream] * gradients[stream], axis=1) for stream in range(2)
        ]
        branch_grads = [
            (modulation[:, layer_at, stream, 5][:, None, :] * gradients[stream]).astype(
                jnp.bfloat16
            )
            for stream in range(2)
        ]
        down_bias_grad = [
            jnp.sum(branch_grads[stream].astype(jnp.float32), axis=(0, 1)) for stream in range(2)
        ]
        whole_grads = gather_grads(branch_grads)
        down_grad = [
            jnp.einsum(
                "snd,snf->df",
                whole_grads[stream],
                activated[stream],
                preferred_element_type=jnp.float32,
            )
            for stream in range(2)
        ]
        act_grad = [
            jnp.einsum(
                "snd,df->snf",
                whole_grads[stream],
                down_weight[layer_at, stream],
                preferred_element_type=jnp.float32,
            )
            for stream in range(2)
        ]
        hidden_grad = [
            jax.vjp(gelu_tanh, hidden[stream])[1](act_grad[stream])[0].astype(jnp.bfloat16)
            for stream in range(2)
        ]
        up_bias_grad = [
            jnp.sum(hidden_grad[stream].astype(jnp.float32), axis=(0, 1)) for stream in range(2)
        ]
        up_grad = [
            jnp.einsum(
                "snd,snf->df",
                second_mod[stream],
                hidden_grad[stream],
                preferred_element_type=jnp.float32,
            )
            for stream in range(2)
        ]
        norm_partials = [
            jnp.einsum(
                "snf,df->snd",
                hidden_grad[stream],
                up_weight[layer_at, stream],
                preferred_element_type=jnp.float32,
            )
            for stream in range(2)
        ]
        second_back = norm_backward(
            norm_partials,
            second_norm,
            [mod_view[:, layer_at, stream, 4] for stream in range(2)],
            offset,
            share_width,
        )
        gradients = [gradients[stream] + second_back[stream][0] for stream in range(2)]
        first_gate = [
            jnp.sum(first_branch[stream] * gradients[stream], axis=1) for stream in range(2)
        ]
        branch_grads = [
            (modulation[:, layer_at, stream, 2][:, None, :] * gradients[stream]).astype(
                jnp.bfloat16
            )
            for stream in range(2)
        ]
        out_bias_grad = [
            jnp.sum(branch_grads[stream].astype(jnp.float32), axis=(0, 1)) for stream in range(2)
        ]
        whole_grads = gather_grads(branch_grads)
        pieces = [attended[:, :image_rows], attended[:, image_rows:]]
        out_grad = [
            jnp.einsum(
                "kux,kut->xt",
                whole_grads[stream],
                pieces[stream],
                preferred_element_type=jnp.float32,
            )
            for stream in range(2)
        ]
        head_grads = jnp.concatenate(
            [
                jnp.einsum(
                    "hom,mr->hor",
                    whole_grads[stream],
                    out_weight[layer_at, stream],
                    preferred_element_type=jnp.float32,
                )
                for stream in range(2)
            ],
            axis=1,
        ).astype(jnp.bfloat16)
        joint_grad = attend_back(joint_qkv, log_total, head_grads, heads_here, score_scale)
        stream_grads = [joint_grad[:, :image_rows], joint_grad[:, image_rows:]]
        qkv_bias_grad = [
            jnp.sum(stream_grads[stream].astype(jnp.float32), axis=(0, 1)) for stream in range(2)
        ]
        qkv_grad = [
            jnp.einsum(
                "snd,snje->dje",
                moddeds[stream],
                stream_grads[stream],
                preferred_element_type=jnp.float32,
            )
            for stream in range(2)
        ]
        norm_partials = [
            jnp.einsum(
                "snje,dje->snd",
                stream_grads[stream],
                qkv_weight[layer_at, stream],
                preferred_element_type=jnp.float32,
            )
            for stream in range(2)
        ]
        first_back = norm_backward(
            norm_partials,
            first_norm,
            [mod_view[:, layer_at, stream, 1] for stream in range(2)],
            offset,
            share_width,
        )
        gradients = [gradients[stream] + first_back[stream][0] for stream in range(2)]
        mod_parts[layer_at] = jnp.stack(
            [
                jnp.stack(
                    [
                        first_back[stream][1],
                        first_back[stream][2],
                        first_gate[stream],
                        second_back[stream][1],
                        second_back[stream][2],
                        second_gate[stream],
                    ],
                    axis=1,
                )
                for stream in range(2)
            ],
            axis=1,
        )
        bias_parts[layer_at] = (
            jnp.stack(qkv_bias_grad, axis=0),
            jnp.stack(out_bias_grad, axis=0),
            jnp.stack(up_bias_grad, axis=0),
            jnp.stack(down_bias_grad, axis=0),
        )
        weight_parts[layer_at] = (
            jnp.stack(qkv_grad, axis=0),
            jnp.stack(out_grad, axis=0),
            jnp.stack(up_grad, axis=0),
            jnp.stack(down_grad, axis=0),
        )
    reduced = (
        lax.psum_scatter(
            jnp.stack([weight_parts[0][0]], axis=0).astype(jnp.bfloat16),
            "dp",
            scatter_dimension=2,
            tiled=True,
        ).astype(jnp.float32),
        lax.psum_scatter(
            jnp.stack([weight_parts[0][1]], axis=0).astype(jnp.bfloat16),
            "dp",
            scatter_dimension=2,
            tiled=True,
        ).astype(jnp.float32),
        lax.psum_scatter(
            jnp.stack([weight_parts[0][2]], axis=0).astype(jnp.bfloat16),
            "dp",
            scatter_dimension=2,
            tiled=True,
        ).astype(jnp.float32),
        lax.psum_scatter(
            jnp.stack([weight_parts[0][3]], axis=0).astype(jnp.bfloat16),
            "dp",
            scatter_dimension=2,
            tiled=True,
        ).astype(jnp.float32),
    )
    bias_totals = lax.psum(
        (
            jnp.stack([bias_parts[0][0]], axis=0),
            jnp.stack([bias_parts[0][1]], axis=0),
            jnp.stack([bias_parts[0][2]], axis=0),
            jnp.stack([bias_parts[0][3]], axis=0),
        ),
        "dp",
    )
    mod_grad = jnp.stack(mod_parts, axis=1).astype(jnp.bfloat16)
    all_mod = lax.all_gather(mod_grad, "dp", axis=0, tiled=True)
    mod_wgrad = jnp.einsum("sc,slxjd->lxcjd", cond_act, all_mod, preferred_element_type=jnp.float32)
    mod_bgrad = jnp.sum(all_mod.astype(jnp.float32), axis=0)
    act_partial = jnp.einsum(
        "slxjd,lxcjd->sc", all_mod, mod_weight, preferred_element_type=jnp.float32
    )
    act_total = lax.psum(act_partial, "tensor")
    cond_grad = jax.vjp(jax.nn.silu, cond_float)[1](act_total)[0]
    return (
        residual[0],
        residual[1],
        gradients[0],
        gradients[1],
        cond_grad,
        mod_wgrad,
        mod_bgrad,
        reduced[0],
        bias_totals[0],
        reduced[1],
        bias_totals[1],
        reduced[2],
        bias_totals[2],
        reduced[3],
        bias_totals[3],
    )


def nt_dot(a, b):
    return lax.dot_general(a, b, (((1,), (1,)), ((), ())), preferred_element_type=F32)


def nn_dot(a, b):
    return lax.dot_general(a, b, (((1,), (0,)), ((), ())), preferred_element_type=F32)


def tn_dot(a, b):
    return lax.dot_general(a, b, (((0,), (0,)), ((), ())), preferred_element_type=F32)


def exact_nt(a, b):
    return lax.dot_general(
        a, b, (((1,), (1,)), ((), ())), preferred_element_type=F32, precision=lax.Precision.HIGHEST
    )


def exact_tn(a, b):
    return lax.dot_general(
        a, b, (((0,), (0,)), ((), ())), preferred_element_type=F32, precision=lax.Precision.HIGHEST
    )


def sds(shape, dtype):
    return jax.ShapeDtypeStruct(shape, dtype)


def cost(flops, arrays, outs):
    moved = sum(a.size * a.dtype.itemsize for a in arrays)
    moved += sum(o.size * o.dtype.itemsize for o in outs)
    return pl.CostEstimate(flops=flops, bytes_accessed=moved, transcendentals=0)


def eye_rows():
    return (
        lax.broadcasted_iota(jnp.int32, (8, 128), 0) == lax.broadcasted_iota(jnp.int32, (8, 128), 1)
    ).astype(F32)


def norm_stats(pieces, width):
    total = sum(jnp.sum(p, axis=-1, keepdims=True) for p in pieces)
    mean = total / width
    centred = [p - mean for p in pieces]
    var = sum(jnp.sum(c * c, axis=-1, keepdims=True) for c in centred) / width
    return mean, lax.rsqrt(var + EPS), centred


def stat_rows(first, second):
    lane = lax.broadcasted_iota(jnp.int32, (first.shape[0], 128), 1)
    both = jnp.where(lane == 0, first, jnp.where(lane == 1, second, 0.0))
    return exact_nt(eye_rows(), both)


def stat_cols(first, second):
    lane = lax.broadcasted_iota(jnp.int32, (first.shape[0], 128), 1)
    return jnp.where(lane == 0, first, jnp.where(lane == 1, second, 0.0))


class Links:
    def __init__(self, send, recv):
        self.send_sem, self.recv_sem = send, recv
        me = lax.axis_index("tensor")
        self.peers = [me, me + 1 - 2 * (me % 2), (me + 2) % 4, 3 - me]

    def enter(self, extra=()):
        barrier = pltpu.get_barrier_semaphore()
        for peer in self.peers[1:]:
            pl.semaphore_signal(barrier, inc=1, device_id={"tensor": peer}, device_id_type=MESH)
        for peer in extra:
            pl.semaphore_signal(barrier, inc=1, device_id={"dp": peer}, device_id_type=MESH)
        pl.semaphore_wait(barrier, 3 + len(extra))

    def copy(self, src, dst, kind, c, peer):
        return pltpu.make_async_remote_copy(
            src_ref=src,
            dst_ref=dst,
            send_sem=self.send_sem.at[kind, c],
            recv_sem=self.recv_sem.at[kind, c],
            device_id={"tensor": peer},
            device_id_type=MESH,
        )

    def route(self, c):
        odd = c % 2
        first = self.peers[1] * (1 - odd) + self.peers[2] * odd
        second = self.peers[2] * (1 - odd) + self.peers[1] * odd
        return 1 + odd, 2 - odd, first, second

    def gather_copy(self, i, src, buf, kind, c):
        near, far, first, second = self.route(c)
        if i == 0:
            return self.copy(src, buf.at[c, near], kind, c, first)
        if i == 1:
            return self.copy(src, buf.at[c, far], kind + 1, c, second)
        return self.copy(buf.at[c, near], buf.at[c, 3], kind + 2, c, second)

    def gather_start(self, *args):
        self.gather_copy(0, *args).start()
        self.gather_copy(1, *args).start()

    def gather_relay(self, *args):
        self.gather_copy(0, *args).wait_recv()
        self.gather_copy(2, *args).start()

    def gather_finish(self, *args):
        self.gather_copy(1, *args).wait_recv()
        self.gather_copy(2, *args).wait_recv()

    def gather_sent(self, *args):
        for i in range(3):
            self.gather_copy(i, *args).wait_send()

    def scatter_copy(self, i, part, relayed, got, kind, c):
        near, _, first, second = self.route(c)
        if i == 0:
            return self.copy(part.at[c, 3], got.at[c, 0], kind, c, first)
        if i == 1:
            return self.copy(part.at[c, near], got.at[c, 1], kind + 1, c, first)
        return self.copy(relayed.at[c], got.at[c, 2], kind + 2, c, second)

    def scatter_start(self, *args):
        self.scatter_copy(0, *args).start()
        self.scatter_copy(1, *args).start()

    def scatter_relay(self, part, relayed, got, kind, c):
        self.scatter_copy(0, part, relayed, got, kind, c).wait_recv()
        _, far, _, _ = self.route(c)
        relayed[c] = (part[c, far].astype(F32) + got[c, 0].astype(F32)).astype(BF16)
        self.scatter_copy(2, part, relayed, got, kind, c).start()

    def scatter_sent(self, *args):
        for i in range(3):
            self.scatter_copy(i, *args).wait_send()

    def scatter_finish(self, part, relayed, got, kind, c):
        self.scatter_copy(1, part, relayed, got, kind, c).wait_recv()
        self.scatter_copy(2, part, relayed, got, kind, c).wait_recv()
        return part[c, 0].astype(F32) + got[c, 1].astype(F32) + got[c, 2].astype(F32)

    def rows_copies(self, src, dst, kind, c):
        return [
            self.copy(src.at[c], dst.at[c, k - 1], kind + k - 1, c, self.peers[k]) for k in (1, 2, 3)
        ]

    def rows_start(self, src, dst, kind, c):
        for copy in self.rows_copies(src, dst, kind, c):
            copy.start()

    def rows_finish(self, src, dst, kind, c):
        for copy in self.rows_copies(src, dst, kind, c):
            copy.wait_recv()
        return src[c] + dst[c, 0] + dst[c, 1] + dst[c, 2]


class Column:
    def __init__(self, chips, send, recv):
        index = lax.axis_index("dp")
        self.chips, self.z, self.core = chips, index // 2, index % 2
        self.send_sem, self.recv_sem = send, recv
        self.others = [((self.z + r) % chips) * 2 + self.core for r in range(1, chips)]

    def copy(self, src, dst, kind, i, chip):
        return pltpu.make_async_remote_copy(
            src_ref=src,
            dst_ref=dst,
            send_sem=self.send_sem.at[kind, i],
            recv_sem=self.recv_sem.at[kind, i],
            device_id={"dp": chip * 2 + self.core},
            device_id_type=MESH,
        )

    def hop(self, buf, kind, dist, way, behind):
        step = 1 - 2 * way
        origin = self.z - step * (dist + behind)
        block = buf.at[origin]
        return self.copy(block, block, kind, 2 * dist + way, self.z + step * (1 - behind))

    def sends(self, dist, way):
        if way == 0:
            return (self.z >= dist) & (self.z < self.chips - 1)
        return (self.z < self.chips - dist) & (self.z > 0)

    def receives(self, dist, way):
        return self.z > dist if way == 0 else self.z < self.chips - 1 - dist

    def spread(self, buf, kind, dist):
        for way in (0, 1):
            if dist:

                @pl.when(self.receives(dist - 1, way))
                def _():
                    self.hop(buf, kind, dist - 1, way, 1).wait_recv()

            if dist < self.chips - 1:

                @pl.when(self.sends(dist, way))
                def _():
                    self.hop(buf, kind, dist, way, 0).start()

    def spread_sent(self, buf, kind):
        for dist in range(self.chips - 1):
            for way in (0, 1):

                @pl.when(self.sends(dist, way))
                def _():
                    self.hop(buf, kind, dist, way, 0).wait_send()

    def block_of(self, chip):
        me = lax.axis_index("tensor")
        return (chip % 2 + me % 2) % 2 + 2 * ((chip // 2 + me // 2) % 2)

    def deal_copy(self, blocks, buf, kind, r, taken):
        chip = (self.z + r) % self.chips
        src = blocks.at[self.block_of(chip), pl.ds(0, taken), :]
        return self.copy(src, buf.at[self.z], kind, r - 1, chip)

    def deal(self, blocks, buf, kind, taken):
        for r in range(1, self.chips):
            self.deal_copy(blocks, buf, kind, r, taken).start()

    def deal_own(self, blocks, buf, sem, taken):
        src = blocks.at[self.block_of(self.z), pl.ds(0, taken), :]
        return pltpu.make_async_copy(src, buf.at[self.z], sem)

    def deal_wait(self, blocks, buf, kind, taken):
        for r in range(1, self.chips):
            self.deal_copy(blocks, buf, kind, r, taken).wait()


def wait_sends(copies):
    for copy in copies:
        copy.wait_send()


def stages(count, steps):
    last = max(offset for offset, _ in steps)

    def tick(t, carry):
        for offset, step in steps:
            c = t - offset

            @pl.when((c >= 0) & (c < count))
            def _():
                step(c)

        return carry

    lax.fori_loop(0, count + last, tick, 0)


def front_kernel(dp, valid, refs_in, refs_out, scratch):
    x_ref, cot_ref, act_ref, modw_ref, modb_ref, wq_ref, bq_ref = refs_in
    m_ref, qkv_ref, o_ref, lse_ref, g_ref, xp_ref, mod_ref, gsum_ref, zm_ref = refs_out
    modw, wq, terms, got, k_all, aug, local, send, recv, msend, mrecv, zsend, zrecv = scratch
    count, rows, feats = x_ref.shape
    cols = qkv_ref.shape[-1]
    width = 4 * feats
    links = Links(send, recv)
    column = Column(dp // 2, zsend, zrecv)
    taken = zm_ref.shape[1]
    text = count - 1
    mine = lax.axis_index("dp")
    others = [(mine + r) % dp for r in range(1, dp)]
    load_mod = pltpu.make_async_copy(modw_ref, modw, local.at[0])
    load_wq = pltpu.make_async_copy(wq_ref, wq, local.at[1])
    load_mod.start()
    load_wq.start()
    links.enter(others)
    for c in (text, *range(text)):
        links.gather_start(x_ref.at[c], xp_ref, 0, c)
    load_mod.wait()
    act = act_ref[...]
    for j in range(12):
        terms[:, j, :] = nn_dot(act, modw[j])
    pushes = [
        pltpu.make_async_remote_copy(
            src_ref=terms.at[others[r]],
            dst_ref=got.at[r],
            send_sem=msend.at[r],
            recv_sem=mrecv.at[r],
            device_id={"dp": others[r]},
            device_id_type=MESH,
        )
        for r in range(dp - 1)
    ]
    for push in pushes:
        push.start()
    for c in range(count):
        xp_ref[c, 0] = x_ref[c]
    total = terms[mine] + modb_ref[...]
    for r, push in enumerate(pushes):
        push.wait_recv()
        total = total + got[r]
    mod_ref[0] = total
    mod_copies = [
        links.copy(mod_ref.at[0], mod_ref.at[k], 6, k, links.peers[k]) for k in (1, 2, 3)
    ]
    for copy in mod_copies:
        copy.start()
    for c in (text, *range(text)):
        links.gather_relay(x_ref.at[c], xp_ref, 0, c)
    for c in range(count):
        stream = c // (count - 1)
        g = (total[stream * 6 + 5 : stream * 6 + 6, :] * cot_ref[c].astype(F32)).astype(BF16)
        g_ref[c, 0] = g
        gsum_ref[c : c + 1, :] = jnp.sum(g.astype(F32), axis=0, keepdims=True)
    for c in (text, *range(text)):
        links.gather_start(g_ref.at[c, 0], g_ref, 3, c)
    for copy in mod_copies:
        copy.wait_recv()
    load_wq.wait()

    def project(s, carry):
        c = (s + text) % count
        stream = c // (count - 1)
        links.gather_finish(x_ref.at[c], xp_ref, 0, c)
        _, inv, centred = norm_stats([xp_ref[c, k].astype(F32) for k in range(4)], width)
        acc = [None] * 3
        for k in range(4):
            shift = mod_ref[k, pl.ds(stream * 6, 1), :]
            scale = mod_ref[k, pl.ds(stream * 6 + 1, 1), :]
            m = (centred[k] * inv * (1.0 + scale) + shift).astype(BF16)
            m_ref[c, k] = m
            for j in range(3):
                part = nn_dot(m, wq[stream, j, links.peers[k]])
                acc[j] = part if k == 0 else acc[j] + part
        for j in range(3):
            qkv_ref[j, c] = (acc[j] + bq_ref[stream, j : j + 1, :]).astype(BF16)
        links.gather_relay(g_ref.at[c, 0], g_ref, 3, c)

        @pl.when(s == 0)
        def _():
            column.deal(m_ref.at[text], zm_ref, 0, taken)
            column.deal_own(m_ref.at[text], zm_ref, local.at[2], taken).start()

        return carry

    lax.fori_loop(0, count, project, 0)

    owner = lax.broadcasted_iota(jnp.int32, (1, 128), 1) // HEAD_DIM

    def heads_pair(p, carry):
        lanes = pl.ds(pl.multiple_of(p * 128, 128), 128)
        for c in range(count):
            size = min(rows, valid - c * rows)
            sl = slice(c * rows, c * rows + size)
            k_all[sl, :] = qkv_ref[1, c, :size, lanes]
            values = qkv_ref[2, c, :size, lanes]
            for h in range(2):
                aug[h, sl, :] = jnp.where(owner == h, values, jnp.ones_like(values))

        def chunk(c, inner):
            q = qkv_ref[0, c, :, lanes] * jnp.asarray(HEAD_DIM**-0.5, BF16)
            out, lse = [], []
            for h in range(2):
                scores = nt_dot(jnp.where(owner == h, q, jnp.zeros_like(q)), k_all[...])
                top = jnp.max(scores, axis=-1, keepdims=True)
                acc = nn_dot(jnp.exp(scores - top).astype(BF16), aug[h])
                other = (1 - h) * HEAD_DIM
                denom = acc[:, other : other + 1]
                out.append(acc / denom)
                lse.append(top + jnp.log(denom))
            o_ref[c, :, lanes] = jnp.where(owner == 0, out[0], out[1]).astype(BF16)
            lse_ref[c, :, lanes] = jnp.where(owner == 0, lse[0], lse[1])
            return inner

        lax.fori_loop(0, count, chunk, 0)
        return carry

    lax.fori_loop(0, cols // 128, heads_pair, 0)
    for c in range(count):
        links.gather_finish(g_ref.at[c, 0], g_ref, 3, c)
        links.gather_sent(x_ref.at[c], xp_ref, 0, c)
        links.gather_sent(g_ref.at[c, 0], g_ref, 3, c)
    wait_sends(mod_copies)
    wait_sends(pushes)
    column.deal_own(m_ref.at[text], zm_ref, local.at[2], taken).wait()
    column.deal_wait(m_ref.at[text], zm_ref, 0, taken)


def front_call(dp, valid, taken, x, cot, act, mod_w, mod_b, wq, bq):
    count, rows, feats = x.shape
    cols = wq.shape[-1]
    arrays = [x, cot, act, mod_w, mod_b, wq, bq]
    outs = [
        sds((count, 4, rows, feats), BF16),
        sds((3, count, rows, cols), BF16),
        sds((count, rows, cols), BF16),
        sds((count, rows, cols), F32),
        sds((count, 4, rows, feats), BF16),
        sds((count, 4, rows, feats), BF16),
        sds((4, 12, feats), F32),
        sds((count, feats), F32),
        sds((dp // 2, taken, feats), BF16),
    ]
    n_in, n_out = len(arrays), len(outs)

    def kernel(*refs):
        front_kernel(dp, valid, refs[:n_in], refs[n_in : n_in + n_out], refs[n_in + n_out :])

    return pl.pallas_call(
        kernel,
        out_shape=outs,
        in_specs=[VMEM, VMEM, VMEM, ANY, VMEM, ANY, VMEM],
        out_specs=[VMEM] * (n_out - 1) + [ANY],
        scratch_shapes=[
            pltpu.VMEM(mod_w.shape, BF16),
            pltpu.VMEM(wq.shape, BF16),
            pltpu.VMEM((dp, 12, feats), F32),
            pltpu.VMEM((dp - 1, 12, feats), F32),
            pltpu.VMEM((valid, 128), BF16),
            pltpu.VMEM((2, valid, 128), BF16),
            pltpu.SemaphoreType.DMA((3,)),
            pltpu.SemaphoreType.DMA((7, count)),
            pltpu.SemaphoreType.DMA((7, count)),
            pltpu.SemaphoreType.DMA((dp - 1,)),
            pltpu.SemaphoreType.DMA((dp - 1,)),
            pltpu.SemaphoreType.DMA((1, dp // 2 - 1)),
            pltpu.SemaphoreType.DMA((1, dp // 2 - 1)),
        ],
        compiler_params=pltpu.CompilerParams(
            collective_id=1, has_side_effects=True, vmem_limit_bytes=56 * MIB
        ),
        cost_estimate=cost(20 * 10**9, arrays, outs),
        name="front",
    )(*arrays)


HB = 512


def middle_kernel(chips, refs_in, refs_out, scratch):
    o_ref, x_ref, cot_ref, db2_ref, mod_ref, wo_ref, up_ref, down_ref, ub_ref, ob_ref = refs_in
    x1_out, m2_out, a_out, du_out, b2_out, g1_out = refs_out[:6]
    g_ref, do_ref, line_ref, dub_ref, zr_ref, zl_ref, zo_ref = refs_out[6:]
    (wo, up, down, db2, part, relayed, got, xp, branch, acc_m, acc_b, cols_s) = scratch[:12]
    (x1_s, m2_s, a_s, du_s, b2_s, g1_s, srow, sgot, local, out_sem, send, recv) = scratch[12:24]
    zsend, zrecv, zlocal = scratch[24:]
    count, _, feats = x_ref.shape
    width = 4 * feats
    hidden = up.shape[-1]
    links = Links(send, recv)
    column = Column(chips, zsend, zrecv)
    text = count - 1
    taken = zo_ref.shape[1]

    def at(s):
        return (s + text) % count

    loads = [
        pltpu.make_async_copy(src, dst, local.at[i])
        for i, (src, dst) in enumerate(
            [(wo_ref, wo), (up_ref, up), (down_ref, down), (db2_ref, db2)]
        )
    ]
    for load in loads:
        load.start()
    links.enter(column.others)
    loads[0].wait()

    def flush(staged, out, kind, s):
        return pltpu.make_async_copy(staged.at[s % 2], out.at[at(s)], out_sem.at[kind, s % 2])

    first_rows = pl.ds(0, taken)

    def own_rights():
        return [
            pltpu.make_async_copy(
                du_s.at[0, first_rows, :], zr_ref.at[column.z, 0], zlocal.at[0]
            ),
            pltpu.make_async_copy(a_s.at[0, first_rows, :], zr_ref.at[column.z, 1], zlocal.at[1]),
            column.deal_own(m2_s.at[0], zl_ref.at[0], zlocal.at[2], taken),
        ]

    def own_early():
        return [
            pltpu.make_async_copy(o_ref.at[text, first_rows, :], zo_ref.at[column.z], zlocal.at[3]),
            column.deal_own(db2.at[text], zl_ref.at[1], zlocal.at[4], taken),
        ]

    def column_early(s):
        @pl.when(s == 0)
        def _():
            loads[3].wait()
            for copy in own_early():
                copy.start()
            column.deal(db2.at[text], zl_ref.at[1], 3, taken)
            for copy in own_early():
                copy.wait()
            column.spread(zo_ref, 1, 0)

    def column_start(s):
        @pl.when(s == 0)
        def _():
            for copy in own_rights():
                copy.wait()
            flush(m2_s, m2_out, 1, 0).wait()
            column.spread(zr_ref, 0, 0)
            column.deal(m2_out.at[text], zl_ref.at[0], 2, taken)
            column.spread(zo_ref, 1, 1)

    def column_relay(dist):
        def step(s):
            @pl.when(s == 0)
            def _():
                column.spread(zr_ref, 0, dist)
                if dist == 1:
                    column.spread(zo_ref, 1, 2)

        return step

    def project(s):
        c = at(s)
        stream = c // (count - 1)
        o = o_ref[c]
        for k in (3, 1, 2, 0):
            part[c, k] = nt_dot(o, wo[stream, links.peers[k]]).astype(BF16)
        links.scatter_start(part, relayed, got, 0, c)

    def first_relay(s):
        c = at(s)
        links.scatter_relay(part, relayed, got, 0, c)

    def residual(s):
        c = at(s)
        stream = c // (count - 1)
        total = links.scatter_finish(part, relayed, got, 0, c)
        add = total + ob_ref[pl.ds(stream, 1), :]
        branch[c] = add
        moved = x_ref[c].astype(F32) + mod_ref[0, pl.ds(stream * 6 + 2, 1), :] * add

        @pl.when(s >= 2)
        def _():
            flush(x1_s, x1_out, 0, s - 2).wait()

        x1_s[s % 2] = moved
        flush(x1_s, x1_out, 0, s).start()
        xp[c, 0] = moved.astype(BF16)
        links.gather_start(xp.at[c, 0], xp, 3, c)

    def second_relay(s):
        c = at(s)
        links.gather_relay(xp.at[c, 0], xp, 3, c)

    def feed_forward(s):
        c = at(s)
        stream = c // (count - 1)
        slot = s % 2

        @pl.when(s == 0)
        def _():
            for load in loads[1:3]:
                load.wait()

        @pl.when(s >= 2)
        def _():
            for kind, (staged, out) in enumerate(
                [(a_s, a_out), (du_s, du_out), (b2_s, b2_out)]
            ):
                flush(staged, out, kind + 2, s - 2).wait()

        @pl.when(s >= 3)
        def _():
            flush(m2_s, m2_out, 1, s - 2).wait()

        links.gather_finish(xp.at[c, 0], xp, 3, c)
        links.scatter_sent(part, relayed, got, 0, c)
        mean, inv, centred = norm_stats([xp[c, k].astype(F32) for k in range(4)], width)
        for k in range(4):
            shift = mod_ref[k, pl.ds(stream * 6 + 3, 1), :]
            scale = mod_ref[k, pl.ds(stream * 6 + 4, 1), :]
            m2_s[slot, k] = (centred[k] * inv * (1.0 + scale) + shift).astype(BF16)

        def block(b, carry):
            cols = pl.ds(pl.multiple_of(b * HB, HB), HB)
            u = ub_ref[pl.ds(stream, 1), cols]
            for k in range(4):
                u = u + nn_dot(m2_s[slot, k], up[stream, links.peers[k], :, cols])
            da = None
            for k in range(4):
                piece = nn_dot(db2[c, k], down[stream, links.peers[k], :, cols])
                da = piece if da is None else da + piece
            square = u * u
            th = jnp.tanh(u * (GELU_C + (GELU_C * GELU_K) * square))
            up_half = 0.5 + 0.5 * th
            a = (u * up_half).astype(BF16)
            slope = up_half * (
                1.0 + u * (1.0 - th) * (GELU_C + (3.0 * GELU_C * GELU_K) * square)
            )
            du = (da * slope).astype(BF16)
            a_s[slot, :, cols] = a
            du_s[slot, :, cols] = du
            dub_ref[pl.ds(c, 1), cols] = jnp.sum(du.astype(F32), axis=0, keepdims=True)
            for k in range(4):
                dm = nt_dot(du, up[stream, links.peers[k], :, cols])
                bb = nt_dot(a, down[stream, links.peers[k], :, cols])

                @pl.when(b == 0)
                def _():
                    acc_m[k] = dm
                    acc_b[k] = bb

                @pl.when(b != 0)
                def _():
                    acc_m[k] += dm
                    acc_b[k] += bb

            return carry

        lax.fori_loop(0, hidden // HB, block, 0)
        first = second = None
        for k in range(4):
            dm = acc_m[k]
            part[c, k] = dm.astype(BF16)
            dh = dm * (1.0 + mod_ref[k, pl.ds(stream * 6 + 4, 1), :])
            one = jnp.sum(dh, axis=-1, keepdims=True)
            two = jnp.sum(dh * (xp[c, k].astype(F32) - mean), axis=-1, keepdims=True)
            first = one if first is None else first + one
            second = two if second is None else second + two
        srow[c] = stat_rows(first, second * inv)
        links.scatter_start(part, relayed, got, 6, c)
        links.rows_start(srow, sgot, 12, c)
        cols_s[c] = stat_cols(mean, inv)
        for k in range(4):
            b2_s[slot, k] = acc_b[k].astype(BF16)
        for kind, (staged, out) in enumerate(
            [(m2_s, m2_out), (a_s, a_out), (du_s, du_out), (b2_s, b2_out)]
        ):
            flush(staged, out, kind + 1, s).start()

        @pl.when(s == 0)
        def _():
            for copy in own_rights():
                copy.start()

    def third_relay(s):
        c = at(s)
        links.scatter_relay(part, relayed, got, 6, c)

    def norm_back(s):
        c = at(s)
        stream = c // (count - 1)
        total = links.scatter_finish(part, relayed, got, 6, c)
        sums = exact_tn(links.rows_finish(srow, sgot, 12, c), eye_rows())
        mean, inv = cols_s[c, :, 0:1], cols_s[c, :, 1:2]
        normed = (xp[c, 0].astype(F32) - mean) * inv
        grad = total * (1.0 + mod_ref[0, pl.ds(stream * 6 + 4, 1), :])
        g = cot_ref[c].astype(F32) + inv * (
            grad - sums[:, 0:1] / width - normed * (sums[:, 1:2] / width)
        )
        db = (mod_ref[0, pl.ds(stream * 6 + 2, 1), :] * g).astype(BF16)
        g_ref[c, 0] = db
        links.gather_start(g_ref.at[c, 0], g_ref, 9, c)

        @pl.when(s >= 2)
        def _():
            flush(g1_s, g1_out, 5, s - 2).wait()

        g1_s[s % 2] = g
        flush(g1_s, g1_out, 5, s).start()
        line_ref[c, 0:1, :] = jnp.sum(total, axis=0, keepdims=True)
        line_ref[c, 1:2, :] = jnp.sum(total * normed, axis=0, keepdims=True)
        line_ref[c, 2:3, :] = jnp.sum(branch[c] * g, axis=0, keepdims=True)
        line_ref[c, 3:4, :] = jnp.sum(db.astype(F32), axis=0, keepdims=True)

    def fourth_relay(s):
        c = at(s)
        links.gather_relay(g_ref.at[c, 0], g_ref, 9, c)

    def head_grads(s):
        c = at(s)
        stream = c // (count - 1)
        links.gather_finish(g_ref.at[c, 0], g_ref, 9, c)
        acc = None
        for k in range(4):
            piece = nn_dot(g_ref[c, k], wo[stream, links.peers[k]])
            acc = piece if acc is None else acc + piece
        do_ref[c] = acc.astype(BF16)

    stages(
        count,
        [
            (7, fourth_relay),
            (5, third_relay),
            (3, second_relay),
            (1, first_relay),
            (6, norm_back),
            (2, residual),
            (0, project),
            (1, column_early),
            (5, column_start),
            (7, column_relay(1)),
            (9, column_relay(2)),
            (8, head_grads),
            (4, feed_forward),
        ],
    )
    column.spread(zr_ref, 0, chips - 1)
    column.spread(zo_ref, 1, chips - 1)
    column.deal_wait(m2_out.at[text], zl_ref.at[0], 2, taken)
    column.deal_wait(db2.at[text], zl_ref.at[1], 3, taken)
    column.spread_sent(zr_ref, 0)
    column.spread_sent(zo_ref, 1)
    for c in range(count):
        links.gather_sent(xp.at[c, 0], xp, 3, c)
        links.scatter_sent(part, relayed, got, 6, c)
        links.gather_sent(g_ref.at[c, 0], g_ref, 9, c)
        wait_sends(links.rows_copies(srow, sgot, 12, c))
    for c in (count - 2, count - 1):
        for kind, (staged, out) in enumerate(
            [
                (x1_s, x1_out),
                (m2_s, m2_out),
                (a_s, a_out),
                (du_s, du_out),
                (b2_s, b2_out),
                (g1_s, g1_out),
            ]
        ):
            flush(staged, out, kind, c).wait()


def middle_call(dp, taken, o, x, cot, db2, mods, wo, up, down, ub, ob):
    count, rows, feats = x.shape
    cols, hidden = wo.shape[-1], up.shape[-1]
    arrays = [o, x, cot, db2, mods, wo, up, down, ub, ob]
    outs = [
        sds((count, rows, feats), F32),
        sds((count, 4, rows, feats), BF16),
        sds((count, rows, hidden), BF16),
        sds((count, rows, hidden), BF16),
        sds((count, 4, rows, feats), BF16),
        sds((count, rows, feats), F32),
        sds((count, 4, rows, feats), BF16),
        sds((count, rows, cols), BF16),
        sds((count, 4, feats), F32),
        sds((count, hidden), F32),
        sds((dp // 2, 2, taken, hidden), BF16),
        sds((2, dp // 2, taken, feats), BF16),
        sds((dp // 2, taken, cols), BF16),
    ]
    n_in, n_out = len(arrays), len(outs)

    def kernel(*refs):
        middle_kernel(dp // 2, refs[:n_in], refs[n_in : n_in + n_out], refs[n_in + n_out :])

    return pl.pallas_call(
        kernel,
        out_shape=outs,
        in_specs=[VMEM, VMEM, VMEM, ANY, VMEM, ANY, ANY, ANY, VMEM, VMEM],
        out_specs=[ANY] * 6 + [VMEM] * 4 + [ANY] * 3,
        scratch_shapes=[
            pltpu.VMEM(wo.shape, BF16),
            pltpu.VMEM(up.shape, BF16),
            pltpu.VMEM(down.shape, BF16),
            pltpu.VMEM(db2.shape, BF16),
            pltpu.VMEM((count, 4, rows, feats), BF16),
            pltpu.VMEM((count, rows, feats), BF16),
            pltpu.VMEM((count, 3, rows, feats), BF16),
            pltpu.VMEM((count, 4, rows, feats), BF16),
            pltpu.VMEM((count, rows, feats), F32),
            pltpu.VMEM((4, rows, feats), F32),
            pltpu.VMEM((4, rows, feats), F32),
            pltpu.VMEM((count, rows, 128), F32),
            pltpu.VMEM((2, rows, feats), F32),
            pltpu.VMEM((2, 4, rows, feats), BF16),
            pltpu.VMEM((2, rows, hidden), BF16),
            pltpu.VMEM((2, rows, hidden), BF16),
            pltpu.VMEM((2, 4, rows, feats), BF16),
            pltpu.VMEM((2, rows, feats), F32),
            pltpu.VMEM((count, 8, rows), F32),
            pltpu.VMEM((count, 3, 8, rows), F32),
            pltpu.SemaphoreType.DMA((4,)),
            pltpu.SemaphoreType.DMA((6, 2)),
            pltpu.SemaphoreType.DMA((15, count)),
            pltpu.SemaphoreType.DMA((15, count)),
            pltpu.SemaphoreType.DMA((4, dp - 2)),
            pltpu.SemaphoreType.DMA((4, dp - 2)),
            pltpu.SemaphoreType.DMA((5,)),
        ],
        compiler_params=pltpu.CompilerParams(
            collective_id=2, has_side_effects=True, vmem_limit_bytes=63 * MIB
        ),
        cost_estimate=cost(30 * 10**9, arrays, outs),
        name="middle",
    )(*arrays)


def back_kernel(chips, valid, blocks, refs_in, refs_out, scratch):
    qkv_ref, o_ref, do_ref, lse_ref, b2_ref, x1_ref, cot_ref, g1_ref, xp_ref, mod_ref = refs_in[:10]
    wq_ref, db_ref, db1_ref = refs_in[10:]
    dqkv_ref, x2_ref, grad_ref, line_ref, bias_ref, zq_ref, zd_ref = refs_out
    wq, q_all, k_all, v_all, do_all, lse_all, od_all, dk_all, dv_all, dqt_all, dq_all = scratch[:11]
    part, relayed, got, relayed2, got2, cols_s, srow, sgot, local, send, recv = scratch[11:22]
    zsend, zrecv = scratch[22:]
    count, rows, feats = cot_ref.shape
    cols = o_ref.shape[-1]
    width = 4 * feats
    links = Links(send, recv)
    column = Column(chips, zsend, zrecv)
    text = count - 1
    taken = zd_ref.shape[1]
    load = pltpu.make_async_copy(wq_ref, wq, local.at[0])
    load.start()
    links.enter(column.others)
    for c in range(count):
        links.scatter_start(b2_ref, relayed2, got2, 0, c)
    own_db = pltpu.make_async_copy(
        db1_ref.at[text, column.block_of(column.z), pl.ds(0, taken), :],
        zd_ref.at[column.z],
        local.at[1],
    )
    own_db.start()
    column.deal(db1_ref.at[text], zd_ref, 1, taken)
    own_q = [
        pltpu.make_async_copy(
            dqkv_ref.at[j, text, pl.ds(0, taken), :], zq_ref.at[column.z, j], local.at[2 + j]
        )
        for j in range(3)
    ]
    scale = jnp.asarray(HEAD_DIM**-0.5, BF16)
    head_row = lax.broadcasted_iota(jnp.int32, (8, 128), 0)
    lane = lax.broadcasted_iota(jnp.int32, (8, 128), 1)
    first_lane = (lane == head_row * HEAD_DIM).astype(F32)
    within = (lane // HEAD_DIM == head_row).astype(F32)
    owner = lax.broadcasted_iota(jnp.int32, (1, 128), 1) // HEAD_DIM
    zero = jnp.zeros((), BF16)
    for c in range(count):
        size = min(rows, valid - c * rows)
        if size < rows:
            for j in range(3):
                dqkv_ref[j, c] = jnp.zeros((rows, cols), BF16)

    def heads_pair(p, carry):
        lanes = pl.ds(pl.multiple_of(p * 128, 128), 128)
        for c in range(count):
            size = min(rows, valid - c * rows)
            sl = slice(c * rows, c * rows + size)
            q_all[sl, :] = qkv_ref[0, c, :size, lanes] * scale
            k_all[sl, :] = qkv_ref[1, c, :size, lanes]
            v_all[sl, :] = qkv_ref[2, c, :size, lanes]
            do = do_ref[c, :size, lanes]
            do_all[sl, :] = do
            lse_all[sl, :] = lse_ref[c, :size, lanes]
            od_all[sl, :] = o_ref[c, :size, lanes].astype(F32) * do.astype(F32)
        lse_rows = exact_nt(first_lane, lse_all[...])
        dot_rows = exact_nt(within, od_all[...])
        dqt = None
        for h in range(2):
            mine = owner == h
            q = jnp.where(mine, q_all[...], zero)
            do = jnp.where(mine, do_all[...], zero)
            lse_row, dot_row = lse_rows[h : h + 1, :], dot_rows[h : h + 1, :]
            for start, size in blocks:
                sl = slice(start, start + size)
                keys, values = k_all[sl, :], v_all[sl, :]
                weights = jnp.exp(nt_dot(keys, q) - lse_row)
                grads = (weights * (nt_dot(values, do) - dot_row)).astype(BF16)
                dv = nn_dot(weights.astype(BF16), do)
                dk = nn_dot(grads, q)
                if h == 0:
                    dv_all[sl, :] = dv
                    dk_all[sl, :] = dk
                else:
                    dv_all[sl, :] += dv
                    dk_all[sl, :] += dk
                piece = tn_dot(jnp.where(mine, keys, zero) * scale, grads)
                dqt = piece if dqt is None else dqt + piece
        dqt_all[:, :valid] = dqt
        dq_all[...] = dqt_all[...].T
        for c in range(count):
            size = min(rows, valid - c * rows)
            sl = slice(c * rows, c * rows + size)
            dqkv_ref[0, c, :size, lanes] = dq_all[sl, :].astype(BF16)
            dqkv_ref[1, c, :size, lanes] = dk_all[sl, :].astype(BF16)
            dqkv_ref[2, c, :size, lanes] = dv_all[sl, :].astype(BF16)

        @pl.when(p == 0)
        def _():
            for c in range(count):
                links.scatter_relay(b2_ref, relayed2, got2, 0, c)

        return carry

    lax.fori_loop(0, cols // 128, heads_pair, 0)
    for copy in own_q:
        copy.start()
    load.wait()

    def column_step(dist):
        def step(c):
            @pl.when(c == 0)
            def _():
                if dist == 0:
                    for copy in own_q:
                        copy.wait()
                column.spread(zq_ref, 0, dist)

        return step

    def input_grads(c):
        stream = c // (count - 1)
        mean, inv, centred = norm_stats([xp_ref[c, k].astype(F32) for k in range(4)], width)
        first = second = None
        for k in (3, 1, 2, 0):
            dm = None
            for j in range(3):
                piece = nt_dot(dqkv_ref[j, c], wq[stream, j, links.peers[k]])
                dm = piece if dm is None else dm + piece
            part[c, k] = dm.astype(BF16)
            dh = dm * (1.0 + mod_ref[k, pl.ds(stream * 6 + 1, 1), :])
            one = jnp.sum(dh, axis=-1, keepdims=True)
            two = jnp.sum(dh * centred[k], axis=-1, keepdims=True)
            first = one if first is None else first + one
            second = two if second is None else second + two
        srow[c] = stat_rows(first, second * inv)
        links.scatter_start(part, relayed, got, 3, c)
        links.rows_start(srow, sgot, 6, c)
        cols_s[c] = stat_cols(mean, inv)
        for j in range(3):
            bias_ref[c, j : j + 1, :] = jnp.sum(
                dqkv_ref[j, c].astype(F32), axis=0, keepdims=True
            )

    def last_relay(c):
        links.scatter_relay(part, relayed, got, 3, c)

    def out_stream(c):
        stream = c // (count - 1)
        total = links.scatter_finish(b2_ref, relayed2, got2, 0, c)
        add = total + db_ref[pl.ds(stream, 1), :]
        x2_ref[c] = x1_ref[c] + mod_ref[0, pl.ds(stream * 6 + 5, 1), :] * add
        line_ref[c, 2:3, :] = jnp.sum(add * cot_ref[c].astype(F32), axis=0, keepdims=True)

    def norm_back(c):
        stream = c // (count - 1)
        total = links.scatter_finish(part, relayed, got, 3, c)
        sums = exact_tn(links.rows_finish(srow, sgot, 6, c), eye_rows())
        mean, inv = cols_s[c, :, 0:1], cols_s[c, :, 1:2]
        normed = (xp_ref[c, 0].astype(F32) - mean) * inv
        grad = total * (1.0 + mod_ref[0, pl.ds(stream * 6 + 1, 1), :])
        grad_ref[c] = g1_ref[c] + inv * (
            grad - sums[:, 0:1] / width - normed * (sums[:, 1:2] / width)
        )
        line_ref[c, 0:1, :] = jnp.sum(total, axis=0, keepdims=True)
        line_ref[c, 1:2, :] = jnp.sum(total * normed, axis=0, keepdims=True)

    stages(
        count,
        [
            (1, last_relay),
            (0, column_step(0)),
            (2, column_step(1)),
            (4, column_step(2)),
            (0, input_grads),
            (2, norm_back),
            (1, out_stream),
        ],
    )
    column.spread(zq_ref, 0, chips - 1)
    column.spread_sent(zq_ref, 0)
    own_db.wait()
    column.deal_wait(db1_ref.at[text], zd_ref, 1, taken)
    for c in range(count):
        links.scatter_sent(b2_ref, relayed2, got2, 0, c)
        links.scatter_sent(part, relayed, got, 3, c)
        wait_sends(links.rows_copies(srow, sgot, 6, c))


def back_call(dp, valid, taken, qkv, o, do, lse, b2, x1, cot, g1, xp, mods, wq, down_b, db1):
    count, rows, feats = cot.shape
    cols = o.shape[-1]
    padded = -(-valid // 128) * 128
    step = -(-valid // 3 // 16) * 16
    blocks = [(b, min(step, valid - b)) for b in range(0, valid, step)]
    arrays = [qkv, o, do, lse, b2, x1, cot, g1, xp, mods, wq, down_b, db1]
    outs = [
        sds(qkv.shape, BF16),
        sds((count, rows, feats), F32),
        sds((count, rows, feats), F32),
        sds((count, 3, feats), F32),
        sds((count, 3, cols), F32),
        sds((dp // 2, 3, taken, cols), BF16),
        sds((dp // 2, taken, feats), BF16),
    ]
    n_in, n_out = len(arrays), len(outs)

    def kernel(*refs):
        back_kernel(dp // 2, valid, blocks, refs[:n_in], refs[n_in : n_in + n_out], refs[n_in + n_out :])

    return pl.pallas_call(
        kernel,
        out_shape=outs,
        in_specs=[VMEM] * 10 + [ANY, VMEM, ANY],
        out_specs=[VMEM] * (n_out - 2) + [ANY] * 2,
        scratch_shapes=[pltpu.VMEM(wq.shape, BF16)]
        + [pltpu.VMEM((valid, 128), BF16)] * 4
        + [pltpu.VMEM((valid, 128), F32)] * 4
        + [
            pltpu.VMEM((128, padded), F32),
            pltpu.VMEM((padded, 128), F32),
            pltpu.VMEM((count, 4, rows, feats), BF16),
            pltpu.VMEM((count, rows, feats), BF16),
            pltpu.VMEM((count, 3, rows, feats), BF16),
            pltpu.VMEM((count, rows, feats), BF16),
            pltpu.VMEM((count, 3, rows, feats), BF16),
            pltpu.VMEM((count, rows, 128), F32),
            pltpu.VMEM((count, 8, rows), F32),
            pltpu.VMEM((count, 3, 8, rows), F32),
            pltpu.SemaphoreType.DMA((5,)),
            pltpu.SemaphoreType.DMA((9, count)),
            pltpu.SemaphoreType.DMA((9, count)),
            pltpu.SemaphoreType.DMA((2, dp - 2)),
            pltpu.SemaphoreType.DMA((2, dp - 2)),
        ],
        compiler_params=pltpu.CompilerParams(
            collective_id=3, has_side_effects=True, vmem_limit_bytes=63 * MIB
        ),
        cost_estimate=cost(40 * 10**9, arrays, outs),
        name="back",
    )(*arrays)


def flat(value):
    return value.reshape((-1,) + value.shape[-1:])


def wgrad_kernel(pairs, split, t_ref, *refs):
    out_ref = refs[-1]
    slot = 0
    at = 0
    for groups in pairs:
        left, right = flat(refs[at][:, 0]), refs[at + 1]
        at += 2
        for j in range(groups):
            acc = tn_dot(left, flat(right[j] if groups > 1 else right[...]))
            size = acc.shape[0] // split
            for p in range(split):
                out_ref[p, slot] = acc[p * size : (p + 1) * size].astype(BF16)
            slot += 1


def wgrad_call(base, pairs, dp):
    count, _, rows, feats = pairs[0][0].shape
    chunks = count - 1
    cols = pairs[0][1].shape[-1]
    split = dp // 4
    groups = [right.shape[0] if right.ndim == 4 else 1 for _, right in pairs]
    slots = sum(groups)
    arrays, specs = [], []
    for (left, right), g in zip(pairs, groups):
        arrays += [left, right]
        specs.append(pl.BlockSpec((chunks, 1, rows, feats), lambda k, t: (0, k, 0, 0)))
        if g > 1:
            specs.append(pl.BlockSpec((g, chunks, rows, cols), lambda k, t: (0, 0, 0, 0)))
        else:
            specs.append(pl.BlockSpec((chunks, rows, cols), lambda k, t: (0, 0, 0)))
    out = sds((dp, slots, feats // split, cols), BF16)

    def kernel(*refs):
        wgrad_kernel(groups, split, *refs)

    return pl.pallas_call(
        kernel,
        out_shape=[out],
        grid_spec=pltpu.PrefetchScalarGridSpec(
            num_scalar_prefetch=1,
            grid=(4,),
            in_specs=specs,
            out_specs=[
                pl.BlockSpec(
                    (split, slots, feats // split, cols), lambda k, t: (t[0] ^ k, 0, 0, 0)
                )
            ],
        ),
        compiler_params=pltpu.CompilerParams(
            dimension_semantics=("arbitrary",), vmem_limit_bytes=48 * MIB
        ),
        cost_estimate=cost(2 * 4 * feats * slots * cols * chunks * rows, arrays, [out]),
    )(base, *arrays)[0]


def text_kernel(refs_in, refs_out, scratch):
    zm_ref, zl_ref, zd_ref, zq_ref, zr_ref, zo_ref = refs_in
    at_ref, ff_ref = refs_out
    send_a, got_a, send_f, got_f, keep_a, keep_f, send, recv = scratch
    index = lax.axis_index("dp")
    core = index % 2
    partner = index + 1 - 2 * core
    barrier = pltpu.get_barrier_semaphore()
    pl.semaphore_signal(barrier, inc=1, device_id={"dp": partner}, device_id_type=MESH)
    pl.semaphore_wait(barrier, 1)
    half = at_ref.shape[1]

    def move(src, dst, i):
        return pltpu.make_async_remote_copy(
            src_ref=src.at[i],
            dst_ref=dst.at[i],
            send_sem=send.at[i if src is send_a else 4 + i],
            recv_sem=recv.at[i if src is send_a else 4 + i],
            device_id={"dp": partner},
            device_id_type=MESH,
        )

    work = [
        (zl_ref.at[0], zr_ref.at[:, 0], keep_f, send_f, got_f, ff_ref, 0),
        (zl_ref.at[1], zr_ref.at[:, 1], keep_f, send_f, got_f, ff_ref, 1),
        (zm_ref, zq_ref.at[:, 0], keep_a, send_a, got_a, at_ref, 0),
        (zm_ref, zq_ref.at[:, 1], keep_a, send_a, got_a, at_ref, 1),
        (zm_ref, zq_ref.at[:, 2], keep_a, send_a, got_a, at_ref, 2),
        (zd_ref, zo_ref, keep_a, send_a, got_a, at_ref, 3),
    ]
    for left, right, keep, out, got, _, i in work:
        keep[i] = tn_dot(flat(left[...]), flat(right[...]))
        out[i] = keep[i, pl.ds((1 - core) * half, half), :].astype(BF16)
        move(out, got, i).start()
    for left, right, keep, out, got, final, i in work:
        move(out, got, i).wait_recv()
        final[i] = keep[i, pl.ds(core * half, half), :] + got[i].astype(F32)
    for left, right, keep, out, got, final, i in work:
        move(out, got, i).wait_send()


def text_call(zm, zl, zd, zq, zr, zo):
    feats, cols, hidden = zm.shape[-1], zq.shape[-1], zr.shape[-1]
    half = feats // 2
    arrays = [zm, zl, zd, zq, zr, zo]
    outs = [sds((4, half, cols), F32), sds((2, half, hidden), F32)]

    def kernel(*refs):
        text_kernel(refs[:6], refs[6:8], refs[8:])

    return pl.pallas_call(
        kernel,
        out_shape=outs,
        in_specs=[VMEM] * 6,
        out_specs=[VMEM] * 2,
        scratch_shapes=[
            pltpu.VMEM((4, half, cols), BF16),
            pltpu.VMEM((4, half, cols), BF16),
            pltpu.VMEM((2, half, hidden), BF16),
            pltpu.VMEM((2, half, hidden), BF16),
            pltpu.VMEM((4, feats, cols), F32),
            pltpu.VMEM((2, feats, hidden), F32),
            pltpu.SemaphoreType.DMA((6,)),
            pltpu.SemaphoreType.DMA((6,)),
        ],
        compiler_params=pltpu.CompilerParams(
            collective_id=4, has_side_effects=True, vmem_limit_bytes=40 * MIB
        ),
        cost_estimate=cost(6 * 10**9, arrays, outs),
        name="dw_text",
    )(*arrays)


def rows_kernel(dp, row_ref, all_ref, sum_ref, send, recv):
    mine = lax.axis_index("dp")
    others = [(mine + r) % dp for r in range(1, dp)]
    barrier = pltpu.get_barrier_semaphore()
    for peer in others:
        pl.semaphore_signal(barrier, inc=1, device_id={"dp": peer}, device_id_type=MESH)
    pl.semaphore_wait(barrier, dp - 1)
    copies = [
        pltpu.make_async_remote_copy(
            src_ref=row_ref,
            dst_ref=all_ref.at[mine],
            send_sem=send.at[r],
            recv_sem=recv.at[r],
            device_id={"dp": peer},
            device_id_type=MESH,
        )
        for r, peer in enumerate(others)
    ]
    for copy in copies:
        copy.start()
    all_ref[mine] = row_ref[...]
    for copy in copies:
        copy.wait()
    total = all_ref[0]
    for s in range(1, dp):
        total = total + all_ref[s]
    sum_ref[...] = total


def rows_call(dp, rows):
    outs = [sds((dp,) + rows.shape, F32), sds(rows.shape, F32)]
    return pl.pallas_call(
        functools.partial(rows_kernel, dp),
        out_shape=outs,
        in_specs=[VMEM],
        out_specs=[VMEM] * 2,
        scratch_shapes=[
            pltpu.SemaphoreType.DMA((dp - 1,)),
            pltpu.SemaphoreType.DMA((dp - 1,)),
        ],
        compiler_params=pltpu.CompilerParams(
            collective_id=5, has_side_effects=True, vmem_limit_bytes=16 * MIB
        ),
        cost_estimate=cost(10**6, [rows], outs),
        name="rows",
    )(rows)


def fast_body(
    dp,
    image_in,
    text_in,
    cond_in,
    mod_weight,
    mod_bias,
    qkv_weight,
    qkv_bias,
    out_weight,
    out_bias,
    up_weight,
    up_bias,
    down_weight,
    down_bias,
    image_cot,
    text_cot,
):
    base = lax.axis_index("tensor").astype(jnp.int32).reshape(1)
    feats = image_in.shape[2]
    images, texts = image_in.shape[1], text_in.shape[1]
    rows = images // 4
    valid = images + texts

    def join(image, text):
        padded = jnp.pad(text[0], ((0, rows - texts), (0, 0)))
        return jnp.concatenate([image[0].reshape(4, rows, feats), padded[None]], axis=0)

    def parted(value):
        image = value[:4].reshape(1, images, feats)
        return image, value[4:, :texts]

    x, cot = join(image_in, text_in), join(image_cot, text_cot)
    cond_float = cond_in.astype(F32)
    cond_act = jax.nn.silu(cond_float).astype(BF16)
    mod_w = jnp.transpose(mod_weight[0], (0, 2, 1, 3)).reshape(12, -1, feats)
    mod_b = mod_bias[0].reshape(12, feats).astype(F32)
    qkv_w = jnp.transpose(qkv_weight[0], (0, 2, 1, 3))
    qkv_w = qkv_w.reshape(2, 3, 4, feats, qkv_w.shape[-1])
    out_w = out_weight[0].reshape(2, 4, feats, -1)
    up_w = up_weight[0].reshape(2, 4, feats, -1)
    down_w = down_weight[0].reshape(2, 4, feats, -1)

    taken = -(-texts // 16) * 16
    m, qkv, o, lse, db2, xp, mods, db2_sum, zm = front_call(
        dp, valid, taken, x, cot, cond_act, mod_w, mod_b, qkv_w, qkv_bias[0].astype(F32)
    )
    up_b, out_b, down_b = (b[0].astype(F32) for b in (up_bias, out_bias, down_bias))
    x1, m2, act, du, b2, g1, db1, do, lines2, du_sum, zr, zl, zo = middle_call(
        dp, taken, o, x, cot, db2, mods, out_w, up_w, down_w, up_b, out_b
    )
    part = wgrad_call(base, [(m2, du), (db2, act)], dp)
    do, part = lax.optimization_barrier((do, part))
    ff_sum = lax.psum_scatter(part, "dp", scatter_dimension=0, tiled=True)
    dqkv, x2, grad, lines1, qkv_sum, zq, zd = back_call(
        dp, valid, taken, qkv, o, do, lse, b2, x1, cot, g1, xp, mods, qkv_w, down_b, db1
    )
    part2 = wgrad_call(base, [(m, dqkv), (db1, o)], dp)
    part2, zq = lax.optimization_barrier((part2, zq))
    at_sum = lax.psum_scatter(part2, "dp", scatter_dimension=0, tiled=True)
    at_text, ff_text = text_call(zm, zl, zd, zq, zr, zo)

    def by_stream(value):
        return jnp.stack([jnp.sum(value[:4], axis=0), value[4]])

    late, early = by_stream(lines1), by_stream(lines2)
    mod_rows = jnp.stack(
        [late[:, 0], late[:, 1], early[:, 2], early[:, 0], early[:, 1], late[:, 2]], axis=1
    )
    mod_rows = mod_rows.reshape(12, feats).astype(BF16).astype(F32)
    every = [
        mod_rows,
        by_stream(qkv_sum).reshape(6, feats),
        early[:, 3],
        by_stream(du_sum).reshape(8, feats),
        by_stream(db2_sum),
        jnp.zeros((2, feats), F32),
    ]
    all_rows, row_sums = rows_call(dp, jnp.concatenate(every, axis=0))
    all_mod = all_rows[:, :12].astype(BF16)
    mod_wgrad = jnp.einsum("sc,sgd->gcd", cond_act, all_mod, preferred_element_type=F32)
    mod_wgrad = jnp.transpose(mod_wgrad.reshape(1, 2, 6, -1, feats), (0, 1, 3, 2, 4))
    act_part = jnp.einsum("sgd,gcd->sc", all_mod, mod_w, preferred_element_type=F32)
    act_total = act_part + sum(
        lax.ppermute(act_part, "tensor", [(i, i ^ k) for i in range(4)]) for k in (1, 2, 3)
    )
    cond_grad = jax.vjp(jax.nn.silu, cond_float)[1](act_total)[0]
    mod_bgrad = row_sums[:12].reshape(1, 2, 6, feats)
    biases = (
        row_sums[12:18].reshape(1, 2, 3, feats),
        row_sums[18:20][None],
        row_sums[20:28].reshape(1, 2, 4 * feats),
        row_sums[28:30][None],
    )
    at_image, ff_image = at_sum[0].astype(F32), ff_sum[0].astype(F32)
    qkv_wgrad = jnp.transpose(jnp.stack([at_image[:3], at_text[:3]])[None], (0, 1, 3, 2, 4))

    def streams(image, text):
        return jnp.stack([image, text])[None]

    image_out, text_out = parted(x2)
    image_grad, text_grad = parted(grad)
    return (
        image_out,
        text_out,
        image_grad,
        text_grad,
        cond_grad,
        mod_wgrad,
        mod_bgrad,
        qkv_wgrad,
        biases[0],
        streams(at_image[3], at_text[3]),
        biases[1],
        streams(ff_image[0], ff_text[0]),
        biases[2],
        streams(ff_image[1], ff_text[1]),
        biases[3],
    )


def solution(mesh):
    dp, tensor = mesh.shape["dp"], mesh.shape["tensor"]
    square = dp == 8 and tensor == 4
    chosen = functools.partial(fast_body, dp) if square else plain_body
    return jax.shard_map(
        chosen,
        mesh=mesh,
        in_specs=(
            P("dp", None, "tensor"),
            P("dp", None, "tensor"),
            P(None, "dp"),
            P(None, None, "dp", None, "tensor"),
            P(None, None, None, "tensor"),
            P(None, None, None, None, "tensor"),
            P(None, None, None, "tensor"),
            P(None, None, None, "tensor"),
            P(None, None, "tensor"),
            P(None, None, None, "tensor"),
            P(None, None, "tensor"),
            P(None, None, None, "tensor"),
            P(None, None, "tensor"),
            P("dp", None, "tensor"),
            P("dp", None, "tensor"),
        ),
        out_specs=(
            P("dp", None, "tensor"),
            P("dp", None, "tensor"),
            P("dp", None, "tensor"),
            P("dp", None, "tensor"),
            P(None, "dp"),
            P(None, None, "dp", None, "tensor"),
            P(None, None, None, "tensor"),
            P(None, None, "dp", None, "tensor"),
            P(None, None, None, "tensor"),
            P(None, None, "dp", "tensor"),
            P(None, None, "tensor"),
            P(None, None, "dp", "tensor"),
            P(None, None, "tensor"),
            P(None, None, "dp", "tensor"),
            P(None, None, "tensor"),
        ),
        check_vma=False,
    )
```

```python
import functools

import jax
import jax.numpy as jnp
from jax import lax
from jax.experimental import pallas as pl
from jax.experimental.pallas import tpu as pltpu
from jax.sharding import PartitionSpec as P

HEAD_DIM = 64
EPS = 1e-06
F32 = jnp.float32
BF16 = jnp.bfloat16
GELU_C = 0.7978845608028654
GELU_K = 0.044715
MIB = 1 << 20
MESH = pl.DeviceIdType.MESH
VMEM = pl.BlockSpec(memory_space=pltpu.VMEM)
ANY = pl.BlockSpec(memory_space=pl.ANY)


eps_norm = 1e-06


def gelu_tanh(values):
    return jax.nn.gelu(values, approximate=True)


def share_of(whole_row, offset, share_width):
    return lax.dynamic_slice_in_dim(whole_row, offset, share_width, whole_row.ndim - 1)


def norm_forward(shards, shifts, scales):
    saved_norm = []
    gathered = (
        lax.all_gather(shards[0].astype(jnp.bfloat16), "tensor", axis=2, tiled=True).astype(
            jnp.float32
        ),
        lax.all_gather(shards[1].astype(jnp.bfloat16), "tensor", axis=2, tiled=True).astype(
            jnp.float32
        ),
    )
    moddeds = []
    for stream in range(2):
        row_mean = jnp.mean(gathered[stream], axis=-1, keepdims=True)
        centred = gathered[stream] - row_mean
        inv_std = lax.rsqrt(jnp.mean(centred * centred, axis=-1, keepdims=True) + eps_norm)
        normed = centred * inv_std
        moddeds.append(
            (normed * (1.0 + scales[stream][:, None, :]) + shifts[stream][:, None, :]).astype(
                jnp.bfloat16
            )
        )
        saved_norm.append((normed, inv_std))
    return (moddeds, saved_norm)


def norm_backward(partials, saved_norm, scales, offset, share_width):
    results = []
    totals = (
        lax.psum(partials[0].astype(jnp.bfloat16), "tensor").astype(jnp.float32),
        lax.psum(partials[1].astype(jnp.bfloat16), "tensor").astype(jnp.float32),
    )
    for stream in range(2):
        normed, inv_std = saved_norm[stream]
        grad_normed = totals[stream] * (1.0 + scales[stream][:, None, :])
        mean_grad = jnp.mean(grad_normed, axis=-1, keepdims=True)
        mean_cross = jnp.mean(grad_normed * normed, axis=-1, keepdims=True)
        local_total = share_of(totals[stream], offset, share_width)
        local_normed = share_of(normed, offset, share_width)
        local_grad = share_of(grad_normed, offset, share_width)
        results.append(
            (
                inv_std * (local_grad - mean_grad - local_normed * mean_cross),
                jnp.sum(local_total, axis=1),
                jnp.sum(local_total * local_normed, axis=1),
            )
        )
    return results


def reduce_branches(partials):
    return (
        lax.psum_scatter(
            partials[0].astype(jnp.bfloat16), "tensor", scatter_dimension=2, tiled=True
        ).astype(jnp.float32),
        lax.psum_scatter(
            partials[1].astype(jnp.bfloat16), "tensor", scatter_dimension=2, tiled=True
        ).astype(jnp.float32),
    )


def gather_grads(branch_grads):
    return (
        lax.all_gather(branch_grads[0], "tensor", axis=2, tiled=True),
        lax.all_gather(branch_grads[1], "tensor", axis=2, tiled=True),
    )


def attend(joint_qkv, heads_here, score_scale):
    seq_count, tokens = (joint_qkv.shape[0], joint_qkv.shape[1])
    separated = joint_qkv.reshape(seq_count, tokens, 3, heads_here, HEAD_DIM)
    scores = (
        jnp.einsum(
            "sqhd,skhd->shqk",
            separated[:, :, 0],
            separated[:, :, 1],
            preferred_element_type=jnp.float32,
        )
        * score_scale
    )
    highest_score = jnp.max(scores, axis=-1, keepdims=True)
    raised = jnp.exp(scores - highest_score)
    denominator = jnp.sum(raised, axis=-1, keepdims=True)
    weights = (raised / denominator).astype(jnp.bfloat16)
    mixed_heads = jnp.einsum(
        "shqk,skhd->sqhd", weights, separated[:, :, 2], preferred_element_type=jnp.float32
    )
    return (
        mixed_heads.astype(jnp.bfloat16).reshape(seq_count, tokens, heads_here * HEAD_DIM),
        highest_score + jnp.log(denominator),
    )


def attend_back(joint_qkv, log_total, head_grads, heads_here, score_scale):
    seq_count, tokens = (joint_qkv.shape[0], joint_qkv.shape[1])
    separated = joint_qkv.reshape(seq_count, tokens, 3, heads_here, HEAD_DIM)
    queries, keys_all, values = (separated[:, :, 0], separated[:, :, 1], separated[:, :, 2])
    outgrad = head_grads.reshape(seq_count, tokens, heads_here, HEAD_DIM)
    scores = (
        jnp.einsum("sqhd,skhd->shqk", queries, keys_all, preferred_element_type=jnp.float32)
        * score_scale
    )
    weights = jnp.exp(scores - log_total)
    weight_grad = jnp.einsum("sqhd,skhd->shqk", outgrad, values, preferred_element_type=jnp.float32)
    row_dot = jnp.sum(weights * weight_grad, axis=-1, keepdims=True)
    score_grad = (weights * (weight_grad - row_dot)).astype(jnp.bfloat16)
    query_grad = (
        jnp.einsum("shqk,skhd->sqhd", score_grad, keys_all, preferred_element_type=jnp.float32)
        * score_scale
    )
    key_grad = (
        jnp.einsum("shqk,sqhd->skhd", score_grad, queries, preferred_element_type=jnp.float32)
        * score_scale
    )
    value_grad = jnp.einsum(
        "shqk,sqhd->skhd", weights.astype(jnp.bfloat16), outgrad, preferred_element_type=jnp.float32
    )
    stacked = jnp.stack([query_grad, key_grad, value_grad], axis=2)
    return stacked.reshape(seq_count, tokens, 3, heads_here * HEAD_DIM).astype(jnp.bfloat16)


def plain_body(
    image_in,
    text_in,
    cond_in,
    mod_weight,
    mod_bias,
    qkv_weight,
    qkv_bias,
    out_weight,
    out_bias,
    up_weight,
    up_bias,
    down_weight,
    down_bias,
    image_cot,
    text_cot,
):
    share_width = image_in.shape[2]
    offset = lax.axis_index("tensor") * share_width
    heads_here = qkv_weight.shape[4] // HEAD_DIM
    score_scale = HEAD_DIM ** (-0.5)
    image_rows = image_in.shape[1]
    layer_count = qkv_weight.shape[0]
    cond_float = cond_in.astype(jnp.float32)
    cond_act = jax.nn.silu(cond_float).astype(jnp.bfloat16)
    mod_terms = jnp.einsum(
        "sc,lxcjd->slxjd", cond_act, mod_weight, preferred_element_type=jnp.float32
    )
    modulation = lax.psum_scatter(
        mod_terms, "dp", scatter_dimension=0, tiled=True
    ) + mod_bias.astype(jnp.float32)
    mod_view = lax.all_gather(modulation, "tensor", axis=4, tiled=True)
    residual = [image_in.astype(jnp.float32), text_in.astype(jnp.float32)]
    layer_at = 0
    moddeds, first_norm = norm_forward(
        residual,
        [mod_view[:, layer_at, stream, 0] for stream in range(2)],
        [mod_view[:, layer_at, stream, 1] for stream in range(2)],
    )
    projected = [
        (
            jnp.einsum(
                "snd,dje->snje",
                moddeds[stream],
                qkv_weight[layer_at, stream],
                preferred_element_type=jnp.float32,
            )
            + qkv_bias[layer_at, stream]
        ).astype(jnp.bfloat16)
        for stream in range(2)
    ]
    joint_qkv = jnp.concatenate(projected, axis=1)
    attended, log_total = attend(joint_qkv, heads_here, score_scale)
    pieces = [attended[:, :image_rows], attended[:, image_rows:]]
    summed = reduce_branches(
        [
            jnp.einsum(
                "puj,oj->puo",
                pieces[stream],
                out_weight[layer_at, stream],
                preferred_element_type=jnp.float32,
            )
            for stream in range(2)
        ]
    )
    first_branch = [summed[stream] + out_bias[layer_at, stream] for stream in range(2)]
    residual = [
        residual[stream] + modulation[:, layer_at, stream, 2][:, None, :] * first_branch[stream]
        for stream in range(2)
    ]
    second_mod, second_norm = norm_forward(
        residual,
        [mod_view[:, layer_at, stream, 3] for stream in range(2)],
        [mod_view[:, layer_at, stream, 4] for stream in range(2)],
    )
    hidden = [
        jnp.einsum(
            "snd,df->snf",
            second_mod[stream],
            up_weight[layer_at, stream],
            preferred_element_type=jnp.float32,
        )
        + up_bias[layer_at, stream]
        for stream in range(2)
    ]
    activated = [gelu_tanh(hidden[stream]).astype(jnp.bfloat16) for stream in range(2)]
    summed = reduce_branches(
        [
            jnp.einsum(
                "snf,df->snd",
                activated[stream],
                down_weight[layer_at, stream],
                preferred_element_type=jnp.float32,
            )
            for stream in range(2)
        ]
    )
    second_branch = [summed[stream] + down_bias[layer_at, stream] for stream in range(2)]
    residual = [
        residual[stream] + modulation[:, layer_at, stream, 5][:, None, :] * second_branch[stream]
        for stream in range(2)
    ]
    forward_saved = [
        (
            moddeds,
            first_norm,
            joint_qkv,
            attended,
            log_total,
            first_branch,
            second_mod,
            second_norm,
            hidden,
            activated,
            second_branch,
        )
    ]
    gradients = [image_cot.astype(jnp.float32), text_cot.astype(jnp.float32)]
    mod_parts = [None] * layer_count
    weight_parts = [None] * layer_count
    bias_parts = [None] * layer_count
    for layer_at in reversed(range(layer_count)):
        (
            moddeds,
            first_norm,
            joint_qkv,
            attended,
            log_total,
            first_branch,
            second_mod,
            second_norm,
            hidden,
            activated,
            second_branch,
        ) = forward_saved[layer_at]
        second_gate = [
            jnp.sum(second_branch[stream] * gradients[stream], axis=1) for stream in range(2)
        ]
        branch_grads = [
            (modulation[:, layer_at, stream, 5][:, None, :] * gradients[stream]).astype(
                jnp.bfloat16
            )
            for stream in range(2)
        ]
        down_bias_grad = [
            jnp.sum(branch_grads[stream].astype(jnp.float32), axis=(0, 1)) for stream in range(2)
        ]
        whole_grads = gather_grads(branch_grads)
        down_grad = [
            jnp.einsum(
                "snd,snf->df",
                whole_grads[stream],
                activated[stream],
                preferred_element_type=jnp.float32,
            )
            for stream in range(2)
        ]
        act_grad = [
            jnp.einsum(
                "snd,df->snf",
                whole_grads[stream],
                down_weight[layer_at, stream],
                preferred_element_type=jnp.float32,
            )
            for stream in range(2)
        ]
        hidden_grad = [
            jax.vjp(gelu_tanh, hidden[stream])[1](act_grad[stream])[0].astype(jnp.bfloat16)
            for stream in range(2)
        ]
        up_bias_grad = [
            jnp.sum(hidden_grad[stream].astype(jnp.float32), axis=(0, 1)) for stream in range(2)
        ]
        up_grad = [
            jnp.einsum(
                "snd,snf->df",
                second_mod[stream],
                hidden_grad[stream],
                preferred_element_type=jnp.float32,
            )
            for stream in range(2)
        ]
        norm_partials = [
            jnp.einsum(
                "snf,df->snd",
                hidden_grad[stream],
                up_weight[layer_at, stream],
                preferred_element_type=jnp.float32,
            )
            for stream in range(2)
        ]
        second_back = norm_backward(
            norm_partials,
            second_norm,
            [mod_view[:, layer_at, stream, 4] for stream in range(2)],
            offset,
            share_width,
        )
        gradients = [gradients[stream] + second_back[stream][0] for stream in range(2)]
        first_gate = [
            jnp.sum(first_branch[stream] * gradients[stream], axis=1) for stream in range(2)
        ]
        branch_grads = [
            (modulation[:, layer_at, stream, 2][:, None, :] * gradients[stream]).astype(
                jnp.bfloat16
            )
            for stream in range(2)
        ]
        out_bias_grad = [
            jnp.sum(branch_grads[stream].astype(jnp.float32), axis=(0, 1)) for stream in range(2)
        ]
        whole_grads = gather_grads(branch_grads)
        pieces = [attended[:, :image_rows], attended[:, image_rows:]]
        out_grad = [
            jnp.einsum(
                "kux,kut->xt",
                whole_grads[stream],
                pieces[stream],
                preferred_element_type=jnp.float32,
            )
            for stream in range(2)
        ]
        head_grads = jnp.concatenate(
            [
                jnp.einsum(
                    "hom,mr->hor",
                    whole_grads[stream],
                    out_weight[layer_at, stream],
                    preferred_element_type=jnp.float32,
                )
                for stream in range(2)
            ],
            axis=1,
        ).astype(jnp.bfloat16)
        joint_grad = attend_back(joint_qkv, log_total, head_grads, heads_here, score_scale)
        stream_grads = [joint_grad[:, :image_rows], joint_grad[:, image_rows:]]
        qkv_bias_grad = [
            jnp.sum(stream_grads[stream].astype(jnp.float32), axis=(0, 1)) for stream in range(2)
        ]
        qkv_grad = [
            jnp.einsum(
                "snd,snje->dje",
                moddeds[stream],
                stream_grads[stream],
                preferred_element_type=jnp.float32,
            )
            for stream in range(2)
        ]
        norm_partials = [
            jnp.einsum(
                "snje,dje->snd",
                stream_grads[stream],
                qkv_weight[layer_at, stream],
                preferred_element_type=jnp.float32,
            )
            for stream in range(2)
        ]
        first_back = norm_backward(
            norm_partials,
            first_norm,
            [mod_view[:, layer_at, stream, 1] for stream in range(2)],
            offset,
            share_width,
        )
        gradients = [gradients[stream] + first_back[stream][0] for stream in range(2)]
        mod_parts[layer_at] = jnp.stack(
            [
                jnp.stack(
                    [
                        first_back[stream][1],
                        first_back[stream][2],
                        first_gate[stream],
                        second_back[stream][1],
                        second_back[stream][2],
                        second_gate[stream],
                    ],
                    axis=1,
                )
                for stream in range(2)
            ],
            axis=1,
        )
        bias_parts[layer_at] = (
            jnp.stack(qkv_bias_grad, axis=0),
            jnp.stack(out_bias_grad, axis=0),
            jnp.stack(up_bias_grad, axis=0),
            jnp.stack(down_bias_grad, axis=0),
        )
        weight_parts[layer_at] = (
            jnp.stack(qkv_grad, axis=0),
            jnp.stack(out_grad, axis=0),
            jnp.stack(up_grad, axis=0),
            jnp.stack(down_grad, axis=0),
        )
    reduced = (
        lax.psum_scatter(
            jnp.stack([weight_parts[0][0]], axis=0).astype(jnp.bfloat16),
            "dp",
            scatter_dimension=2,
            tiled=True,
        ).astype(jnp.float32),
        lax.psum_scatter(
            jnp.stack([weight_parts[0][1]], axis=0).astype(jnp.bfloat16),
            "dp",
            scatter_dimension=2,
            tiled=True,
        ).astype(jnp.float32),
        lax.psum_scatter(
            jnp.stack([weight_parts[0][2]], axis=0).astype(jnp.bfloat16),
            "dp",
            scatter_dimension=2,
            tiled=True,
        ).astype(jnp.float32),
        lax.psum_scatter(
            jnp.stack([weight_parts[0][3]], axis=0).astype(jnp.bfloat16),
            "dp",
            scatter_dimension=2,
            tiled=True,
        ).astype(jnp.float32),
    )
    bias_totals = lax.psum(
        (
            jnp.stack([bias_parts[0][0]], axis=0),
            jnp.stack([bias_parts[0][1]], axis=0),
            jnp.stack([bias_parts[0][2]], axis=0),
            jnp.stack([bias_parts[0][3]], axis=0),
        ),
        "dp",
    )
    mod_grad = jnp.stack(mod_parts, axis=1).astype(jnp.bfloat16)
    all_mod = lax.all_gather(mod_grad, "dp", axis=0, tiled=True)
    mod_wgrad = jnp.einsum("sc,slxjd->lxcjd", cond_act, all_mod, preferred_element_type=jnp.float32)
    mod_bgrad = jnp.sum(all_mod.astype(jnp.float32), axis=0)
    act_partial = jnp.einsum(
        "slxjd,lxcjd->sc", all_mod, mod_weight, preferred_element_type=jnp.float32
    )
    act_total = lax.psum(act_partial, "tensor")
    cond_grad = jax.vjp(jax.nn.silu, cond_float)[1](act_total)[0]
    return (
        residual[0],
        residual[1],
        gradients[0],
        gradients[1],
        cond_grad,
        mod_wgrad,
        mod_bgrad,
        reduced[0],
        bias_totals[0],
        reduced[1],
        bias_totals[1],
        reduced[2],
        bias_totals[2],
        reduced[3],
        bias_totals[3],
    )


def nt_dot(a, b):
    return lax.dot_general(a, b, (((1,), (1,)), ((), ())), preferred_element_type=F32)


def nn_dot(a, b):
    return lax.dot_general(a, b, (((1,), (0,)), ((), ())), preferred_element_type=F32)


def tn_dot(a, b):
    return lax.dot_general(a, b, (((0,), (0,)), ((), ())), preferred_element_type=F32)


def exact_nt(a, b):
    return lax.dot_general(
        a, b, (((1,), (1,)), ((), ())), preferred_element_type=F32, precision=lax.Precision.HIGHEST
    )


def exact_tn(a, b):
    return lax.dot_general(
        a, b, (((0,), (0,)), ((), ())), preferred_element_type=F32, precision=lax.Precision.HIGHEST
    )


def sds(shape, dtype):
    return jax.ShapeDtypeStruct(shape, dtype)


def cost(flops, arrays, outs):
    moved = sum(a.size * a.dtype.itemsize for a in arrays)
    moved += sum(o.size * o.dtype.itemsize for o in outs)
    return pl.CostEstimate(flops=flops, bytes_accessed=moved, transcendentals=0)


def eye_rows():
    return (
        lax.broadcasted_iota(jnp.int32, (8, 128), 0) == lax.broadcasted_iota(jnp.int32, (8, 128), 1)
    ).astype(F32)


def norm_stats(pieces, width):
    total = sum(jnp.sum(p, axis=-1, keepdims=True) for p in pieces)
    mean = total / width
    centred = [p - mean for p in pieces]
    var = sum(jnp.sum(c * c, axis=-1, keepdims=True) for c in centred) / width
    return mean, lax.rsqrt(var + EPS), centred


def stat_rows(first, second):
    lane = lax.broadcasted_iota(jnp.int32, (first.shape[0], 128), 1)
    both = jnp.where(lane == 0, first, jnp.where(lane == 1, second, 0.0))
    return exact_nt(eye_rows(), both)


def stat_cols(first, second):
    lane = lax.broadcasted_iota(jnp.int32, (first.shape[0], 128), 1)
    return jnp.where(lane == 0, first, jnp.where(lane == 1, second, 0.0))


class Links:
    def __init__(self, send, recv, text, rows, taken):
        self.send_sem, self.recv_sem = send, recv
        self.text, self.rows, self.taken = text, rows, taken
        me = lax.axis_index("tensor")
        self.peers = [me, me + 1 - 2 * (me % 2), (me + 2) % 4, 3 - me]

    def enter(self, extra=()):
        barrier = pltpu.get_barrier_semaphore()
        for peer in self.peers[1:]:
            pl.semaphore_signal(barrier, inc=1, device_id={"tensor": peer}, device_id_type=MESH)
        for peer in extra:
            pl.semaphore_signal(barrier, inc=1, device_id={"dp": peer}, device_id_type=MESH)
        pl.semaphore_wait(barrier, 3 + len(extra))

    def copy(self, src, dst, kind, c, peer):
        return pltpu.make_async_remote_copy(
            src_ref=src,
            dst_ref=dst,
            send_sem=self.send_sem.at[kind, c],
            recv_sem=self.recv_sem.at[kind, c],
            device_id={"tensor": peer},
            device_id_type=MESH,
        )

    def route(self, c):
        odd = c % 2
        first = self.peers[1] * (1 - odd) + self.peers[2] * odd
        second = self.peers[2] * (1 - odd) + self.peers[1] * odd
        return 1 + odd, 2 - odd, first, second

    def act(self, action, copy, i, *args):
        c = args[-1]
        if isinstance(c, int):
            getattr(copy(i, self.taken if c == self.text else self.rows, *args), action)()
            return

        @pl.when(c == self.text)
        def _():
            getattr(copy(i, self.taken, *args), action)()

        @pl.when(c != self.text)
        def _():
            getattr(copy(i, self.rows, *args), action)()

    def clear(self, *views):
        for view in views:
            view[self.taken :, :] = jnp.zeros((self.rows - self.taken, view.shape[-1]), BF16)

    def gather_copy(self, i, rows, src, buf, kind, c):
        near, far, first, second = self.route(c)
        some = pl.ds(0, rows)
        if i == 0:
            return self.copy(src.at[some, :], buf.at[c, near, some, :], kind, c, first)
        if i == 1:
            return self.copy(src.at[some, :], buf.at[c, far, some, :], kind + 1, c, second)
        return self.copy(buf.at[c, near, some, :], buf.at[c, 3, some, :], kind + 2, c, second)

    def gather_start(self, *args):
        self.act("start", self.gather_copy, 0, *args)
        self.act("start", self.gather_copy, 1, *args)

    def gather_relay(self, *args):
        self.act("wait_recv", self.gather_copy, 0, *args)
        self.act("start", self.gather_copy, 2, *args)

    def gather_finish(self, *args):
        self.act("wait_recv", self.gather_copy, 1, *args)
        self.act("wait_recv", self.gather_copy, 2, *args)

    def gather_sent(self, *args):
        for i in range(3):
            self.act("wait_send", self.gather_copy, i, *args)

    def scatter_copy(self, i, rows, part, relayed, got, kind, c):
        near, _, first, second = self.route(c)
        some = pl.ds(0, rows)
        if i == 0:
            return self.copy(part.at[c, 3, some, :], got.at[c, 0, some, :], kind, c, first)
        if i == 1:
            return self.copy(part.at[c, near, some, :], got.at[c, 1, some, :], kind + 1, c, first)
        return self.copy(relayed.at[c, some, :], got.at[c, 2, some, :], kind + 2, c, second)

    def scatter_start(self, *args):
        self.act("start", self.scatter_copy, 0, *args)
        self.act("start", self.scatter_copy, 1, *args)

    def scatter_relay(self, part, relayed, got, kind, c):
        args = (part, relayed, got, kind, c)
        self.act("wait_recv", self.scatter_copy, 0, *args)
        _, far, _, _ = self.route(c)
        relayed[c] = (part[c, far].astype(F32) + got[c, 0].astype(F32)).astype(BF16)
        self.act("start", self.scatter_copy, 2, *args)

    def scatter_sent(self, *args):
        for i in range(3):
            self.act("wait_send", self.scatter_copy, i, *args)

    def scatter_finish(self, part, relayed, got, kind, c):
        args = (part, relayed, got, kind, c)
        self.act("wait_recv", self.scatter_copy, 1, *args)
        self.act("wait_recv", self.scatter_copy, 2, *args)
        return part[c, 0].astype(F32) + got[c, 1].astype(F32) + got[c, 2].astype(F32)

    def rows_copies(self, src, dst, kind, c):
        return [
            self.copy(src.at[c], dst.at[c, k - 1], kind + k - 1, c, self.peers[k]) for k in (1, 2, 3)
        ]

    def rows_start(self, src, dst, kind, c):
        for copy in self.rows_copies(src, dst, kind, c):
            copy.start()

    def rows_finish(self, src, dst, kind, c):
        for copy in self.rows_copies(src, dst, kind, c):
            copy.wait_recv()
        return src[c] + dst[c, 0] + dst[c, 1] + dst[c, 2]


class Column:
    def __init__(self, chips, send, recv):
        index = lax.axis_index("dp")
        self.chips, self.z, self.core = chips, index // 2, index % 2
        self.send_sem, self.recv_sem = send, recv
        self.others = [((self.z + r) % chips) * 2 + self.core for r in range(1, chips)]

    def copy(self, src, dst, kind, i, chip):
        return pltpu.make_async_remote_copy(
            src_ref=src,
            dst_ref=dst,
            send_sem=self.send_sem.at[kind, i],
            recv_sem=self.recv_sem.at[kind, i],
            device_id={"dp": chip * 2 + self.core},
            device_id_type=MESH,
        )

    def hop(self, buf, kind, dist, way, behind):
        step = 1 - 2 * way
        origin = self.z - step * (dist + behind)
        block = buf.at[origin]
        return self.copy(block, block, kind, 2 * dist + way, self.z + step * (1 - behind))

    def sends(self, dist, way):
        if way == 0:
            return (self.z >= dist) & (self.z < self.chips - 1)
        return (self.z < self.chips - dist) & (self.z > 0)

    def receives(self, dist, way):
        return self.z > dist if way == 0 else self.z < self.chips - 1 - dist

    def spread(self, buf, kind, dist):
        for way in (0, 1):
            if dist:

                @pl.when(self.receives(dist - 1, way))
                def _():
                    self.hop(buf, kind, dist - 1, way, 1).wait_recv()

            if dist < self.chips - 1:

                @pl.when(self.sends(dist, way))
                def _():
                    self.hop(buf, kind, dist, way, 0).start()

    def spread_sent(self, buf, kind):
        for dist in range(self.chips - 1):
            for way in (0, 1):

                @pl.when(self.sends(dist, way))
                def _():
                    self.hop(buf, kind, dist, way, 0).wait_send()

    def block_of(self, chip):
        me = lax.axis_index("tensor")
        return (chip % 2 + me % 2) % 2 + 2 * ((chip // 2 + me // 2) % 2)

    def deal_copy(self, blocks, buf, kind, r, taken):
        chip = (self.z + r) % self.chips
        src = blocks.at[self.block_of(chip), pl.ds(0, taken), :]
        return self.copy(src, buf.at[self.z], kind, r - 1, chip)

    def deal(self, blocks, buf, kind, taken):
        for r in range(1, self.chips):
            self.deal_copy(blocks, buf, kind, r, taken).start()

    def deal_own(self, blocks, buf, sem, taken):
        src = blocks.at[self.block_of(self.z), pl.ds(0, taken), :]
        return pltpu.make_async_copy(src, buf.at[self.z], sem)

    def deal_wait(self, blocks, buf, kind, taken):
        for r in range(1, self.chips):
            self.deal_copy(blocks, buf, kind, r, taken).wait()


def wait_sends(copies):
    for copy in copies:
        copy.wait_send()


def stages(count, steps):
    last = max(offset for offset, _ in steps)

    def tick(t, carry):
        for offset, step in steps:
            c = t - offset

            @pl.when((c >= 0) & (c < count))
            def _():
                step(c)

        return carry

    lax.fori_loop(0, count + last, tick, 0)


def front_kernel(dp, valid, refs_in, refs_out, scratch):
    x_ref, cot_ref, act_ref, modw_ref, modb_ref, wq_ref, bq_ref = refs_in
    m_ref, qkv_ref, o_ref, lse_ref, g_ref, xp_ref, mod_ref, gsum_ref, zm_ref = refs_out
    modw, wq, terms, got, k_all, aug, local, send, recv, msend, mrecv, zsend, zrecv = scratch
    count, rows, feats = x_ref.shape
    cols = qkv_ref.shape[-1]
    width = 4 * feats
    taken = zm_ref.shape[1]
    text = count - 1
    links = Links(send, recv, text, rows, taken)
    column = Column(dp // 2, zsend, zrecv)
    mine = lax.axis_index("dp")
    others = [(mine + r) % dp for r in range(1, dp)]
    load_mod = pltpu.make_async_copy(modw_ref, modw, local.at[0])
    load_wq = pltpu.make_async_copy(wq_ref, wq, local.at[1])
    load_mod.start()
    load_wq.start()
    links.clear(*[ref.at[text, k] for ref in (xp_ref, g_ref) for k in (1, 2, 3)])
    links.enter(others)
    for c in (text, *range(text)):
        links.gather_start(x_ref.at[c], xp_ref, 0, c)
    load_mod.wait()
    act = act_ref[...]
    for j in range(12):
        terms[:, j, :] = nn_dot(act, modw[j])
    pushes = [
        pltpu.make_async_remote_copy(
            src_ref=terms.at[others[r]],
            dst_ref=got.at[r],
            send_sem=msend.at[r],
            recv_sem=mrecv.at[r],
            device_id={"dp": others[r]},
            device_id_type=MESH,
        )
        for r in range(dp - 1)
    ]
    for push in pushes:
        push.start()
    for c in range(count):
        xp_ref[c, 0] = x_ref[c]
    total = terms[mine] + modb_ref[...].astype(F32)
    for r, push in enumerate(pushes):
        push.wait_recv()
        total = total + got[r]
    mod_ref[0] = total
    mod_copies = [
        links.copy(mod_ref.at[0], mod_ref.at[k], 6, k, links.peers[k]) for k in (1, 2, 3)
    ]
    for copy in mod_copies:
        copy.start()
    for c in (text, *range(text)):
        links.gather_relay(x_ref.at[c], xp_ref, 0, c)
    for c in range(count):
        stream = c // (count - 1)
        g = (total[stream * 6 + 5 : stream * 6 + 6, :] * cot_ref[c].astype(F32)).astype(BF16)
        g_ref[c, 0] = g
        gsum_ref[c : c + 1, :] = jnp.sum(g.astype(F32), axis=0, keepdims=True)
    for c in (text, *range(text)):
        links.gather_start(g_ref.at[c, 0], g_ref, 3, c)
    for copy in mod_copies:
        copy.wait_recv()
    load_wq.wait()

    def project(s, carry):
        c = (s + text) % count
        stream = c // (count - 1)
        links.gather_finish(x_ref.at[c], xp_ref, 0, c)
        _, inv, centred = norm_stats([xp_ref[c, k].astype(F32) for k in range(4)], width)
        acc = [None] * 3
        for k in range(4):
            shift = mod_ref[k, pl.ds(stream * 6, 1), :]
            scale = mod_ref[k, pl.ds(stream * 6 + 1, 1), :]
            m = (centred[k] * inv * (1.0 + scale) + shift).astype(BF16)
            m_ref[c, k] = m
            for j in range(3):
                part = nn_dot(m, wq[stream, j, links.peers[k]])
                acc[j] = part if k == 0 else acc[j] + part
        for j in range(3):
            qkv_ref[j, c] = (acc[j] + bq_ref[stream, j : j + 1, :].astype(F32)).astype(BF16)
        links.gather_relay(g_ref.at[c, 0], g_ref, 3, c)

        @pl.when(s == 0)
        def _():
            column.deal(m_ref.at[text], zm_ref, 0, taken)
            column.deal_own(m_ref.at[text], zm_ref, local.at[2], taken).start()

        return carry

    lax.fori_loop(0, count, project, 0)

    owner = lax.broadcasted_iota(jnp.int32, (1, 128), 1) // HEAD_DIM

    def heads_pair(p, carry):
        lanes = pl.ds(pl.multiple_of(p * 128, 128), 128)
        for c in range(count):
            size = min(rows, valid - c * rows)
            sl = slice(c * rows, c * rows + size)
            k_all[sl, :] = qkv_ref[1, c, :size, lanes]
            values = qkv_ref[2, c, :size, lanes]
            for h in range(2):
                aug[h, sl, :] = jnp.where(owner == h, values, jnp.ones_like(values))

        def chunk(c, inner):
            q = qkv_ref[0, c, :, lanes] * jnp.asarray(HEAD_DIM**-0.5, BF16)
            out, lse = [], []
            for h in range(2):
                scores = nt_dot(jnp.where(owner == h, q, jnp.zeros_like(q)), k_all[...])
                top = jnp.max(scores, axis=-1, keepdims=True)
                acc = nn_dot(jnp.exp(scores - top).astype(BF16), aug[h])
                other = (1 - h) * HEAD_DIM
                denom = acc[:, other : other + 1]
                out.append(acc / denom)
                lse.append(top + jnp.log(denom))
            o_ref[c, :, lanes] = jnp.where(owner == 0, out[0], out[1]).astype(BF16)
            lse_ref[c, :, lanes] = jnp.where(owner == 0, lse[0], lse[1])
            return inner

        lax.fori_loop(0, count, chunk, 0)
        return carry

    lax.fori_loop(0, cols // 128, heads_pair, 0)
    for c in range(count):
        links.gather_finish(g_ref.at[c, 0], g_ref, 3, c)
        links.gather_sent(x_ref.at[c], xp_ref, 0, c)
        links.gather_sent(g_ref.at[c, 0], g_ref, 3, c)
    wait_sends(mod_copies)
    wait_sends(pushes)
    column.deal_own(m_ref.at[text], zm_ref, local.at[2], taken).wait()
    column.deal_wait(m_ref.at[text], zm_ref, 0, taken)


def front_call(dp, valid, taken, x, cot, act, mod_w, mod_b, wq, bq):
    count, rows, feats = x.shape
    cols = wq.shape[-1]
    arrays = [x, cot, act, mod_w, mod_b, wq, bq]
    outs = [
        sds((count, 4, rows, feats), BF16),
        sds((3, count, rows, cols), BF16),
        sds((count, rows, cols), BF16),
        sds((count, rows, cols), F32),
        sds((count, 4, rows, feats), BF16),
        sds((count, 4, rows, feats), BF16),
        sds((4, 12, feats), F32),
        sds((count, feats), F32),
        sds((dp // 2, taken, feats), BF16),
    ]
    n_in, n_out = len(arrays), len(outs)

    def kernel(*refs):
        front_kernel(dp, valid, refs[:n_in], refs[n_in : n_in + n_out], refs[n_in + n_out :])

    return pl.pallas_call(
        kernel,
        out_shape=outs,
        in_specs=[VMEM, VMEM, VMEM, ANY, VMEM, ANY, VMEM],
        out_specs=[VMEM] * (n_out - 1) + [ANY],
        scratch_shapes=[
            pltpu.VMEM(mod_w.shape, BF16),
            pltpu.VMEM(wq.shape, BF16),
            pltpu.VMEM((dp, 12, feats), F32),
            pltpu.VMEM((dp - 1, 12, feats), F32),
            pltpu.VMEM((valid, 128), BF16),
            pltpu.VMEM((2, valid, 128), BF16),
            pltpu.SemaphoreType.DMA((3,)),
            pltpu.SemaphoreType.DMA((7, count)),
            pltpu.SemaphoreType.DMA((7, count)),
            pltpu.SemaphoreType.DMA((dp - 1,)),
            pltpu.SemaphoreType.DMA((dp - 1,)),
            pltpu.SemaphoreType.DMA((1, dp // 2 - 1)),
            pltpu.SemaphoreType.DMA((1, dp // 2 - 1)),
        ],
        compiler_params=pltpu.CompilerParams(
            collective_id=1, has_side_effects=True, vmem_limit_bytes=56 * MIB
        ),
        cost_estimate=cost(20 * 10**9, arrays, outs),
        name="front",
    )(*arrays)


HB = 512


def middle_kernel(chips, refs_in, refs_out, scratch):
    o_ref, x_ref, cot_ref, db2_ref, mod_ref, wo_ref, up_ref, down_ref, ub_ref, ob_ref = refs_in
    x1_out, m2_out, a_out, du_out, b2_out, g1_out = refs_out[:6]
    g_ref, do_ref, line_ref, dub_ref, zr_ref, zl_ref, zo_ref = refs_out[6:]
    (wo, up, down, db2, part, relayed, got, xp, branch, acc_m, acc_b, cols_s) = scratch[:12]
    (x1_s, m2_s, a_s, du_s, b2_s, g1_s, srow, sgot, local, out_sem, send, recv) = scratch[12:24]
    zsend, zrecv, zlocal = scratch[24:]
    count, rows, feats = x_ref.shape
    width = 4 * feats
    hidden = up.shape[-1]
    text = count - 1
    taken = zo_ref.shape[1]
    links = Links(send, recv, text, rows, taken)
    column = Column(chips, zsend, zrecv)

    def at(s):
        return (s + text) % count

    loads = [
        pltpu.make_async_copy(src, dst, local.at[i])
        for i, (src, dst) in enumerate(
            [(wo_ref, wo), (up_ref, up), (down_ref, down), (db2_ref, db2)]
        )
    ]
    for load in loads:
        load.start()
    links.clear(*[ref.at[text, k] for ref in (xp, g_ref) for k in (1, 2, 3)])
    links.clear(*[got.at[text, k] for k in (0, 1, 2)])
    links.enter(column.others)
    loads[0].wait()

    def flush(staged, out, kind, s):
        return pltpu.make_async_copy(staged.at[s % 2], out.at[at(s)], out_sem.at[kind, s % 2])

    first_rows = pl.ds(0, taken)

    def own_rights():
        return [
            pltpu.make_async_copy(
                du_s.at[0, first_rows, :], zr_ref.at[column.z, 0], zlocal.at[0]
            ),
            pltpu.make_async_copy(a_s.at[0, first_rows, :], zr_ref.at[column.z, 1], zlocal.at[1]),
            column.deal_own(m2_s.at[0], zl_ref.at[0], zlocal.at[2], taken),
        ]

    def own_early():
        return [
            pltpu.make_async_copy(o_ref.at[text, first_rows, :], zo_ref.at[column.z], zlocal.at[3]),
            column.deal_own(db2.at[text], zl_ref.at[1], zlocal.at[4], taken),
        ]

    def own_last():
        return column.deal_own(g_ref.at[text], zl_ref.at[2], zlocal.at[5], taken)

    def column_early(s):
        @pl.when(s == 0)
        def _():
            loads[3].wait()
            for copy in own_early():
                copy.start()
            column.deal(db2.at[text], zl_ref.at[1], 3, taken)
            for copy in own_early():
                copy.wait()
            column.spread(zo_ref, 1, 0)

    def column_start(s):
        @pl.when(s == 0)
        def _():
            for copy in own_rights():
                copy.wait()
            flush(m2_s, m2_out, 1, 0).wait()
            column.spread(zr_ref, 0, 0)
            column.deal(m2_out.at[text], zl_ref.at[0], 2, taken)
            column.spread(zo_ref, 1, 1)

    def column_relay(dist):
        def step(s):
            @pl.when(s == 0)
            def _():
                column.spread(zr_ref, 0, dist)
                if dist == 1:
                    column.spread(zo_ref, 1, 2)

        return step

    def project(s):
        c = at(s)
        stream = c // (count - 1)
        o = o_ref[c]
        for k in (3, 1, 2, 0):
            part[c, k] = nt_dot(o, wo[stream, links.peers[k]]).astype(BF16)
        links.scatter_start(part, relayed, got, 0, c)

    def first_relay(s):
        c = at(s)
        links.scatter_relay(part, relayed, got, 0, c)

    def residual(s):
        c = at(s)
        stream = c // (count - 1)
        total = links.scatter_finish(part, relayed, got, 0, c)
        bias = jnp.where(c == text, ob_ref[1:2, :], ob_ref[0:1, :]).astype(F32)
        add = total + bias
        branch[c] = add
        moved = x_ref[c].astype(F32) + mod_ref[0, pl.ds(stream * 6 + 2, 1), :] * add

        @pl.when(s >= 2)
        def _():
            flush(x1_s, x1_out, 0, s - 2).wait()

        x1_s[s % 2] = moved
        flush(x1_s, x1_out, 0, s).start()
        xp[c, 0] = moved.astype(BF16)
        links.gather_start(xp.at[c, 0], xp, 3, c)

    def second_relay(s):
        c = at(s)
        links.gather_relay(xp.at[c, 0], xp, 3, c)

    def feed_forward(s):
        c = at(s)
        stream = c // (count - 1)
        slot = s % 2

        @pl.when(s == 0)
        def _():
            for load in loads[1:3]:
                load.wait()

        @pl.when(s >= 2)
        def _():
            for kind, (staged, out) in enumerate(
                [(a_s, a_out), (du_s, du_out), (b2_s, b2_out)]
            ):
                flush(staged, out, kind + 2, s - 2).wait()

        @pl.when(s >= 3)
        def _():
            flush(m2_s, m2_out, 1, s - 2).wait()

        links.gather_finish(xp.at[c, 0], xp, 3, c)
        links.scatter_sent(part, relayed, got, 0, c)
        mean, inv, centred = norm_stats([xp[c, k].astype(F32) for k in range(4)], width)
        for k in range(4):
            shift = mod_ref[k, pl.ds(stream * 6 + 3, 1), :]
            scale = mod_ref[k, pl.ds(stream * 6 + 4, 1), :]
            m2_s[slot, k] = (centred[k] * inv * (1.0 + scale) + shift).astype(BF16)

        def block(b, carry):
            cols = pl.ds(pl.multiple_of(b * HB, HB), HB)
            u = jnp.where(c == text, ub_ref[1:2, cols], ub_ref[0:1, cols]).astype(F32)
            for k in range(4):
                u = u + nn_dot(m2_s[slot, k], up[stream, links.peers[k], :, cols])
            da = None
            for k in range(4):
                piece = nn_dot(db2[c, k], down[stream, links.peers[k], :, cols])
                da = piece if da is None else da + piece
            square = u * u
            th = jnp.tanh(u * (GELU_C + (GELU_C * GELU_K) * square))
            up_half = 0.5 + 0.5 * th
            a = (u * up_half).astype(BF16)
            slope = up_half * (
                1.0 + u * (1.0 - th) * (GELU_C + (3.0 * GELU_C * GELU_K) * square)
            )
            du = (da * slope).astype(BF16)
            a_s[slot, :, cols] = a
            du_s[slot, :, cols] = du
            dub_ref[pl.ds(c, 1), cols] = jnp.sum(du.astype(F32), axis=0, keepdims=True)
            for k in range(4):
                dm = nt_dot(du, up[stream, links.peers[k], :, cols])
                bb = nt_dot(a, down[stream, links.peers[k], :, cols])

                @pl.when(b == 0)
                def _():
                    acc_m[k] = dm
                    acc_b[k] = bb

                @pl.when(b != 0)
                def _():
                    acc_m[k] += dm
                    acc_b[k] += bb

            return carry

        lax.fori_loop(0, hidden // HB, block, 0)
        first = second = None
        for k in range(4):
            dm = acc_m[k]
            part[c, k] = dm.astype(BF16)
            dh = dm * (1.0 + mod_ref[k, pl.ds(stream * 6 + 4, 1), :])
            one = jnp.sum(dh, axis=-1, keepdims=True)
            two = jnp.sum(dh * (xp[c, k].astype(F32) - mean), axis=-1, keepdims=True)
            first = one if first is None else first + one
            second = two if second is None else second + two
        srow[c] = stat_rows(first, second * inv)
        links.scatter_start(part, relayed, got, 6, c)
        links.rows_start(srow, sgot, 12, c)
        cols_s[c] = stat_cols(mean, inv)
        for k in range(4):
            b2_s[slot, k] = acc_b[k].astype(BF16)
        for kind, (staged, out) in enumerate(
            [(m2_s, m2_out), (a_s, a_out), (du_s, du_out), (b2_s, b2_out)]
        ):
            flush(staged, out, kind + 1, s).start()

        @pl.when(s == 0)
        def _():
            for copy in own_rights():
                copy.start()

    def third_relay(s):
        c = at(s)
        links.scatter_relay(part, relayed, got, 6, c)

    def norm_back(s):
        c = at(s)
        stream = c // (count - 1)
        total = links.scatter_finish(part, relayed, got, 6, c)
        sums = exact_tn(links.rows_finish(srow, sgot, 12, c), eye_rows())
        mean, inv = cols_s[c, :, 0:1], cols_s[c, :, 1:2]
        normed = (xp[c, 0].astype(F32) - mean) * inv
        grad = total * (1.0 + mod_ref[0, pl.ds(stream * 6 + 4, 1), :])
        g = cot_ref[c].astype(F32) + inv * (
            grad - sums[:, 0:1] / width - normed * (sums[:, 1:2] / width)
        )
        db = (mod_ref[0, pl.ds(stream * 6 + 2, 1), :] * g).astype(BF16)
        g_ref[c, 0] = db
        links.gather_start(g_ref.at[c, 0], g_ref, 9, c)

        @pl.when(s >= 2)
        def _():
            flush(g1_s, g1_out, 5, s - 2).wait()

        g1_s[s % 2] = g
        flush(g1_s, g1_out, 5, s).start()
        line_ref[c, 0:1, :] = jnp.sum(total, axis=0, keepdims=True)
        line_ref[c, 1:2, :] = jnp.sum(total * normed, axis=0, keepdims=True)
        line_ref[c, 2:3, :] = jnp.sum(branch[c] * g, axis=0, keepdims=True)
        line_ref[c, 3:4, :] = jnp.sum(db.astype(F32), axis=0, keepdims=True)

    def fourth_relay(s):
        c = at(s)
        links.gather_relay(g_ref.at[c, 0], g_ref, 9, c)

    def head_grads(s):
        c = at(s)
        stream = c // (count - 1)
        links.gather_finish(g_ref.at[c, 0], g_ref, 9, c)
        acc = None
        for k in range(4):
            piece = nn_dot(g_ref[c, k], wo[stream, links.peers[k]])
            acc = piece if acc is None else acc + piece
        do_ref[c] = acc.astype(BF16)

        @pl.when(s == 0)
        def _():
            column.deal(g_ref.at[text], zl_ref.at[2], 4, taken)
            own_last().start()

    stages(
        count,
        [
            (7, fourth_relay),
            (5, third_relay),
            (3, second_relay),
            (1, first_relay),
            (6, norm_back),
            (2, residual),
            (0, project),
            (1, column_early),
            (5, column_start),
            (7, column_relay(1)),
            (9, column_relay(2)),
            (8, head_grads),
            (4, feed_forward),
        ],
    )
    column.spread(zr_ref, 0, chips - 1)
    column.spread(zo_ref, 1, chips - 1)
    column.deal_wait(m2_out.at[text], zl_ref.at[0], 2, taken)
    column.deal_wait(db2.at[text], zl_ref.at[1], 3, taken)
    column.deal_wait(g_ref.at[text], zl_ref.at[2], 4, taken)
    own_last().wait()
    column.spread_sent(zr_ref, 0)
    column.spread_sent(zo_ref, 1)
    for c in range(count):
        links.gather_sent(xp.at[c, 0], xp, 3, c)
        links.scatter_sent(part, relayed, got, 6, c)
        links.gather_sent(g_ref.at[c, 0], g_ref, 9, c)
        wait_sends(links.rows_copies(srow, sgot, 12, c))
    for c in (count - 2, count - 1):
        for kind, (staged, out) in enumerate(
            [
                (x1_s, x1_out),
                (m2_s, m2_out),
                (a_s, a_out),
                (du_s, du_out),
                (b2_s, b2_out),
                (g1_s, g1_out),
            ]
        ):
            flush(staged, out, kind, c).wait()


def middle_call(dp, taken, o, x, cot, db2, mods, wo, up, down, ub, ob):
    count, rows, feats = x.shape
    cols, hidden = wo.shape[-1], up.shape[-1]
    arrays = [o, x, cot, db2, mods, wo, up, down, ub, ob]
    outs = [
        sds((count, rows, feats), F32),
        sds((count, 4, rows, feats), BF16),
        sds((count, rows, hidden), BF16),
        sds((count, rows, hidden), BF16),
        sds((count, 4, rows, feats), BF16),
        sds((count, rows, feats), F32),
        sds((count, 4, rows, feats), BF16),
        sds((count, rows, cols), BF16),
        sds((count, 4, feats), F32),
        sds((count, hidden), F32),
        sds((dp // 2, 2, taken, hidden), BF16),
        sds((3, dp // 2, taken, feats), BF16),
        sds((dp // 2, taken, cols), BF16),
    ]
    n_in, n_out = len(arrays), len(outs)

    def kernel(*refs):
        middle_kernel(dp // 2, refs[:n_in], refs[n_in : n_in + n_out], refs[n_in + n_out :])

    return pl.pallas_call(
        kernel,
        out_shape=outs,
        in_specs=[VMEM, VMEM, VMEM, ANY, VMEM, ANY, ANY, ANY, VMEM, VMEM],
        out_specs=[ANY] * 6 + [VMEM] * 4 + [ANY] * 3,
        scratch_shapes=[
            pltpu.VMEM(wo.shape, BF16),
            pltpu.VMEM(up.shape, BF16),
            pltpu.VMEM(down.shape, BF16),
            pltpu.VMEM(db2.shape, BF16),
            pltpu.VMEM((count, 4, rows, feats), BF16),
            pltpu.VMEM((count, rows, feats), BF16),
            pltpu.VMEM((count, 3, rows, feats), BF16),
            pltpu.VMEM((count, 4, rows, feats), BF16),
            pltpu.VMEM((count, rows, feats), F32),
            pltpu.VMEM((4, rows, feats), F32),
            pltpu.VMEM((4, rows, feats), F32),
            pltpu.VMEM((count, rows, 128), F32),
            pltpu.VMEM((2, rows, feats), F32),
            pltpu.VMEM((2, 4, rows, feats), BF16),
            pltpu.VMEM((2, rows, hidden), BF16),
            pltpu.VMEM((2, rows, hidden), BF16),
            pltpu.VMEM((2, 4, rows, feats), BF16),
            pltpu.VMEM((2, rows, feats), F32),
            pltpu.VMEM((count, 8, rows), F32),
            pltpu.VMEM((count, 3, 8, rows), F32),
            pltpu.SemaphoreType.DMA((4,)),
            pltpu.SemaphoreType.DMA((6, 2)),
            pltpu.SemaphoreType.DMA((15, count)),
            pltpu.SemaphoreType.DMA((15, count)),
            pltpu.SemaphoreType.DMA((5, dp - 2)),
            pltpu.SemaphoreType.DMA((5, dp - 2)),
            pltpu.SemaphoreType.DMA((6,)),
        ],
        compiler_params=pltpu.CompilerParams(
            collective_id=2, has_side_effects=True, vmem_limit_bytes=63 * MIB
        ),
        cost_estimate=cost(30 * 10**9, arrays, outs),
        name="middle",
    )(*arrays)


def back_kernel(valid, taken, blocks, refs_in, refs_out, scratch):
    qkv_ref, o_ref, do_ref, lse_ref, b2_ref, x1_ref, cot_ref, mod_ref, db_ref = refs_in
    dqkv_ref, x2_ref, gate_ref = refs_out
    q_all, k_all, v_all, do_all, lse_all, od_all, dk_all, dv_all, dqt_all, dq_all = scratch[:10]
    relayed2, got2, send, recv = scratch[10:]
    count, rows, _ = cot_ref.shape
    cols = o_ref.shape[-1]
    text = count - 1
    links = Links(send, recv, text, rows, taken)
    links.clear(*[got2.at[text, k] for k in (0, 1, 2)])
    links.enter()
    for c in range(count):
        links.scatter_start(b2_ref, relayed2, got2, 0, c)
    scale = jnp.asarray(HEAD_DIM**-0.5, BF16)
    head_row = lax.broadcasted_iota(jnp.int32, (8, 128), 0)
    lane = lax.broadcasted_iota(jnp.int32, (8, 128), 1)
    first_lane = (lane == head_row * HEAD_DIM).astype(F32)
    within = (lane // HEAD_DIM == head_row).astype(F32)
    owner = lax.broadcasted_iota(jnp.int32, (1, 128), 1) // HEAD_DIM
    zero = jnp.zeros((), BF16)
    for c in range(count):
        size = min(rows, valid - c * rows)
        if size < rows:
            for j in range(3):
                dqkv_ref[j, c] = jnp.zeros((rows, cols), BF16)

    def heads_pair(p, carry):
        lanes = pl.ds(pl.multiple_of(p * 128, 128), 128)
        for c in range(count):
            size = min(rows, valid - c * rows)
            sl = slice(c * rows, c * rows + size)
            q_all[sl, :] = qkv_ref[0, c, :size, lanes] * scale
            k_all[sl, :] = qkv_ref[1, c, :size, lanes]
            v_all[sl, :] = qkv_ref[2, c, :size, lanes]
            do = do_ref[c, :size, lanes]
            do_all[sl, :] = do
            lse_all[sl, :] = lse_ref[c, :size, lanes]
            od_all[sl, :] = o_ref[c, :size, lanes].astype(F32) * do.astype(F32)
        lse_rows = exact_nt(first_lane, lse_all[...])
        dot_rows = exact_nt(within, od_all[...])
        dqt = None
        for h in range(2):
            mine = owner == h
            q = jnp.where(mine, q_all[...], zero)
            do = jnp.where(mine, do_all[...], zero)
            lse_row, dot_row = lse_rows[h : h + 1, :], dot_rows[h : h + 1, :]
            for start, size in blocks:
                sl = slice(start, start + size)
                keys, values = k_all[sl, :], v_all[sl, :]
                weights = jnp.exp(nt_dot(keys, q) - lse_row)
                grads = (weights * (nt_dot(values, do) - dot_row)).astype(BF16)
                dv = nn_dot(weights.astype(BF16), do)
                dk = nn_dot(grads, q)
                if h == 0:
                    dv_all[sl, :] = dv
                    dk_all[sl, :] = dk
                else:
                    dv_all[sl, :] += dv
                    dk_all[sl, :] += dk
                piece = tn_dot(jnp.where(mine, keys, zero) * scale, grads)
                dqt = piece if dqt is None else dqt + piece
        dqt_all[:, :valid] = dqt
        dq_all[...] = dqt_all[...].T
        for c in range(count):
            size = min(rows, valid - c * rows)
            sl = slice(c * rows, c * rows + size)
            dqkv_ref[0, c, :size, lanes] = dq_all[sl, :].astype(BF16)
            dqkv_ref[1, c, :size, lanes] = dk_all[sl, :].astype(BF16)
            dqkv_ref[2, c, :size, lanes] = dv_all[sl, :].astype(BF16)

        @pl.when(p == pairs - 2)
        def _():
            for c in range(count):
                links.scatter_relay(b2_ref, relayed2, got2, 0, c)

        return carry

    pairs = cols // 128
    lax.fori_loop(0, pairs, heads_pair, 0)
    for c in range(count):
        stream = c // (count - 1)
        total = links.scatter_finish(b2_ref, relayed2, got2, 0, c)
        bias = jnp.where(c == text, db_ref[1:2, :], db_ref[0:1, :]).astype(F32)
        add = total + bias
        x2_ref[c] = x1_ref[c] + mod_ref[0, pl.ds(stream * 6 + 5, 1), :] * add
        gate_ref[c : c + 1, :] = jnp.sum(add * cot_ref[c].astype(F32), axis=0, keepdims=True)

    for c in range(count):
        links.scatter_sent(b2_ref, relayed2, got2, 0, c)


def back_call(valid, taken, qkv, o, do, lse, b2, x1, cot, mods, down_b):
    count, rows, feats = cot.shape
    padded = -(-valid // 128) * 128
    step = -(-valid // 3 // 16) * 16
    blocks = [(b, min(step, valid - b)) for b in range(0, valid, step)]
    arrays = [qkv, o, do, lse, b2, x1, cot, mods, down_b]
    outs = [
        sds(qkv.shape, BF16),
        sds((count, rows, feats), F32),
        sds((count, feats), F32),
    ]
    n_in, n_out = len(arrays), len(outs)

    def kernel(*refs):
        back_kernel(
            valid, taken, blocks, refs[:n_in], refs[n_in : n_in + n_out], refs[n_in + n_out :]
        )

    return pl.pallas_call(
        kernel,
        out_shape=outs,
        in_specs=[VMEM] * n_in,
        out_specs=[VMEM] * n_out,
        scratch_shapes=[pltpu.VMEM((valid, 128), BF16)] * 4
        + [pltpu.VMEM((valid, 128), F32)] * 4
        + [
            pltpu.VMEM((128, padded), F32),
            pltpu.VMEM((padded, 128), F32),
            pltpu.VMEM((count, rows, feats), BF16),
            pltpu.VMEM((count, 3, rows, feats), BF16),
            pltpu.SemaphoreType.DMA((3, count)),
            pltpu.SemaphoreType.DMA((3, count)),
        ],
        compiler_params=pltpu.CompilerParams(
            collective_id=3, has_side_effects=True, vmem_limit_bytes=56 * MIB
        ),
        cost_estimate=cost(30 * 10**9, arrays, outs),
        name="back",
    )(*arrays)


def last_kernel(chips, refs_in, refs_out, scratch):
    dqkv_ref, g1_ref, xp_ref, mod_ref, wq_ref = refs_in
    grad_ref, line_ref, bias_ref, zq_ref = refs_out
    wq, part, relayed, got, cols_s, srow, sgot, local, send, recv, zsend, zrecv = scratch
    count, rows, feats = g1_ref.shape
    width = 4 * feats
    text = count - 1
    taken = zq_ref.shape[2]
    links = Links(send, recv, text, rows, taken)
    column = Column(chips, zsend, zrecv)
    load = pltpu.make_async_copy(wq_ref, wq, local.at[0])
    load.start()
    own_q = [
        pltpu.make_async_copy(
            dqkv_ref.at[j, text, pl.ds(0, taken), :], zq_ref.at[column.z, j], local.at[1 + j]
        )
        for j in range(3)
    ]
    for copy in own_q:
        copy.start()
    links.clear(*[got.at[text, k] for k in (0, 1, 2)])
    links.enter(column.others)
    for copy in own_q:
        copy.wait()
    column.spread(zq_ref, 0, 0)
    load.wait()

    def column_step(dist):
        def step(c):
            @pl.when(c == 0)
            def _():
                column.spread(zq_ref, 0, dist)

        return step

    def input_grads(c):
        stream = c // (count - 1)
        mean, inv, centred = norm_stats([xp_ref[c, k].astype(F32) for k in range(4)], width)
        first = second = None
        for k in (3, 1, 2, 0):
            dm = None
            for j in range(3):
                piece = nt_dot(dqkv_ref[j, c], wq[stream, j, links.peers[k]])
                dm = piece if dm is None else dm + piece
            part[c, k] = dm.astype(BF16)
            dh = dm * (1.0 + mod_ref[k, pl.ds(stream * 6 + 1, 1), :])
            one = jnp.sum(dh, axis=-1, keepdims=True)
            two = jnp.sum(dh * centred[k], axis=-1, keepdims=True)
            first = one if first is None else first + one
            second = two if second is None else second + two
        srow[c] = stat_rows(first, second * inv)
        links.scatter_start(part, relayed, got, 3, c)
        links.rows_start(srow, sgot, 6, c)
        cols_s[c] = stat_cols(mean, inv)
        for j in range(3):
            bias_ref[c, j : j + 1, :] = jnp.sum(
                dqkv_ref[j, c].astype(F32), axis=0, keepdims=True
            )

    def last_relay(c):
        links.scatter_relay(part, relayed, got, 3, c)

    def norm_back(c):
        stream = c // (count - 1)
        total = links.scatter_finish(part, relayed, got, 3, c)
        sums = exact_tn(links.rows_finish(srow, sgot, 6, c), eye_rows())
        mean, inv = cols_s[c, :, 0:1], cols_s[c, :, 1:2]
        normed = (xp_ref[c, 0].astype(F32) - mean) * inv
        grad = total * (1.0 + mod_ref[0, pl.ds(stream * 6 + 1, 1), :])
        grad_ref[c] = g1_ref[c] + inv * (
            grad - sums[:, 0:1] / width - normed * (sums[:, 1:2] / width)
        )
        line_ref[c, 0:1, :] = jnp.sum(total, axis=0, keepdims=True)
        line_ref[c, 1:2, :] = jnp.sum(total * normed, axis=0, keepdims=True)

    stages(
        count,
        [
            (1, last_relay),
            (2, column_step(1)),
            (4, column_step(2)),
            (0, input_grads),
            (2, norm_back),
        ],
    )
    for c in range(count):
        links.scatter_sent(part, relayed, got, 3, c)
        wait_sends(links.rows_copies(srow, sgot, 6, c))
    column.spread(zq_ref, 0, chips - 1)
    column.spread_sent(zq_ref, 0)


def last_call(dp, taken, dqkv, g1, xp, mods, wq):
    count, rows, feats = g1.shape
    cols = dqkv.shape[-1]
    arrays = [dqkv, g1, xp, mods, wq]
    outs = [
        sds((count, rows, feats), F32),
        sds((count, 2, feats), F32),
        sds((count, 3, cols), F32),
        sds((dp // 2, 3, taken, cols), BF16),
    ]
    n_in, n_out = len(arrays), len(outs)

    def kernel(*refs):
        last_kernel(dp // 2, refs[:n_in], refs[n_in : n_in + n_out], refs[n_in + n_out :])

    return pl.pallas_call(
        kernel,
        out_shape=outs,
        in_specs=[VMEM] * 4 + [ANY],
        out_specs=[VMEM] * 3 + [ANY],
        scratch_shapes=[
            pltpu.VMEM(wq.shape, BF16),
            pltpu.VMEM((count, 4, rows, feats), BF16),
            pltpu.VMEM((count, rows, feats), BF16),
            pltpu.VMEM((count, 3, rows, feats), BF16),
            pltpu.VMEM((count, rows, 128), F32),
            pltpu.VMEM((count, 8, rows), F32),
            pltpu.VMEM((count, 3, 8, rows), F32),
            pltpu.SemaphoreType.DMA((4,)),
            pltpu.SemaphoreType.DMA((9, count)),
            pltpu.SemaphoreType.DMA((9, count)),
            pltpu.SemaphoreType.DMA((1, dp - 2)),
            pltpu.SemaphoreType.DMA((1, dp - 2)),
        ],
        compiler_params=pltpu.CompilerParams(
            collective_id=6, has_side_effects=True, vmem_limit_bytes=48 * MIB
        ),
        cost_estimate=cost(15 * 10**9, arrays, outs),
        name="last",
    )(*arrays)


def flat(value):
    return value.reshape((-1,) + value.shape[-1:])


def wgrad_kernel(pairs, split, t_ref, *refs):
    out_ref = refs[-1]
    slot = 0
    at = 0
    for groups in pairs:
        left, right = flat(refs[at][:, 0]), refs[at + 1]
        at += 2
        for j in range(groups):
            acc = tn_dot(left, flat(right[j] if groups > 1 else right[...]))
            size = acc.shape[0] // split
            for p in range(split):
                out_ref[p, slot] = acc[p * size : (p + 1) * size].astype(BF16)
            slot += 1


def wgrad_call(base, pairs, dp):
    count, _, rows, feats = pairs[0][0].shape
    chunks = count - 1
    cols = pairs[0][1].shape[-1]
    split = dp // 4
    groups = [right.shape[0] if right.ndim == 4 else 1 for _, right in pairs]
    slots = sum(groups)
    arrays, specs = [], []
    for (left, right), g in zip(pairs, groups):
        arrays += [left, right]
        specs.append(pl.BlockSpec((chunks, 1, rows, feats), lambda k, t: (0, k, 0, 0)))
        if g > 1:
            specs.append(pl.BlockSpec((g, chunks, rows, cols), lambda k, t: (0, 0, 0, 0)))
        else:
            specs.append(pl.BlockSpec((chunks, rows, cols), lambda k, t: (0, 0, 0)))
    out = sds((dp, slots, feats // split, cols), BF16)

    def kernel(*refs):
        wgrad_kernel(groups, split, *refs)

    return pl.pallas_call(
        kernel,
        out_shape=[out],
        grid_spec=pltpu.PrefetchScalarGridSpec(
            num_scalar_prefetch=1,
            grid=(4,),
            in_specs=specs,
            out_specs=[
                pl.BlockSpec(
                    (split, slots, feats // split, cols), lambda k, t: (t[0] ^ k, 0, 0, 0)
                )
            ],
        ),
        compiler_params=pltpu.CompilerParams(
            dimension_semantics=("arbitrary",), vmem_limit_bytes=48 * MIB
        ),
        cost_estimate=cost(2 * 4 * feats * slots * cols * chunks * rows, arrays, [out]),
    )(base, *arrays)[0]


def text_kernel(refs_in, refs_out, scratch):
    zm_ref, zl_ref, zq_ref, zr_ref, zo_ref = refs_in
    at_ref, ff_ref = refs_out
    send_a, got_a, send_f, got_f, keep_a, keep_f, send, recv = scratch
    index = lax.axis_index("dp")
    core = index % 2
    partner = index + 1 - 2 * core
    barrier = pltpu.get_barrier_semaphore()
    pl.semaphore_signal(barrier, inc=1, device_id={"dp": partner}, device_id_type=MESH)
    pl.semaphore_wait(barrier, 1)
    half = at_ref.shape[1]

    def move(src, dst, i):
        return pltpu.make_async_remote_copy(
            src_ref=src.at[i],
            dst_ref=dst.at[i],
            send_sem=send.at[i if src is send_a else 4 + i],
            recv_sem=recv.at[i if src is send_a else 4 + i],
            device_id={"dp": partner},
            device_id_type=MESH,
        )

    work = [
        (zl_ref.at[0], zr_ref.at[:, 0], keep_f, send_f, got_f, ff_ref, 0),
        (zl_ref.at[1], zr_ref.at[:, 1], keep_f, send_f, got_f, ff_ref, 1),
        (zm_ref, zq_ref.at[:, 0], keep_a, send_a, got_a, at_ref, 0),
        (zm_ref, zq_ref.at[:, 1], keep_a, send_a, got_a, at_ref, 1),
        (zm_ref, zq_ref.at[:, 2], keep_a, send_a, got_a, at_ref, 2),
        (zl_ref.at[2], zo_ref, keep_a, send_a, got_a, at_ref, 3),
    ]
    for left, right, keep, out, got, _, i in work:
        keep[i] = tn_dot(flat(left[...]), flat(right[...]))
        out[i] = keep[i, pl.ds((1 - core) * half, half), :].astype(BF16)
        move(out, got, i).start()
    for left, right, keep, out, got, final, i in work:
        move(out, got, i).wait_recv()
        final[i] = keep[i, pl.ds(core * half, half), :] + got[i].astype(F32)
    for left, right, keep, out, got, final, i in work:
        move(out, got, i).wait_send()


def text_call(zm, zl, zq, zr, zo):
    feats, cols, hidden = zm.shape[-1], zq.shape[-1], zr.shape[-1]
    half = feats // 2
    arrays = [zm, zl, zq, zr, zo]
    outs = [sds((4, half, cols), F32), sds((2, half, hidden), F32)]

    def kernel(*refs):
        text_kernel(refs[:5], refs[5:7], refs[7:])

    return pl.pallas_call(
        kernel,
        out_shape=outs,
        in_specs=[VMEM] * 5,
        out_specs=[VMEM] * 2,
        scratch_shapes=[
            pltpu.VMEM((4, half, cols), BF16),
            pltpu.VMEM((4, half, cols), BF16),
            pltpu.VMEM((2, half, hidden), BF16),
            pltpu.VMEM((2, half, hidden), BF16),
            pltpu.VMEM((4, feats, cols), F32),
            pltpu.VMEM((2, feats, hidden), F32),
            pltpu.SemaphoreType.DMA((6,)),
            pltpu.SemaphoreType.DMA((6,)),
        ],
        compiler_params=pltpu.CompilerParams(
            collective_id=4, has_side_effects=True, vmem_limit_bytes=40 * MIB
        ),
        cost_estimate=cost(6 * 10**9, arrays, outs),
        name="dw_text",
    )(*arrays)


def rows_kernel(dp, row_ref, all_ref, sum_ref, send, recv):
    mine = lax.axis_index("dp")
    others = [(mine + r) % dp for r in range(1, dp)]
    barrier = pltpu.get_barrier_semaphore()
    for peer in others:
        pl.semaphore_signal(barrier, inc=1, device_id={"dp": peer}, device_id_type=MESH)
    pl.semaphore_wait(barrier, dp - 1)
    copies = [
        pltpu.make_async_remote_copy(
            src_ref=row_ref,
            dst_ref=all_ref.at[mine],
            send_sem=send.at[r],
            recv_sem=recv.at[r],
            device_id={"dp": peer},
            device_id_type=MESH,
        )
        for r, peer in enumerate(others)
    ]
    for copy in copies:
        copy.start()
    all_ref[mine] = row_ref[...]
    for copy in copies:
        copy.wait()
    total = all_ref[0]
    for s in range(1, dp):
        total = total + all_ref[s]
    sum_ref[...] = total


def rows_call(dp, rows):
    outs = [sds((dp,) + rows.shape, F32), sds(rows.shape, F32)]
    return pl.pallas_call(
        functools.partial(rows_kernel, dp),
        out_shape=outs,
        in_specs=[VMEM],
        out_specs=[VMEM] * 2,
        scratch_shapes=[
            pltpu.SemaphoreType.DMA((dp - 1,)),
            pltpu.SemaphoreType.DMA((dp - 1,)),
        ],
        compiler_params=pltpu.CompilerParams(
            collective_id=5, has_side_effects=True, vmem_limit_bytes=16 * MIB
        ),
        cost_estimate=cost(10**6, [rows], outs),
        name="rows",
    )(rows)


def fast_body(
    dp,
    image_in,
    text_in,
    cond_in,
    mod_weight,
    mod_bias,
    qkv_weight,
    qkv_bias,
    out_weight,
    out_bias,
    up_weight,
    up_bias,
    down_weight,
    down_bias,
    image_cot,
    text_cot,
):
    base = lax.axis_index("tensor").astype(jnp.int32).reshape(1)
    feats = image_in.shape[2]
    images, texts = image_in.shape[1], text_in.shape[1]
    rows = images // 4
    valid = images + texts

    def join(image, text):
        padded = jnp.pad(text[0], ((0, rows - texts), (0, 0)))
        return jnp.concatenate([image[0].reshape(4, rows, feats), padded[None]], axis=0)

    def parted(value):
        image = value[:4].reshape(1, images, feats)
        return image, value[4:, :texts]

    x, cot = join(image_in, text_in), join(image_cot, text_cot)
    cond_float = cond_in.astype(F32)
    cond_act = jax.nn.silu(cond_float).astype(BF16)
    mod_w = jnp.transpose(mod_weight[0], (0, 2, 1, 3)).reshape(12, -1, feats)
    mod_b = mod_bias[0].reshape(12, feats)
    qkv_w = jnp.transpose(qkv_weight[0], (0, 2, 1, 3))
    qkv_w = qkv_w.reshape(2, 3, 4, feats, qkv_w.shape[-1])
    out_w = out_weight[0].reshape(2, 4, feats, -1)
    up_w = up_weight[0].reshape(2, 4, feats, -1)
    down_w = down_weight[0].reshape(2, 4, feats, -1)

    taken = -(-texts // 16) * 16
    m, qkv, o, lse, db2, xp, mods, db2_sum, zm = front_call(
        dp, valid, taken, x, cot, cond_act, mod_w, mod_b, qkv_w, qkv_bias[0]
    )
    x1, m2, act, du, b2, g1, db1, do, lines2, du_sum, zr, zl, zo = middle_call(
        dp, taken, o, x, cot, db2, mods, out_w, up_w, down_w, up_bias[0], out_bias[0]
    )
    part = wgrad_call(base, [(m2, du), (db2, act)], dp)
    do, part = lax.optimization_barrier((do, part))
    ff_sum = lax.psum_scatter(part, "dp", scatter_dimension=0, tiled=True)
    dqkv, x2, gate2 = back_call(
        valid, taken, qkv, o, do, lse, b2, x1, cot, mods, down_bias[0]
    )
    part2 = wgrad_call(base, [(m, dqkv), (db1, o)], dp)
    part2, dqkv = lax.optimization_barrier((part2, dqkv))
    at_sum = lax.psum_scatter(part2, "dp", scatter_dimension=0, tiled=True)
    grad, lines1, qkv_sum, zq = last_call(dp, taken, dqkv, g1, xp, mods, qkv_w)
    at_text, ff_text = text_call(zm, zl, zq, zr, zo)

    def by_stream(value):
        return jnp.stack([jnp.sum(value[:4], axis=0), value[4]])

    late, early = by_stream(lines1), by_stream(lines2)
    mod_rows = jnp.stack(
        [late[:, 0], late[:, 1], early[:, 2], early[:, 0], early[:, 1], by_stream(gate2)], axis=1
    )
    mod_rows = mod_rows.reshape(12, feats).astype(BF16).astype(F32)
    every = [
        mod_rows,
        by_stream(qkv_sum).reshape(6, feats),
        early[:, 3],
        by_stream(du_sum).reshape(8, feats),
        by_stream(db2_sum),
        jnp.zeros((2, feats), F32),
    ]
    all_rows, row_sums = rows_call(dp, jnp.concatenate(every, axis=0))
    all_mod = all_rows[:, :12].astype(BF16)
    mod_wgrad = jnp.einsum("sc,sgd->gcd", cond_act, all_mod, preferred_element_type=F32)
    mod_wgrad = jnp.transpose(mod_wgrad.reshape(1, 2, 6, -1, feats), (0, 1, 3, 2, 4))
    act_part = jnp.einsum("sgd,gcd->sc", all_mod, mod_w, preferred_element_type=F32)
    act_total = act_part + sum(
        lax.ppermute(act_part, "tensor", [(i, i ^ k) for i in range(4)]) for k in (1, 2, 3)
    )
    cond_grad = jax.vjp(jax.nn.silu, cond_float)[1](act_total)[0]
    mod_bgrad = row_sums[:12].reshape(1, 2, 6, feats)
    biases = (
        row_sums[12:18].reshape(1, 2, 3, feats),
        row_sums[18:20][None],
        row_sums[20:28].reshape(1, 2, 4 * feats),
        row_sums[28:30][None],
    )
    at_image, ff_image = at_sum[0].astype(F32), ff_sum[0].astype(F32)
    qkv_wgrad = jnp.transpose(jnp.stack([at_image[:3], at_text[:3]])[None], (0, 1, 3, 2, 4))

    def streams(image, text):
        return jnp.stack([image, text])[None]

    image_out, text_out = parted(x2)
    image_grad, text_grad = parted(grad)
    return (
        image_out,
        text_out,
        image_grad,
        text_grad,
        cond_grad,
        mod_wgrad,
        mod_bgrad,
        qkv_wgrad,
        biases[0],
        streams(at_image[3], at_text[3]),
        biases[1],
        streams(ff_image[0], ff_text[0]),
        biases[2],
        streams(ff_image[1], ff_text[1]),
        biases[3],
    )


def solution(mesh):
    dp, tensor = mesh.shape["dp"], mesh.shape["tensor"]
    square = dp == 8 and tensor == 4
    chosen = functools.partial(fast_body, dp) if square else plain_body
    return jax.shard_map(
        chosen,
        mesh=mesh,
        in_specs=(
            P("dp", None, "tensor"),
            P("dp", None, "tensor"),
            P(None, "dp"),
            P(None, None, "dp", None, "tensor"),
            P(None, None, None, "tensor"),
            P(None, None, None, None, "tensor"),
            P(None, None, None, "tensor"),
            P(None, None, None, "tensor"),
            P(None, None, "tensor"),
            P(None, None, None, "tensor"),
            P(None, None, "tensor"),
            P(None, None, None, "tensor"),
            P(None, None, "tensor"),
            P("dp", None, "tensor"),
            P("dp", None, "tensor"),
        ),
        out_specs=(
            P("dp", None, "tensor"),
            P("dp", None, "tensor"),
            P("dp", None, "tensor"),
            P("dp", None, "tensor"),
            P(None, "dp"),
            P(None, None, "dp", None, "tensor"),
            P(None, None, None, "tensor"),
            P(None, None, "dp", None, "tensor"),
            P(None, None, None, "tensor"),
            P(None, None, "dp", "tensor"),
            P(None, None, "tensor"),
            P(None, None, "dp", "tensor"),
            P(None, None, "tensor"),
            P(None, None, "dp", "tensor"),
            P(None, None, "tensor"),
        ),
        check_vma=False,
    )
```
